32 devices in a mesh: space: 8 (over z, y), slab: 4 (over x, core).
Axes of the slice: x: 2, y: 2, z: 4, core: 2. Of those that a mesh axis runs over, the one named last changes fastest.
Arguments:
- displacement: float32 [3, 128, 32, 256], P(None, 'space', 'slab'), may hold values from -0.1 to 0.1
- velocity: float32 [3, 128, 32, 256], P(None, 'space', 'slab'), may hold values from -6 to 6
- stress: float32 [6, 128, 32, 256], P(None, 'space', 'slab'), may hold values from -6 to 6
- hourglass: float32 [128, 32, 256], P('space', 'slab'), may hold values from 0.02 to 0.2
- mass: float32 [128, 32, 256], P('space', 'slab'), may hold values from 1 to 4
- contact_route: int32 [8192], P(('space', 'slab')), may hold values from 0 to 383, as said below
- pair_nodes: int32 [5, 32768], P(None, ('space', 'slab')), may hold values from 0 to 383, as said below
- pair_diagonals: float32 [6, 32768], P(None, ('space', 'slab')), may hold values from -5 to 5
- pair_gap: float32 [32768], P(('space', 'slab')), may hold values from -0.3 to 0.3
- pair_stiffness: float32 [32768], P(('space', 'slab')), may hold values from 1 to 10
Outputs:
- velocity_new: float32 [3, 128, 32, 256], P(None, 'space', 'slab')
The draws below stay inside these ranges and needn't reach their ends.
Inputs may be any that keep to these rules, and one draw needn't show every extreme that they name: `contact_route`: values of one device are distinct; value // 48 is the space index of the contact owner (same slab index), value % 48 the slot. In every draw one owner receives all 48 slots from every device of its group, and every owner receives a slot from the device of its own indices. `pair_nodes`: entries of the pairs of one owner name slots that are filled at that owner; entries of one pair need not differ.
All inputs are finite; a program needn't handle non-finite values.
Results may differ from the reference program's by a relative error of at most 0.0003.
Values sent between devices are 32-bit elements; how exact they have to be, the bound alone decides.
No kernel may reach another device: no remote copies, remote signals or barrier semaphores. Data moves between devices by JAX's collectives and lax.ppermute only.
A program may use at most 64 MiB of HBM per device.

```python
import math
import jax
import jax.numpy as jnp
from jax import lax

CX = 16
CY = 8
NZ = 256
P_DEV = 1024
PART_BOUNDARY = 256
HOLDER_LIMIT = 48
SLOTS = 384
NX = 128
NY = 32
PAIRS = 32768
N_SPACE = 8
N_SLAB = 4
DEVICES = 32


def route_table(key):
    elected_holder = jax.random.randint(jax.random.fold_in(key, 1), (), 0, N_SPACE)
    holder_ratings = jax.random.randint(jax.random.fold_in(key, 2), (DEVICES, SLOTS), 0, 2 ** 20)
    position_numbers = jnp.arange(SLOTS, dtype=jnp.int32)
    holder_room_remaining = jnp.arange(DEVICES, dtype=jnp.int32) // N_SLAB
    holder_preference = jnp.where(position_numbers // HOLDER_LIMIT == elected_holder, 2 ** 22, 0)[None, :]
    holder_preference = holder_preference + jnp.where(position_numbers[None, :] == holder_room_remaining[:, None] * HOLDER_LIMIT, 2 ** 21, 0)
    picked_positions = jnp.argsort(-(holder_ratings + holder_preference), axis=1, stable=True)[:, :PART_BOUNDARY]
    shuffle = jnp.argsort(jax.random.randint(jax.random.fold_in(key, 3), (DEVICES, PART_BOUNDARY), 0, 2 ** 20), axis=1, stable=True)
    return jnp.take_along_axis(picked_positions, shuffle, axis=1).astype(jnp.int32)


def draw_contact_route(key, part):
    return route_table(jax.random.fold_in(key, 11)).reshape(-1)


def draw_pair_nodes(key, part):
    route = route_table(jax.random.fold_in(key, 11))
    device_ids = jnp.arange(DEVICES, dtype=jnp.int32)
    owners = route // HOLDER_LIMIT * N_SLAB + (device_ids % N_SLAB)[:, None]
    position_numbers = (device_ids // N_SLAB)[:, None] * HOLDER_LIMIT + route % HOLDER_LIMIT
    live = jnp.zeros((DEVICES, SLOTS), jnp.int32).at[owners.reshape(-1), position_numbers.reshape(-1)].set(1)
    tiebreak = jax.random.randint(jax.random.fold_in(key, 12), (DEVICES, SLOTS), 0, 2 ** 20)
    order = jnp.argsort(-(live * 2 ** 21 + tiebreak), axis=1, stable=True).astype(jnp.int32)
    counts = jnp.sum(live, 1)
    ranks = jax.random.randint(jax.random.fold_in(key, 13), (DEVICES, 5 * P_DEV), 0, 2 ** 20) % counts[:, None]
    refs = jnp.take_along_axis(order, ranks, axis=1).reshape(DEVICES, 5, P_DEV)
    return jnp.transpose(refs, (1, 0, 2)).reshape(5, DEVICES * P_DEV).astype(jnp.int32)


def block_levels(own_key, shape, cuts, low, largest):
    factor_of, own = 1.0, jax.random.fold_in(own_key, 6)
    for axis_at, blocks in cuts:
        steps = jnp.exp(jax.random.uniform(jax.random.fold_in(own, axis_at), (blocks,), jnp.float32, low / len(cuts), largest / len(cuts)))
        factor_of = factor_of * jnp.repeat(steps, shape[axis_at] // blocks).reshape([-1 if axis == axis_at else 1 for axis in range(len(shape))])
    return factor_of


def noise(own_key, dims, spread, limit, shards=(), kind=jnp.bfloat16):
    array = jax.random.normal(own_key, dims, jnp.float32) * spread
    if len(shards) > 0:
        array = block_levels(own_key, dims, shards, -0.22, 0.18) * array
    return jnp.clip(array, min=-limit, max=limit).astype(kind)


def setup_inputs(seed: int = 0) -> dict:
    key_list = jax.random.split(jax.random.key(seed), 11)
    return {
        "displacement": jnp.clip(jax.random.uniform(key_list[0], (3, NX, NY, NZ), jnp.float32, -0.1, 0.1) * block_levels(key_list[0], (3, NX, NY, NZ), ((1, 8), (2, 4)), -0.4, 0.0), -0.1, 0.1),
        "velocity": noise(key_list[1], (3, NX, NY, NZ), 1.0, 6.0, ((1, 8), (2, 4)), jnp.float32),
        "stress": noise(key_list[2], (6, NX, NY, NZ), 1.0, 6.0, ((1, 8), (2, 4)), jnp.float32),
        "hourglass": jnp.clip(jnp.exp(math.log(0.2) - 2.3025851 * jax.random.uniform(key_list[3], (NX, NY, NZ), jnp.float32) ** block_levels(key_list[3], (NX, NY, NZ), ((0, 8), (1, 4)), -0.2, 0.2)), 0.02, 0.2),
        "mass": jnp.clip(jnp.exp(math.log(4.0) - 1.3862944 * jax.random.uniform(key_list[4], (NX, NY, NZ), jnp.float32) ** block_levels(key_list[4], (NX, NY, NZ), ((0, 8), (1, 4)), -0.2, 0.2)), 1.0, 4.0),
        "contact_route": draw_contact_route(jax.random.fold_in(key_list[10], 71), 0),
        "pair_nodes": draw_pair_nodes(jax.random.fold_in(key_list[10], 71), 0),
        "pair_diagonals": noise(key_list[7], (6, PAIRS), 1.0, 5.0, ((1, 32),), jnp.float32),
        "pair_gap": jnp.clip(jax.random.uniform(key_list[8], (PAIRS,), jnp.float32, -0.3, 0.3) * block_levels(key_list[8], (PAIRS,), ((0, 32),), -0.4, 0.0), -0.3, 0.3),
        "pair_stiffness": jnp.clip(jnp.exp(math.log(10.0) - 2.3025851 * jax.random.uniform(key_list[9], (PAIRS,), jnp.float32) ** block_levels(key_list[9], (PAIRS,), ((0, 32),), -0.2, 0.2)), 1.0, 10.0),
    }


time_step = 0.5


def element_forces(u_ext, v_ext, stress, hourglass, zmask):
    planes = stress.shape[1]
    columns = stress.shape[2]
    depth = stress.shape[3]
    corner_u = []
    corner_v = []
    signs = []
    for corner in range(8):
        offset_x = corner // 4
        offset_y = (corner // 2) % 2
        offset_z = corner % 2
        corner_u.append(jnp.roll(u_ext[:, offset_x:offset_x + planes, offset_y:offset_y + columns], -offset_z, 3))
        corner_v.append(jnp.roll(v_ext[:, offset_x:offset_x + planes, offset_y:offset_y + columns], -offset_z, 3))
        signs.append((2.0 * offset_x - 1.0, 2.0 * offset_y - 1.0, 2.0 * offset_z - 1.0))
    jacobian = []
    for m in range(3):
        line = []
        for n in range(3):
            total = jnp.full(corner_u[0].shape[1:], 0.5 if m == n else 0.0, jnp.float32)
            for corner in range(8):
                total = total + corner_u[corner][m] * (signs[corner][n] / 8.0)
            line.append(total)
        jacobian.append(line)
    cofactor = [[jacobian[(m + 1) % 3][(n + 1) % 3] * jacobian[(m + 2) % 3][(n + 2) % 3]
                 - jacobian[(m + 1) % 3][(n + 2) % 3] * jacobian[(m + 2) % 3][(n + 1) % 3]
                 for n in range(3)] for m in range(3)]
    voigt = [[0, 5, 4], [5, 1, 3], [4, 3, 2]]
    bases = [[s[1] * s[2] for s in signs], [s[0] * s[2] for s in signs],
             [s[0] * s[1] for s in signs], [s[0] * s[1] * s[2] for s in signs]]
    modes = []
    for i in range(4):
        modes.append(sum(bases[i][corner] * corner_v[corner] for corner in range(8)))
    output = jnp.zeros((3, planes + 1, columns + 1, depth), jnp.float32)
    for corner in range(8):
        offset_x = corner // 4
        offset_y = (corner // 2) % 2
        offset_z = corner % 2
        grads = [sum(cofactor[k][n] * signs[corner][n] for n in range(3)) for k in range(3)]
        viscous = sum(bases[i][corner] * modes[i] for i in range(4))
        parts = []
        for m in range(3):
            value = sum(stress[voigt[m][k]] * grads[k] for k in range(3))
            parts.append((value + hourglass * viscous[m]) * zmask)
        force = jnp.roll(jnp.stack(parts), offset_z, 3)
        output = output.at[:, offset_x:offset_x + planes, offset_y:offset_y + columns].add(force)
    return output


def pair_forces(table, pair_nodes, pair_diagonals, pair_gap, pair_stiffness, width):
    picked = [table[:, pair_nodes[j]] for j in range(5)]
    slave = picked[0]
    first = pair_diagonals[0:3] + picked[3] - picked[1]
    second = pair_diagonals[3:6] + picked[4] - picked[2]
    normal = jnp.stack([first[1] * second[2] - first[2] * second[1],
                        first[2] * second[0] - first[0] * second[2],
                        first[0] * second[1] - first[1] * second[0]])
    centre = (picked[1] + picked[2] + picked[3] + picked[4]) * 0.25
    gap = pair_gap + jnp.sum((slave - centre) * normal, 0)
    push = pair_stiffness * jnp.maximum(-gap, 0.0)
    slave_force = push * normal
    master_force = -0.25 * slave_force
    forces = jnp.zeros((3, width), jnp.float32).at[:, pair_nodes[0]].add(slave_force)
    for j in range(1, 5):
        forces = forces.at[:, pair_nodes[j]].add(master_force)
    return forces


def reference(displacement, velocity, stress, hourglass, mass, contact_route, pair_nodes, pair_diagonals, pair_gap, pair_stiffness):
    zmask = (jnp.arange(NZ) < NZ - 1).astype(jnp.float32)
    u_wrap = jnp.concatenate([displacement, displacement[:, :1]], 1)
    v_wrap = jnp.concatenate([velocity, velocity[:, :1]], 1)

    def block(index):
        start = (index * CX).astype(jnp.int32)
        u_ext = lax.dynamic_slice_in_dim(u_wrap, start, CX + 1, 1)
        v_ext = lax.dynamic_slice_in_dim(v_wrap, start, CX + 1, 1)
        u_ext = jnp.concatenate([u_ext, u_ext[:, :, :1]], 2)
        v_ext = jnp.concatenate([v_ext, v_ext[:, :, :1]], 2)
        local_stress = lax.dynamic_slice_in_dim(stress, start, CX, 1)
        local_visc = lax.dynamic_slice_in_dim(hourglass, start, CX, 0)
        out = element_forces(u_ext, v_ext, local_stress, local_visc, zmask)
        return out[:, :, :NY].at[:, :, 0].add(out[:, :, NY])

    blocks = lax.map(block, jnp.arange(N_SPACE, dtype=jnp.int32))
    main = blocks[:, :, :CX]
    extra = jnp.roll(blocks[:, :, CX], 1, 0)
    main = main.at[:, :, 0].add(extra)
    internal = jnp.transpose(main, (1, 0, 2, 3, 4)).reshape(3, NX, NY, NZ)

    shaped = displacement.reshape(3, N_SPACE, CX, N_SLAB, CY, NZ)
    faces = jnp.stack([shaped[..., 0], shaped[..., NZ - 1]], 1)
    faces = jnp.transpose(faces, (0, 2, 4, 1, 3, 5)).reshape(3, DEVICES * PART_BOUNDARY)
    device_ids = jnp.arange(DEVICES, dtype=jnp.int32)
    route = contact_route.reshape(DEVICES, PART_BOUNDARY)
    owners = (route // HOLDER_LIMIT) * N_SLAB + (device_ids % N_SLAB)[:, None]
    position_numbers = (device_ids // N_SLAB)[:, None] * HOLDER_LIMIT + route % HOLDER_LIMIT
    flat_index = (owners * SLOTS + position_numbers).reshape(-1)
    table = jnp.zeros((3, DEVICES * SLOTS), jnp.float32).at[:, flat_index].set(faces)
    refs = pair_nodes + ((jnp.arange(PAIRS, dtype=jnp.int32) // P_DEV) * SLOTS)[None, :]
    forces = pair_forces(table, refs, pair_diagonals, pair_gap, pair_stiffness, DEVICES * SLOTS)
    back = forces[:, flat_index].reshape(3, N_SPACE, N_SLAB, 2, CX, CY)
    back = jnp.transpose(back, (0, 3, 1, 4, 2, 5)).reshape(3, 2, NX, NY)
    contact = jnp.zeros((3, NX, NY, NZ), jnp.float32)
    contact = contact.at[..., 0].set(back[:, 0]).at[..., NZ - 1].set(back[:, 1])
    return velocity + time_step * (contact - internal) / mass
```

```python
import functools

import jax
import jax.numpy as jnp
from jax import lax
from jax.experimental import pallas as pl
from jax.experimental.pallas import tpu as pltpu
from jax.sharding import PartitionSpec as P

time_step = 0.5
LANES = 128
VOIGT = [[0, 5, 4], [5, 1, 3], [4, 3, 2]]


def moved(value, dx, dy):
    nx = lax.axis_size("space")
    ny = lax.axis_size("slab")
    pairs = [
        (a * ny + b, ((a + dx) % nx) * ny + (b + dy) % ny) for a in range(nx) for b in range(ny)
    ]
    return lax.ppermute(value, ("space", "slab"), pairs)


def kernel_call(body, outs, scratch=()):
    return pl.pallas_call(
        body,
        out_shape=outs,
        scratch_shapes=list(scratch),
    )


def three_parts(value):
    high = value.astype(jnp.bfloat16)
    rest = value - high.astype(jnp.float32)
    middle = rest.astype(jnp.bfloat16)
    low = (rest - middle.astype(jnp.float32)).astype(jnp.bfloat16)
    return jnp.concatenate([high, middle, low], 0)


def contract_lanes(lhs, rhs):
    return lax.dot_general(lhs, rhs, (((1,), (1,)), ((), ())), preferred_element_type=jnp.float32)


def layout(nspace, surf_count):
    capacity = max(2, (3 * surf_count // 2 + nspace - 1) // nspace)
    pack = max(1, LANES // capacity)
    while nspace % pack:
        pack -= 1
    return capacity, pack, nspace // pack


def route_body(nspace, capacity, pack, blocks, u_ref, route_ref, out_ref, rows_ref):
    planes, columns, depth = u_ref.shape[1:]
    side = planes * columns
    lane = lax.broadcasted_iota(jnp.int32, (side, LANES), 1)
    rows_ref[...] = jnp.zeros(rows_ref.shape, jnp.float32)
    for c in range(3):
        bottom = u_ref[c, :, :, 0:LANES].reshape(side, LANES)
        top = u_ref[c, :, :, depth - LANES : depth].reshape(side, LANES)
        both = jnp.where(lane == LANES - 1, top, bottom).T
        rows_ref[c : c + 1, 0:side] = both[0:1]
        rows_ref[c : c + 1, side : 2 * side] = both[LANES - 1 : LANES]
    parts = three_parts(rows_ref[...])
    route = route_ref[...]
    for b in range(blocks):
        slot = lax.broadcasted_iota(jnp.int32, (LANES, 2 * side), 0) + b * pack * capacity
        chosen = jnp.where(slot == route, 1.0, 0.0).astype(jnp.bfloat16)
        got = contract_lanes(parts, chosen)
        got = got[0:8] + got[8:16] + got[16:24]
        for q in range(pack):
            out_ref[b * pack + q] = got


def matrix_body(capacity, pack, blocks, nodes_ref, out_ref):
    rows = 16
    pairs = nodes_ref.shape[1]
    nodes = [nodes_ref[j : j + 1, :] for j in range(5)]
    for b in range(blocks):
        for g in range(LANES // rows):
            slot = lax.broadcasted_iota(jnp.int32, (rows, pairs), 0) + (
                b * pack * capacity + g * rows
            )
            total = jnp.where(nodes[0] == slot, 1.0, 0.0)
            for j in range(1, 5):
                total = total - jnp.where(nodes[j] == slot, 0.25, 0.0)
            start = b * LANES + g * rows
            out_ref[start : start + rows, :] = total.astype(jnp.bfloat16)


def looked_up(table_ref, slots, capacity, offset, count):
    shape = slots[0].shape

    def step(s, found):
        shift = s * capacity - offset
        result = []
        for slot, old in zip(slots, found):
            here = (slot >= s * capacity) & (slot < (s + 1) * capacity)
            index = (slot - shift) & (LANES - 1)
            new = []
            for c in range(3):
                row = jnp.broadcast_to(table_ref[s, c : c + 1, :], shape)
                new.append(jnp.where(here, jnp.take_along_axis(row, index, axis=1), old[c]))
            result.append(tuple(new))
        return tuple(result)

    zero = jnp.zeros(shape, jnp.float32)
    found = tuple((zero, zero, zero) for _ in slots)
    if count <= 16:
        for s in range(count):
            found = step(s, found)
        return found
    return lax.fori_loop(0, count, step, found)


def pair_body(
    nspace, capacity, pack, blocks, table_ref, nodes_ref, diag_ref, gap_ref, stiff_ref, matrix_ref, out_ref, rows_ref
):
    offset = (lax.axis_index("space") % pack) * capacity
    picked = looked_up(table_ref, [nodes_ref[j] for j in range(5)], capacity, offset, nspace)
    slave = picked[0]
    first = [diag_ref[c] + picked[3][c] - picked[1][c] for c in range(3)]
    second = [diag_ref[3 + c] + picked[4][c] - picked[2][c] for c in range(3)]
    normal = [
        first[(c + 1) % 3] * second[(c + 2) % 3] - first[(c + 2) % 3] * second[(c + 1) % 3]
        for c in range(3)
    ]
    gap = gap_ref[...]
    for c in range(3):
        centre = (picked[1][c] + picked[2][c] + picked[3][c] + picked[4][c]) * 0.25
        gap = gap + (slave[c] - centre) * normal[c]
    push = stiff_ref[...] * jnp.maximum(-gap, 0.0)
    rows_ref[...] = jnp.zeros(rows_ref.shape, jnp.float32)
    for c in range(3):
        force = push * normal[c]
        for r in range(force.shape[0]):
            rows_ref[c : c + 1, r * LANES : (r + 1) * LANES] = force[r : r + 1]
    got = contract_lanes(three_parts(rows_ref[...]), matrix_ref[...])
    got = got[0:8] + got[8:16] + got[16:24]
    for b in range(blocks):
        for q in range(pack):
            out_ref[b * pack + q] = got[:, b * LANES : (b + 1) * LANES]


def pack_body(u_ref, v_ref, stress_ref, hour_ref, xdn, xup, ydn, yup, cdd, cud, cdu, cuu):
    planes, columns = u_ref.shape[1:3]
    for c in range(13):
        if c < 3:
            ref = u_ref.at[c]
        elif c < 6:
            ref = v_ref.at[c - 3]
        elif c < 12:
            ref = stress_ref.at[c - 6]
        else:
            ref = hour_ref
        last = ref[planes - 1]
        right = ref[:, columns - 1, :]
        xup[c] = last
        yup[c] = right
        cuu[c : c + 1, :] = last[columns - 1 : columns]
        if c < 6:
            first = ref[0]
            xdn[c] = first
            ydn[c] = ref[:, 0, :]
            cdd[c : c + 1, :] = first[0:1]
            cud[c : c + 1, :] = last[0:1]
            cdu[c : c + 1, :] = first[columns - 1 : columns]


def split(value):
    return jnp.stack([value[:, at : at + LANES] for at in range(0, value.shape[1], LANES)])


def z_pair(f):
    lane = lax.broadcasted_iota(jnp.int32, f.shape, 2)
    turned = pltpu.roll(f, LANES - 1, 2)
    after = jnp.concatenate([turned[1:], turned[:1]], 0)
    upper = jnp.where(lane == LANES - 1, after, turned)
    return f + upper, upper - f


def node_terms(sums, diffs, sums_next, diffs_next):
    result = []
    for c in range(6):
        s0, s1, d0, d1 = sums[c], sums_next[c], diffs[c], diffs_next[c]
        if c < 3:
            result.append((s0 + s1, s1 - s0, d0 + d1))
        else:
            result.append((d1 - d0, d0 + d1, s1 - s0))
    return result


def element_terms(lower, upper, stress, hour):
    eight = []
    for m in range(3):
        row = [
            upper[m][0] - lower[m][0],
            lower[m][1] + upper[m][1],
            lower[m][2] + upper[m][2],
        ]
        row[m] = row[m] + 4.0
        eight.append(row)
    cof = [
        [
            eight[(m + 1) % 3][(n + 1) % 3] * eight[(m + 2) % 3][(n + 2) % 3]
            - eight[(m + 1) % 3][(n + 2) % 3] * eight[(m + 2) % 3][(n + 1) % 3]
            for n in range(3)
        ]
        for m in range(3)
    ]
    hour = hour * 64.0
    result = []
    for m in range(3):
        line = [
            stress[VOIGT[m][0]] * cof[0][n]
            + stress[VOIGT[m][1]] * cof[1][n]
            + stress[VOIGT[m][2]] * cof[2][n]
            for n in range(3)
        ]
        low, up = lower[3 + m], upper[3 + m]
        line.append(hour * (low[0] + up[0]))
        line.append(hour * (up[1] - low[1]))
        line.append(hour * (up[2] - low[2]))
        line.append(hour * (up[0] - low[0]))
        result.append(line)
    return result


def gathered_x(before, after):
    result = []
    for m in range(3):
        p, n = before[m], after[m]
        result.append(
            (
                p[0] - n[0],
                (p[1] + n[1]) + (p[5] - n[5]),
                (p[2] + n[2]) + (p[4] - n[4]),
                (p[3] + n[3]) + (p[6] - n[6]),
            )
        )
    return result


def element_body(
    u_ref, v_ref, stress_ref, hour_ref, mass_ref, ydn, xu, xd, yu, yd, cpp, cmp_, cpm, cmm,
    out_ref, row_ref, halo_s, halo_d, edge_ref, node_ref, elem_ref,
):
    planes, columns, depth = u_ref.shape[1:]
    nb = depth // LANES
    rows = row_ref.shape[1]
    def assembled(first, middle, last):
        row_ref[0, 0:1, :] = first
        row_ref[0, 1 : planes + 1, :] = middle
        if last is not None:
            row_ref[0, planes + 1 : planes + 2, :] = last
        return split(row_ref[0])

    row_ref[...] = jnp.zeros(row_ref.shape, jnp.float32)
    left_s, left_d, mid_s, mid_d = [], [], [], []
    for c in range(6):
        right = assembled(cmp_[c : c + 1, :], yu[c], cpp[c : c + 1, :])
        s, d = z_pair(right)
        halo_s[c] = s
        halo_d[c] = d
        s, d = z_pair(assembled(cmm[c : c + 1, :], yd[c], cpm[c : c + 1, :]))
        left_s.append(s)
        left_d.append(d)
        s, d = z_pair(assembled(xd[c, 0:1, :], ydn[c], xu[c, 0:1, :]))
        mid_s.append(s)
        mid_d.append(d)
    side = node_terms(left_s, left_d, mid_s, mid_d)
    stress = [assembled(cmm[6 + c : 7 + c, :], yd[6 + c], None) for c in range(6)]
    hour = assembled(cmm[12:13, :], yd[12], None)
    above = [tuple(pltpu.roll(q, rows - 1, 1) for q in terms) for terms in side]
    factors = element_terms(side, above, stress, hour)
    below = factors
    upper = [[pltpu.roll(q, rows - 1, 1) for q in line] for line in factors]
    for m, (a, b, c, e) in enumerate(gathered_x(below, upper)):
        edge_ref[m, 0] = a + b
        edge_ref[m, 1] = c + e

    row = lax.broadcasted_iota(jnp.int32, (nb, columns, LANES), 1)
    lane = lax.broadcasted_iota(jnp.int32, (nb, columns, LANES), 2)
    block = lax.broadcasted_iota(jnp.int32, (nb, columns, LANES), 0)

    def node_plane(values, at):
        sums, diffs, sums_next, diffs_next = [], [], [], []
        for c in range(6):
            s, d = z_pair(values[c])
            sums.append(s)
            diffs.append(d)
            hs = halo_s[c, :, pl.ds(at, 1), :]
            hd = halo_d[c, :, pl.ds(at, 1), :]
            sums_next.append(jnp.where(row == columns - 1, hs, pltpu.roll(s, columns - 1, 1)))
            diffs_next.append(jnp.where(row == columns - 1, hd, pltpu.roll(d, columns - 1, 1)))
        return node_terms(sums, diffs, sums_next, diffs_next)

    def keep_nodes(terms):
        for c in range(6):
            for t in range(3):
                node_ref[c, t] = terms[c][t]

    def kept_nodes():
        return [tuple(node_ref[c, t] for t in range(3)) for c in range(6)]

    def keep_elements(factors):
        for m in range(3):
            for t in range(7):
                elem_ref[m, t] = factors[m][t]

    def kept_elements():
        return [[elem_ref[m, t] for t in range(7)] for m in range(3)]

    def write_plane(before, after, i):
        weight = (time_step / 64.0) / split(mass_ref[i])
        for m, (a, b, c, e) in enumerate(gathered_x(before, after)):
            ab = edge_ref[m, 0, :, pl.ds(i, 1), :]
            ce = edge_ref[m, 1, :, pl.ds(i, 1), :]
            p = (a - b) + jnp.where(row == 0, ab, pltpu.roll(a + b, 1, 1))
            r = (c - e) + jnp.where(row == 0, ce, pltpu.roll(c + e, 1, 1))
            up = pltpu.roll(p + r, 1, 2)
            before_up = jnp.concatenate([jnp.zeros_like(up[:1]), up[:-1]], 0)
            force = jnp.where(lane == 0, before_up, up)
            last = (lane == LANES - 1) & (block == nb - 1)
            force = force + jnp.where(last, 0.0, p - r)
            result = split(v_ref[m, i]) - force * weight
            for k in range(nb):
                out_ref[m, i, :, k * LANES : (k + 1) * LANES] = result[k]

    def own_nodes(i):
        return [split(u_ref[c, i]) for c in range(3)] + [split(v_ref[c, i]) for c in range(3)]

    keep_nodes(node_plane([split(xd[c]) for c in range(6)], 0))
    current = node_plane(own_nodes(0), 1)
    keep_elements(
        element_terms(
            kept_nodes(), current, [split(xd[6 + c]) for c in range(6)], split(xd[12])
        )
    )
    keep_nodes(current)

    def step(i, upper):
        factors = element_terms(
            kept_nodes(), upper, [split(stress_ref[c, i - 1]) for c in range(6)], split(hour_ref[i - 1])
        )
        write_plane(kept_elements(), factors, i - 1)
        keep_elements(factors)
        keep_nodes(upper)

    def loop(i, carry):
        step(i, node_plane(own_nodes(i), i + 1))
        return carry

    lax.fori_loop(1, planes, loop, 0)
    step(planes, node_plane([split(xu[c]) for c in range(6)], planes + 1))


def final_body(nspace, capacity, pack, base_ref, mass_ref, table_ref, route_ref, out_ref, rows_ref):
    planes, columns, depth = base_ref.shape[1:]
    side = planes * columns
    offset = (lax.axis_index("space") % pack) * capacity
    (contact,) = looked_up(table_ref, [route_ref[...]], capacity, offset, nspace)
    rows_ref[...] = jnp.zeros(rows_ref.shape, jnp.float32)
    lane = lax.broadcasted_iota(jnp.int32, (planes, columns, LANES), 2)
    low_weight = jnp.where(lane == 0, time_step / mass_ref[:, :, 0:LANES], 0.0)
    high_weight = jnp.where(
        lane == LANES - 1, time_step / mass_ref[:, :, depth - LANES : depth], 0.0
    )
    for m in range(3):
        rows_ref[0:1, :] = contact[m][0:1]
        rows_ref[LANES - 1 : LANES, :] = contact[m][1:2]
        turned = rows_ref[...].T.reshape(planes, columns, LANES)
        for k in range(0, depth, LANES):
            value = base_ref[m, :, :, k : k + LANES]
            if k == 0:
                value = value + low_weight * turned
            if k == depth - LANES:
                value = value + high_weight * turned
            out_ref[m, :, :, k : k + LANES] = value


def local(
    displacement,
    velocity,
    stress,
    hourglass,
    mass,
    contact_route,
    pair_nodes,
    pair_diagonals,
    pair_gap,
    pair_stiffness,
):
    planes, columns, depth = displacement.shape[1:]
    nspace = lax.axis_size("space")
    surf_count = 2 * planes * columns
    pairs = pair_nodes.shape[1]
    capacity, pack, blocks = layout(nspace, surf_count)
    f32 = jnp.float32
    message = jax.ShapeDtypeStruct((nspace, 8, LANES), f32)

    outgoing = kernel_call(
        functools.partial(route_body, nspace, capacity, pack, blocks),
        message,
        [pltpu.VMEM((8, surf_count), f32)],
    )(displacement, contact_route.reshape(1, surf_count))
    received = lax.all_to_all(outgoing, "space", split_axis=0, concat_axis=0, tiled=True)

    def sized(*shape):
        return jax.ShapeDtypeStruct(shape, f32)

    xdn, xup, ydn, yup, cdd, cud, cdu, cuu = kernel_call(
        pack_body,
        (
            sized(6, columns, depth),
            sized(13, columns, depth),
            sized(6, planes, depth),
            sized(13, planes, depth),
            sized(6, depth),
            sized(6, depth),
            sized(6, depth),
            sized(13, depth),
        ),
    )(displacement, velocity, stress, hourglass)
    yu = moved(ydn, 0, -1)
    yd = moved(yup, 0, 1)
    xu = moved(xdn, -1, 0)
    xd = moved(xup, 1, 0)
    cpp = moved(cdd, -1, -1)
    cmp_ = moved(cud, 1, -1)
    cpm = moved(cdu, -1, 1)
    cmm = moved(cuu, 1, 1)

    matrix = kernel_call(
        functools.partial(matrix_body, capacity, pack, blocks),
        jax.ShapeDtypeStruct((blocks * LANES, pairs), jnp.bfloat16),
    )(pair_nodes)
    slot_force = kernel_call(
        functools.partial(pair_body, nspace, capacity, pack, blocks),
        message,
        [pltpu.VMEM((8, pairs), f32)],
    )(
        received,
        pair_nodes.reshape(5, pairs // LANES, LANES),
        pair_diagonals.reshape(6, pairs // LANES, LANES),
        pair_gap.reshape(pairs // LANES, LANES),
        pair_stiffness.reshape(pairs // LANES, LANES),
        matrix,
    )
    returned = lax.all_to_all(slot_force, "space", split_axis=0, concat_axis=0, tiled=True)

    nb = depth // LANES
    rows = (planes + 2 + 7) // 8 * 8
    base = kernel_call(
        element_body,
        jax.ShapeDtypeStruct(displacement.shape, f32),
        [
            pltpu.VMEM((1, rows, depth), f32),
            pltpu.VMEM((6, nb, rows, LANES), f32),
            pltpu.VMEM((6, nb, rows, LANES), f32),
            pltpu.VMEM((3, 2, nb, rows, LANES), f32),
            pltpu.VMEM((6, 3, nb, columns, LANES), f32),
            pltpu.VMEM((3, 7, nb, columns, LANES), f32),
        ],
    )(displacement, velocity, stress, hourglass, mass, ydn, xu, xd, yu, yd, cpp, cmp_, cpm, cmm)

    return kernel_call(
        functools.partial(final_body, nspace, capacity, pack),
        jax.ShapeDtypeStruct(displacement.shape, f32),
        [pltpu.VMEM((LANES, LANES), f32)],
    )(base, mass, returned, contact_route.reshape(2, surf_count // 2))


def solution(mesh):
    in_specs = (
        P(None, "space", "slab", None),
        P(None, "space", "slab", None),
        P(None, "space", "slab", None),
        P("space", "slab", None),
        P("space", "slab", None),
        P(("space", "slab")),
        P(None, ("space", "slab")),
        P(None, ("space", "slab")),
        P(("space", "slab")),
        P(("space", "slab")),
    )
    out_specs = P(None, "space", "slab", None)
    return jax.shard_map(local, mesh=mesh, in_specs=in_specs, out_specs=out_specs, check_vma=False)
```

```python
import functools

import jax
import jax.numpy as jnp
from jax import lax
from jax.experimental import pallas as pl
from jax.experimental.pallas import tpu as pltpu
from jax.sharding import PartitionSpec as P

time_step = 0.5
LANES = 128
VOIGT = [[0, 5, 4], [5, 1, 3], [4, 3, 2]]


def shifted(value, axis, steps):
    count = lax.axis_size(axis)
    return lax.ppermute(value, axis, [(at, (at + steps) % count) for at in range(count)])


def kernel_call(body, inputs, outs, scratch=(), out_specs=None):
    vmem = pl.BlockSpec(memory_space=pltpu.VMEM)
    if out_specs is None:
        out_specs = jax.tree.map(lambda _: vmem, outs)
    return pl.pallas_call(
        body,
        out_shape=outs,
        in_specs=[vmem] * len(inputs),
        out_specs=out_specs,
        scratch_shapes=list(scratch),
    )(*inputs)


def contract_lanes(lhs, rhs):
    return lax.dot_general(lhs, rhs, (((1,), (1,)), ((), ())), preferred_element_type=jnp.float32)


def layout(nspace, surf_count):
    capacity = max(2, (3 * surf_count // 2 + nspace - 1) // nspace)
    pack = max(1, min(LANES // capacity, nspace // 8))
    while nspace % pack:
        pack -= 1
    return capacity, pack, nspace // pack


def block_of(slots, width, blocks):
    block = jnp.zeros_like(slots)
    for b in range(1, blocks):
        block = block + jnp.where(slots >= b * width, 1, 0)
    return block, slots - block * width


def parts_of(rows):
    high = rows.astype(jnp.bfloat16).astype(jnp.float32)
    rest = rows - high
    middle = rest.astype(jnp.bfloat16).astype(jnp.float32)
    return [high, middle, rest - middle]


def places(place, width):
    rows = (width + 15) // 16 * 16
    count = place.shape[1]
    at = lax.broadcasted_iota(jnp.int32, (rows, count), 0)
    return jnp.where(at == place, 1.0, 0.0).astype(jnp.bfloat16)


def spread(parts, block, blocks):
    return [
        jnp.where(block == b, part, 0.0).astype(jnp.bfloat16)
        for part in parts
        for b in range(blocks)
    ]


def write_messages(out_ref, got, pack, blocks, width):
    for b in range(blocks):
        at = [(part * blocks + b) * 8 for part in range(3)]
        total = got[at[0] : at[0] + 8] + got[at[1] : at[1] + 8] + got[at[2] : at[2] + 8]
        for q in range(pack):
            out_ref[b * pack + q, :, 0 : total.shape[1]] = total


def first_body(
    capacity, pack, blocks, u_ref, v_ref, stress_ref, hour_ref, route_ref, out_ref, ydn, yup, rows_ref
):
    planes, columns, depth = u_ref.shape[1:]
    side = planes * columns
    lane = lax.broadcasted_iota(jnp.int32, (side, LANES), 1)
    rows_ref[...] = jnp.zeros(rows_ref.shape, jnp.float32)
    for c in range(3):
        bottom = u_ref[c, :, :, 0:LANES].reshape(side, LANES)
        top = u_ref[c, :, :, depth - LANES : depth].reshape(side, LANES)
        both = jnp.where(lane == LANES - 1, top, bottom).T
        rows_ref[c : c + 1, 0:side] = both[0:1]
        rows_ref[c : c + 1, side : 2 * side] = both[LANES - 1 : LANES]
    width = pack * capacity
    block, place = block_of(route_ref[...], width, blocks)
    entries = spread(parts_of(rows_ref[...]), block, blocks)
    out_ref[...] = jnp.zeros(out_ref.shape, jnp.float32)
    got = contract_lanes(jnp.concatenate(entries, 0), places(place, width))
    write_messages(out_ref, got, pack, blocks, width)
    for c in range(13):
        ref = component(u_ref, v_ref, stress_ref, hour_ref, c)
        yup[c] = ref[:, columns - 1, :]
        if c < 6:
            ydn[c] = ref[:, 0, :]


def component(u_ref, v_ref, stress_ref, hour_ref, c):
    if c < 3:
        return u_ref.at[c]
    if c < 6:
        return v_ref.at[c - 3]
    if c < 12:
        return stress_ref.at[c - 6]
    return hour_ref


def second_body(u_ref, v_ref, stress_ref, hour_ref, yu, yd, xdn, xup):
    planes, columns = u_ref.shape[1:3]
    base = 13 * columns
    for c in range(13):
        ref = component(u_ref, v_ref, stress_ref, hour_ref, c)
        xup[c * columns : (c + 1) * columns, :] = ref[planes - 1]
        xup[base + c : base + c + 1, :] = yd[c, planes - 1 : planes, :]
    for c in range(6):
        ref = component(u_ref, v_ref, stress_ref, hour_ref, c)
        xup[base + 13 + c : base + 14 + c, :] = yu[c, planes - 1 : planes, :]
        xdn[c * columns : (c + 1) * columns, :] = ref[0]
        at = 6 * columns + c
        xdn[at : at + 1, :] = yd[c, 0:1, :]
        xdn[at + 6 : at + 7, :] = yu[c, 0:1, :]


def places_body(width, blocks, nodes_ref, place_ref, block_ref):
    pairs = nodes_ref.shape[1]
    for j in range(5):
        block, place = block_of(nodes_ref[j : j + 1, :], width, blocks)
        block_ref[j : j + 1, :] = block
        place_ref[:, j * pairs : (j + 1) * pairs] = places(place, width)


def looked_up(table_ref, slots, capacity, offset, count):
    shape = slots[0].shape

    def step(s, found):
        shift = s * capacity - offset
        result = []
        for slot, old in zip(slots, found):
            here = (slot >= s * capacity) & (slot < (s + 1) * capacity)
            index = (slot - shift) & (LANES - 1)
            new = []
            for c in range(3):
                row = jnp.broadcast_to(table_ref[s, c : c + 1, :], shape)
                new.append(jnp.where(here, jnp.take_along_axis(row, index, axis=1), old[c]))
            result.append(tuple(new))
        return tuple(result)

    zero = jnp.zeros(shape, jnp.float32)
    found = tuple((zero, zero, zero) for _ in slots)
    if count <= 16:
        for s in range(count):
            found = step(s, found)
        return found
    return lax.fori_loop(0, count, step, found)


def pair_body(
    nspace, capacity, pack, blocks, table_ref, nodes_ref, diag_ref, gap_ref, stiff_ref, place_ref,
    block_ref, out_ref, rows_ref, entry_ref,
):
    offset = (lax.axis_index("space") % pack) * capacity
    picked = looked_up(table_ref, [nodes_ref[j] for j in range(5)], capacity, offset, nspace)
    slave = picked[0]
    first = [diag_ref[c] + picked[3][c] - picked[1][c] for c in range(3)]
    second = [diag_ref[3 + c] + picked[4][c] - picked[2][c] for c in range(3)]
    normal = [
        first[(c + 1) % 3] * second[(c + 2) % 3] - first[(c + 2) % 3] * second[(c + 1) % 3]
        for c in range(3)
    ]
    gap = gap_ref[...]
    for c in range(3):
        centre = (picked[1][c] + picked[2][c] + picked[3][c] + picked[4][c]) * 0.25
        gap = gap + (slave[c] - centre) * normal[c]
    push = stiff_ref[...] * jnp.maximum(-gap, 0.0)
    pairs = rows_ref.shape[1]
    rows_ref[...] = jnp.zeros(rows_ref.shape, jnp.float32)
    for c in range(3):
        force = push * normal[c]
        for r in range(force.shape[0]):
            rows_ref[c : c + 1, r * LANES : (r + 1) * LANES] = force[r : r + 1]
    parts = parts_of(rows_ref[...])
    fourth = [part * -0.25 for part in parts]
    for j in range(5):
        entries = spread(fourth if j else parts, block_ref[j : j + 1, :], blocks)
        entry_ref[:, j * pairs : (j + 1) * pairs] = jnp.concatenate(entries, 0)
    width = pack * capacity
    out_ref[...] = jnp.zeros(out_ref.shape, jnp.float32)
    got = contract_lanes(entry_ref[...], place_ref[...])
    write_messages(out_ref, got, pack, blocks, width)


def split(value):
    return jnp.stack([value[:, at : at + LANES] for at in range(0, value.shape[1], LANES)])


def z_pair(f):
    lane = lax.broadcasted_iota(jnp.int32, f.shape, 2)
    turned = pltpu.roll(f, LANES - 1, 2)
    after = jnp.concatenate([turned[1:], turned[:1]], 0)
    upper = jnp.where(lane == LANES - 1, after, turned)
    return f + upper, upper - f


def node_terms(sums, diffs, sums_next, diffs_next):
    result = []
    for c in range(6):
        s0, s1, d0, d1 = sums[c], sums_next[c], diffs[c], diffs_next[c]
        if c < 3:
            result.append((s0 + s1, s1 - s0, d0 + d1))
        else:
            result.append((d1 - d0, d0 + d1, s1 - s0))
    return result


def element_terms(lower, upper, stress, hour):
    eight = []
    for m in range(3):
        row = [
            upper[m][0] - lower[m][0],
            lower[m][1] + upper[m][1],
            lower[m][2] + upper[m][2],
        ]
        row[m] = row[m] + 4.0
        eight.append(row)
    cof = [
        [
            eight[(m + 1) % 3][(n + 1) % 3] * eight[(m + 2) % 3][(n + 2) % 3]
            - eight[(m + 1) % 3][(n + 2) % 3] * eight[(m + 2) % 3][(n + 1) % 3]
            for n in range(3)
        ]
        for m in range(3)
    ]
    hour = hour * 64.0
    result = []
    for m in range(3):
        line = [
            stress[VOIGT[m][0]] * cof[0][n]
            + stress[VOIGT[m][1]] * cof[1][n]
            + stress[VOIGT[m][2]] * cof[2][n]
            for n in range(3)
        ]
        low, up = lower[3 + m], upper[3 + m]
        line.append(hour * (low[0] + up[0]))
        line.append(hour * (up[1] - low[1]))
        line.append(hour * (up[2] - low[2]))
        line.append(hour * (up[0] - low[0]))
        result.append(line)
    return result


def gathered_x(before, after):
    result = []
    for m in range(3):
        p, n = before[m], after[m]
        result.append(
            (
                p[0] - n[0],
                (p[1] + n[1]) + (p[5] - n[5]),
                (p[2] + n[2]) + (p[4] - n[4]),
                (p[3] + n[3]) + (p[6] - n[6]),
            )
        )
    return result


def element_body(
    u_ref, v_ref, stress_ref, hour_ref, mass_ref, ydn, yu, yd, xu, xd,
    out_ref, row_ref, halo_s, halo_d, edge_ref, node_ref, elem_ref,
):
    planes, columns, depth = u_ref.shape[1:]
    nb = depth // LANES
    rows = row_ref.shape[0]

    def below(c):
        return xd[c * columns : (c + 1) * columns, :]

    def above(c):
        return xu[c * columns : (c + 1) * columns, :]

    def assembled(first, middle, last):
        row_ref[0:1, :] = first
        row_ref[1 : planes + 1, :] = middle
        if last is not None:
            row_ref[planes + 1 : planes + 2, :] = last
        return split(row_ref[...])

    def line(ref, at):
        return ref[at : at + 1, :]

    row_ref[...] = jnp.zeros(row_ref.shape, jnp.float32)
    base = 13 * columns
    left_s, left_d, mid_s, mid_d = [], [], [], []
    for c in range(6):
        right = assembled(line(xd, base + 13 + c), yu[c], line(xu, 6 * columns + 6 + c))
        s, d = z_pair(right)
        halo_s[c] = s
        halo_d[c] = d
        s, d = z_pair(assembled(line(xd, base + c), yd[c], line(xu, 6 * columns + c)))
        left_s.append(s)
        left_d.append(d)
        s, d = z_pair(assembled(line(xd, c * columns), ydn[c], line(xu, c * columns)))
        mid_s.append(s)
        mid_d.append(d)
    side = node_terms(left_s, left_d, mid_s, mid_d)
    stress = [assembled(line(xd, base + 6 + c), yd[6 + c], None) for c in range(6)]
    hour = assembled(line(xd, base + 12), yd[12], None)
    next_side = [tuple(pltpu.roll(q, rows - 1, 1) for q in terms) for terms in side]
    factors = element_terms(side, next_side, stress, hour)
    upper = [[pltpu.roll(q, rows - 1, 1) for q in terms] for terms in factors]
    for m, (a, b, c, e) in enumerate(gathered_x(factors, upper)):
        edge_ref[m, 0] = a + b
        edge_ref[m, 1] = c + e

    row = lax.broadcasted_iota(jnp.int32, (nb, columns, LANES), 1)
    lane = lax.broadcasted_iota(jnp.int32, (nb, columns, LANES), 2)
    block = lax.broadcasted_iota(jnp.int32, (nb, columns, LANES), 0)

    def node_plane(values, at):
        sums, diffs, sums_next, diffs_next = [], [], [], []
        for c in range(6):
            s, d = z_pair(values[c])
            sums.append(s)
            diffs.append(d)
            hs = halo_s[c, :, pl.ds(at, 1), :]
            hd = halo_d[c, :, pl.ds(at, 1), :]
            sums_next.append(jnp.where(row == columns - 1, hs, pltpu.roll(s, columns - 1, 1)))
            diffs_next.append(jnp.where(row == columns - 1, hd, pltpu.roll(d, columns - 1, 1)))
        return node_terms(sums, diffs, sums_next, diffs_next)

    def keep_nodes(terms):
        for c in range(6):
            for t in range(3):
                node_ref[c, t] = terms[c][t]

    def kept_nodes():
        return [tuple(node_ref[c, t] for t in range(3)) for c in range(6)]

    def keep_elements(factors):
        for m in range(3):
            for t in range(7):
                elem_ref[m, t] = factors[m][t]

    def kept_elements():
        return [[elem_ref[m, t] for t in range(7)] for m in range(3)]

    def write_plane(before, after, i):
        weight = (time_step / 64.0) / split(mass_ref[i])
        for m, (a, b, c, e) in enumerate(gathered_x(before, after)):
            ab = edge_ref[m, 0, :, pl.ds(i, 1), :]
            ce = edge_ref[m, 1, :, pl.ds(i, 1), :]
            p = (a - b) + jnp.where(row == 0, ab, pltpu.roll(a + b, 1, 1))
            r = (c - e) + jnp.where(row == 0, ce, pltpu.roll(c + e, 1, 1))
            up = pltpu.roll(p + r, 1, 2)
            before_up = jnp.concatenate([jnp.zeros_like(up[:1]), up[:-1]], 0)
            force = jnp.where(lane == 0, before_up, up)
            last = (lane == LANES - 1) & (block == nb - 1)
            force = force + jnp.where(last, 0.0, p - r)
            result = split(v_ref[m, i]) - force * weight
            for k in range(nb):
                out_ref[m, i, :, k * LANES : (k + 1) * LANES] = result[k]

    def own_nodes(i):
        return [split(u_ref[c, i]) for c in range(3)] + [split(v_ref[c, i]) for c in range(3)]

    keep_nodes(node_plane([split(below(c)) for c in range(6)], 0))
    current = node_plane(own_nodes(0), 1)
    keep_elements(
        element_terms(
            kept_nodes(), current, [split(below(6 + c)) for c in range(6)], split(below(12))
        )
    )
    keep_nodes(current)

    def step(i, upper):
        factors = element_terms(
            kept_nodes(), upper, [split(stress_ref[c, i - 1]) for c in range(6)], split(hour_ref[i - 1])
        )
        write_plane(kept_elements(), factors, i - 1)
        keep_elements(factors)
        keep_nodes(upper)

    def loop(i, carry):
        step(i, node_plane(own_nodes(i), i + 1))
        return carry

    lax.fori_loop(1, planes, loop, 0)
    step(planes, node_plane([split(above(c)) for c in range(6)], planes + 1))


def final_body(nspace, capacity, pack, base_ref, mass_ref, table_ref, route_ref, out_ref, rows_ref):
    planes, columns, depth = base_ref.shape[1:]
    side = planes * columns
    offset = (lax.axis_index("space") % pack) * capacity
    (contact,) = looked_up(table_ref, [route_ref[...]], capacity, offset, nspace)
    rows_ref[...] = jnp.zeros(rows_ref.shape, jnp.float32)
    lane = lax.broadcasted_iota(jnp.int32, (planes, columns, LANES), 2)
    low_weight = jnp.where(lane == 0, time_step / mass_ref[:, :, 0:LANES], 0.0)
    high_weight = jnp.where(
        lane == LANES - 1, time_step / mass_ref[:, :, depth - LANES : depth], 0.0
    )
    for m in range(3):
        rows_ref[0:1, :] = contact[m][0:1]
        rows_ref[LANES - 1 : LANES, :] = contact[m][1:2]
        turned = rows_ref[...].T.reshape(planes, columns, LANES)
        for k in range(0, depth, LANES):
            value = base_ref[m, :, :, k : k + LANES]
            if k == 0:
                value = value + low_weight * turned
            if k == depth - LANES:
                value = value + high_weight * turned
            out_ref[m, :, :, k : k + LANES] = value


def local(
    displacement,
    velocity,
    stress,
    hourglass,
    mass,
    contact_route,
    pair_nodes,
    pair_diagonals,
    pair_gap,
    pair_stiffness,
):
    planes, columns, depth = displacement.shape[1:]
    nspace = lax.axis_size("space")
    surf_count = 2 * planes * columns
    pairs = pair_nodes.shape[1]
    capacity, pack, blocks = layout(nspace, surf_count)
    f32 = jnp.float32
    lines = pairs // LANES

    def sized(*shape):
        return jax.ShapeDtypeStruct(shape, f32)

    def exchanged(value):
        return lax.all_to_all(value, "space", split_axis=0, concat_axis=0, tiled=True)

    message = sized(nspace, 8, LANES)
    width = pack * capacity
    place, block = kernel_call(
        functools.partial(places_body, width, blocks),
        (pair_nodes,),
        (
            jax.ShapeDtypeStruct(((width + 15) // 16 * 16, 5 * pairs), jnp.bfloat16),
            jax.ShapeDtypeStruct((5, pairs), jnp.int32),
        ),
    )
    outgoing, ydn, yup = kernel_call(
        functools.partial(first_body, capacity, pack, blocks),
        (displacement, velocity, stress, hourglass, contact_route.reshape(1, surf_count)),
        (message, sized(6, planes, depth), sized(13, planes, depth)),
        [pltpu.VMEM((8, surf_count), f32)],
    )
    yu = shifted(ydn, "slab", -1)
    yd = shifted(yup, "slab", 1)
    received = exchanged(outgoing)
    xdn, xup = kernel_call(
        second_body,
        (displacement, velocity, stress, hourglass, yu, yd),
        (
            sized((6 * columns + 12 + 7) // 8 * 8, depth),
            sized((13 * columns + 19 + 7) // 8 * 8, depth),
        ),
    )
    xu = shifted(xdn, "space", -1)
    xd = shifted(xup, "space", 1)
    slot_force = kernel_call(
        functools.partial(pair_body, nspace, capacity, pack, blocks),
        (
            received,
            pair_nodes.reshape(5, lines, LANES),
            pair_diagonals.reshape(6, lines, LANES),
            pair_gap.reshape(lines, LANES),
            pair_stiffness.reshape(lines, LANES),
            place,
            block,
        ),
        message,
        [pltpu.VMEM((8, pairs), f32), pltpu.VMEM((24 * blocks, 5 * pairs), jnp.bfloat16)],
    )
    returned = exchanged(slot_force)

    nb = depth // LANES
    rows = (planes + 2 + 7) // 8 * 8
    base = kernel_call(
        element_body,
        (displacement, velocity, stress, hourglass, mass, ydn, yu, yd, xu, xd),
        sized(*displacement.shape),
        [
            pltpu.VMEM((rows, depth), f32),
            pltpu.VMEM((6, nb, rows, LANES), f32),
            pltpu.VMEM((6, nb, rows, LANES), f32),
            pltpu.VMEM((3, 2, nb, rows, LANES), f32),
            pltpu.VMEM((6, 3, nb, columns, LANES), f32),
            pltpu.VMEM((3, 7, nb, columns, LANES), f32),
        ],
    )

    return kernel_call(
        functools.partial(final_body, nspace, capacity, pack),
        (base, mass, returned, contact_route.reshape(2, surf_count // 2)),
        sized(*displacement.shape),
        [pltpu.VMEM((LANES, LANES), f32)],
        pl.BlockSpec(),
    )


def solution(mesh):
    in_specs = (
        P(None, "space", "slab", None),
        P(None, "space", "slab", None),
        P(None, "space", "slab", None),
        P("space", "slab", None),
        P("space", "slab", None),
        P(("space", "slab")),
        P(None, ("space", "slab")),
        P(None, ("space", "slab")),
        P(("space", "slab")),
        P(("space", "slab")),
    )
    out_specs = P(None, "space", "slab", None)
    return jax.shard_map(local, mesh=mesh, in_specs=in_specs, out_specs=out_specs, check_vma=False)
```

```python
import functools

import jax
import jax.numpy as jnp
from jax import lax
from jax.experimental import pallas as pl
from jax.experimental.pallas import tpu as pltpu
from jax.sharding import PartitionSpec as P


time_step = 0.5
LANES = 128
VOIGT = [[0, 5, 4], [5, 1, 3], [4, 3, 2]]


def shifted(value, axis, steps):
    count = lax.axis_size(axis)
    return lax.ppermute(value, axis, [(at, (at + steps) % count) for at in range(count)])


def exchanged(value):
    return lax.all_to_all(value, "space", split_axis=0, concat_axis=0, tiled=True)


def kernel_call(body, inputs, outs, scratch=(), hbm_inputs=0, final=False):
    vmem = pl.BlockSpec(memory_space=pltpu.VMEM)
    hbm = pl.BlockSpec(memory_space=pltpu.HBM)
    spaces = [pltpu.HBM if at < hbm_inputs else pltpu.VMEM for at in range(len(inputs))]
    inputs = [pltpu.with_memory_space_constraint(*pair) for pair in zip(inputs, spaces)]
    space = pltpu.HBM if final else pltpu.VMEM
    return pl.pallas_call(
        body,
        out_shape=jax.tree.map(lambda out: space(out.shape, out.dtype), outs),
        in_specs=[pl.BlockSpec(memory_space=one) for one in spaces],
        out_specs=jax.tree.map(lambda _: hbm if final else vmem, outs),
        scratch_shapes=list(scratch),
        compiler_params=pltpu.CompilerParams(vmem_limit_bytes=16 << 20),
    )(*inputs)


def contract_lanes(lhs, rhs):
    return lax.dot_general(lhs, rhs, (((1,), (1,)), ((), ())), preferred_element_type=jnp.float32)


def layout(nspace, surf_count):
    capacity = max(2, (3 * surf_count // 2 + nspace - 1) // nspace)
    pack = max(1, min(LANES // capacity, nspace // 8))
    while nspace % pack:
        pack -= 1
    return capacity, pack, nspace // pack


def block_of(slots, width, blocks):
    block = jnp.zeros_like(slots)
    for b in range(1, blocks):
        block = block + jnp.where(slots >= b * width, 1, 0)
    return block, slots - block * width


def parts_of(rows):
    high = rows.astype(jnp.bfloat16).astype(jnp.float32)
    rest = rows - high
    middle = rest.astype(jnp.bfloat16).astype(jnp.float32)
    return [high, middle, rest - middle]


def places(place, width):
    rows = (width + 15) // 16 * 16
    count = place.shape[1]
    at = lax.broadcasted_iota(jnp.int32, (rows, count), 0)
    return jnp.where(at == place, 1.0, 0.0).astype(jnp.bfloat16)


def spread(parts, block, blocks):
    return [
        jnp.where(block == b, part, 0.0).astype(jnp.bfloat16)
        for part in parts
        for b in range(blocks)
    ]


def write_messages(out_ref, got, pack, blocks):
    for b in range(blocks):
        at = [(part * blocks + b) * 8 for part in range(3)]
        total = got[at[0] : at[0] + 8] + got[at[1] : at[1] + 8] + got[at[2] : at[2] + 8]
        for q in range(pack):
            out_ref[b * pack + q, :, 0 : total.shape[1]] = total


def first_body(
    capacity, pack, blocks, u_hbm, v_hbm, stress_hbm, hour_hbm, mass_hbm, route_hbm,
    out_ref, ydn, yup, sides_ref, u_ref, v_ref, stress_ref, hour_ref, mass_ref, rows_ref, route_ref, sems,
):
    copies = [
        pltpu.make_async_copy(source, target, sems.at[at])
        for at, (source, target) in enumerate(
            (
                (u_hbm, u_ref),
                (route_hbm, route_ref),
                (v_hbm, v_ref),
                (stress_hbm, stress_ref),
                (hour_hbm, hour_ref),
                (mass_hbm, mass_ref),
            )
        )
    ]
    for copy in copies:
        copy.start()
    out_ref[...] = jnp.zeros(out_ref.shape, jnp.float32)
    rows_ref[...] = jnp.zeros(rows_ref.shape, jnp.float32)
    copies[0].wait()
    copies[1].wait()
    planes, columns, depth = u_ref.shape[1:]
    side = planes * columns
    lane = lax.broadcasted_iota(jnp.int32, (side, LANES), 1)
    for c in range(3):
        bottom = u_ref[c, :, :, 0:LANES].reshape(side, LANES)
        top = u_ref[c, :, :, depth - LANES : depth].reshape(side, LANES)
        both = jnp.where(lane == LANES - 1, top, bottom).T
        rows_ref[c : c + 1, 0:side] = both[0:1]
        rows_ref[c : c + 1, side : 2 * side] = both[LANES - 1 : LANES]
    width = pack * capacity
    route = route_ref[...]
    sides_ref[0:1, :] = route[:, 0:side]
    sides_ref[1:2, :] = route[:, side : 2 * side]
    block, place = block_of(route, width, blocks)
    entries = spread(parts_of(rows_ref[...]), block, blocks)
    got = contract_lanes(jnp.concatenate(entries, 0), places(place, width))
    write_messages(out_ref, got, pack, blocks)
    for copy in copies[2:]:
        copy.wait()
    for c in range(13):
        ref = component(u_ref, v_ref, stress_ref, hour_ref, c)
        yup[c] = ref[:, columns - 1, :]
        if c < 6:
            ydn[c] = ref[:, 0, :]


def component(u_ref, v_ref, stress_ref, hour_ref, c):
    if c < 3:
        return u_ref.at[c]
    if c < 6:
        return v_ref.at[c - 3]
    if c < 12:
        return stress_ref.at[c - 6]
    return hour_ref


def second_body(u_ref, v_ref, stress_ref, hour_ref, yu, yd, xdn, xup):
    planes, columns = u_ref.shape[1:3]
    base = 13 * columns
    for c in range(13):
        ref = component(u_ref, v_ref, stress_ref, hour_ref, c)
        xup[c * columns : (c + 1) * columns, :] = ref[planes - 1]
        xup[base + c : base + c + 1, :] = yd[c, planes - 1 : planes, :]
    for c in range(6):
        ref = component(u_ref, v_ref, stress_ref, hour_ref, c)
        xup[base + 13 + c : base + 14 + c, :] = yu[c, planes - 1 : planes, :]
        xdn[c * columns : (c + 1) * columns, :] = ref[0]
        at = 6 * columns + c
        xdn[at : at + 1, :] = yd[c, 0:1, :]
        xdn[at + 6 : at + 7, :] = yu[c, 0:1, :]


def places_body(
    width, blocks, nodes_hbm, diag_hbm, gap_hbm, stiff_hbm,
    place_ref, block_ref, lines_ref, diag_lines_ref, gap_ref, stiff_ref, nodes_ref, diag_ref, sems,
):
    copies = [
        pltpu.make_async_copy(source, target, sems.at[at])
        for at, (source, target) in enumerate(
            (
                (nodes_hbm, nodes_ref),
                (diag_hbm, diag_ref),
                (gap_hbm, gap_ref),
                (stiff_hbm, stiff_ref),
            )
        )
    ]
    for copy in copies:
        copy.start()
    for copy in copies:
        copy.wait()
    pairs = nodes_ref.shape[1]
    for j in range(5):
        nodes = nodes_ref[j : j + 1, :]
        block, place = block_of(nodes, width, blocks)
        block_ref[j : j + 1, :] = block
        place_ref[:, j * pairs : (j + 1) * pairs] = places(place, width)
        for r in range(pairs // LANES):
            lines_ref[j, r : r + 1, :] = nodes[:, r * LANES : (r + 1) * LANES]
    for c in range(6):
        for r in range(pairs // LANES):
            diag_lines_ref[c, r : r + 1, :] = diag_ref[c : c + 1, r * LANES : (r + 1) * LANES]


def looked_up(table_ref, slots, capacity, offset, count):
    shape = slots[0].shape

    def step(s, found):
        shift = s * capacity - offset
        result = []
        for slot, old in zip(slots, found):
            here = (slot >= s * capacity) & (slot < (s + 1) * capacity)
            index = (slot - shift) & (LANES - 1)
            new = []
            for c in range(3):
                row = jnp.broadcast_to(table_ref[s, c : c + 1, :], shape)
                new.append(jnp.where(here, jnp.take_along_axis(row, index, axis=1), old[c]))
            result.append(tuple(new))
        return tuple(result)

    zero = jnp.zeros(shape, jnp.float32)
    found = tuple((zero, zero, zero) for _ in slots)
    if count <= 16:
        for s in range(count):
            found = step(s, found)
        return found
    return lax.fori_loop(0, count, step, found)


def pair_body(
    nspace, capacity, pack, blocks, table_ref, nodes_ref, diag_ref, gap_ref, stiff_ref, place_ref,
    block_ref, out_ref, rows_ref, entry_ref,
):
    offset = (lax.axis_index("space") % pack) * capacity
    picked = looked_up(table_ref, [nodes_ref[j] for j in range(5)], capacity, offset, nspace)
    slave = picked[0]
    first = [diag_ref[c] + picked[3][c] - picked[1][c] for c in range(3)]
    second = [diag_ref[3 + c] + picked[4][c] - picked[2][c] for c in range(3)]
    normal = [
        first[(c + 1) % 3] * second[(c + 2) % 3] - first[(c + 2) % 3] * second[(c + 1) % 3]
        for c in range(3)
    ]
    gap = gap_ref[...]
    for c in range(3):
        centre = (picked[1][c] + picked[2][c] + picked[3][c] + picked[4][c]) * 0.25
        gap = gap + (slave[c] - centre) * normal[c]
    push = stiff_ref[...] * jnp.maximum(-gap, 0.0)
    pairs = rows_ref.shape[1]
    rows_ref[...] = jnp.zeros(rows_ref.shape, jnp.float32)
    for c in range(3):
        force = push * normal[c]
        for r in range(force.shape[0]):
            rows_ref[c : c + 1, r * LANES : (r + 1) * LANES] = force[r : r + 1]
    parts = parts_of(rows_ref[...])
    fourth = [part * -0.25 for part in parts]
    for j in range(5):
        entries = spread(fourth if j else parts, block_ref[j : j + 1, :], blocks)
        entry_ref[:, j * pairs : (j + 1) * pairs] = jnp.concatenate(entries, 0)
    out_ref[...] = jnp.zeros(out_ref.shape, jnp.float32)
    got = contract_lanes(entry_ref[...], place_ref[...])
    write_messages(out_ref, got, pack, blocks)


def split(value):
    return jnp.stack([value[:, at : at + LANES] for at in range(0, value.shape[1], LANES)])


def z_pair(f):
    lane = lax.broadcasted_iota(jnp.int32, f.shape, 2)
    turned = pltpu.roll(f, LANES - 1, 2)
    after = jnp.concatenate([turned[1:], turned[:1]], 0)
    upper = jnp.where(lane == LANES - 1, after, turned)
    return f + upper, upper - f


def node_terms(sums, diffs, sums_next, diffs_next):
    result = []
    for c in range(6):
        s0, s1, d0, d1 = sums[c], sums_next[c], diffs[c], diffs_next[c]
        if c < 3:
            result.append((s0 + s1, s1 - s0, d0 + d1))
        else:
            result.append((d1 - d0, d0 + d1, s1 - s0))
    return result


def element_terms(lower, upper, stress, hour):
    eight = []
    for m in range(3):
        row = [
            upper[m][0] - lower[m][0],
            lower[m][1] + upper[m][1],
            lower[m][2] + upper[m][2],
        ]
        row[m] = row[m] + 4.0
        eight.append(row)
    cof = [
        [
            eight[(m + 1) % 3][(n + 1) % 3] * eight[(m + 2) % 3][(n + 2) % 3]
            - eight[(m + 1) % 3][(n + 2) % 3] * eight[(m + 2) % 3][(n + 1) % 3]
            for n in range(3)
        ]
        for m in range(3)
    ]
    hour = hour * 64.0
    result = []
    for m in range(3):
        line = [
            stress[VOIGT[m][0]] * cof[0][n]
            + stress[VOIGT[m][1]] * cof[1][n]
            + stress[VOIGT[m][2]] * cof[2][n]
            for n in range(3)
        ]
        low, up = lower[3 + m], upper[3 + m]
        line.append(hour * (low[0] + up[0]))
        line.append(hour * (up[1] - low[1]))
        line.append(hour * (up[2] - low[2]))
        line.append(hour * (up[0] - low[0]))
        result.append(line)
    return result


def gathered_x(before, after):
    result = []
    for m in range(3):
        p, n = before[m], after[m]
        result.append(
            (
                p[0] - n[0],
                (p[1] + n[1]) + (p[5] - n[5]),
                (p[2] + n[2]) + (p[4] - n[4]),
                (p[3] + n[3]) + (p[6] - n[6]),
            )
        )
    return result


def element_body(
    u_ref, v_ref, stress_ref, hour_ref, mass_ref, ydn, yu, yd, xu, xd,
    out_ref, row_ref, halo_s, halo_d, edge_ref, node_ref, elem_ref,
):
    planes, columns, depth = u_ref.shape[1:]
    nb = depth // LANES
    rows = row_ref.shape[0]

    def below(c):
        return xd[c * columns : (c + 1) * columns, :]

    def above(c):
        return xu[c * columns : (c + 1) * columns, :]

    def assembled(first, middle, last):
        row_ref[0:1, :] = first
        row_ref[1 : planes + 1, :] = middle
        if last is not None:
            row_ref[planes + 1 : planes + 2, :] = last
        return split(row_ref[...])

    def line(ref, at):
        return ref[at : at + 1, :]

    row_ref[...] = jnp.zeros(row_ref.shape, jnp.float32)
    base = 13 * columns
    left_s, left_d, mid_s, mid_d = [], [], [], []
    for c in range(6):
        right = assembled(line(xd, base + 13 + c), yu[c], line(xu, 6 * columns + 6 + c))
        s, d = z_pair(right)
        halo_s[c] = s
        halo_d[c] = d
        s, d = z_pair(assembled(line(xd, base + c), yd[c], line(xu, 6 * columns + c)))
        left_s.append(s)
        left_d.append(d)
        s, d = z_pair(assembled(line(xd, c * columns), ydn[c], line(xu, c * columns)))
        mid_s.append(s)
        mid_d.append(d)
    side = node_terms(left_s, left_d, mid_s, mid_d)
    stress = [assembled(line(xd, base + 6 + c), yd[6 + c], None) for c in range(6)]
    hour = assembled(line(xd, base + 12), yd[12], None)
    next_side = [tuple(pltpu.roll(q, rows - 1, 1) for q in terms) for terms in side]
    factors = element_terms(side, next_side, stress, hour)
    upper = [[pltpu.roll(q, rows - 1, 1) for q in terms] for terms in factors]
    for m, (a, b, c, e) in enumerate(gathered_x(factors, upper)):
        edge_ref[m, 0] = a + b
        edge_ref[m, 1] = c + e

    row = lax.broadcasted_iota(jnp.int32, (nb, columns, LANES), 1)
    lane = lax.broadcasted_iota(jnp.int32, (nb, columns, LANES), 2)
    block = lax.broadcasted_iota(jnp.int32, (nb, columns, LANES), 0)

    def node_plane(values, at):
        sums, diffs, sums_next, diffs_next = [], [], [], []
        for c in range(6):
            s, d = z_pair(values[c])
            sums.append(s)
            diffs.append(d)
            hs = halo_s[c, :, pl.ds(at, 1), :]
            hd = halo_d[c, :, pl.ds(at, 1), :]
            sums_next.append(jnp.where(row == columns - 1, hs, pltpu.roll(s, columns - 1, 1)))
            diffs_next.append(jnp.where(row == columns - 1, hd, pltpu.roll(d, columns - 1, 1)))
        return node_terms(sums, diffs, sums_next, diffs_next)

    def keep_nodes(terms):
        for c in range(6):
            for t in range(3):
                node_ref[c, t] = terms[c][t]

    def kept_nodes():
        return [tuple(node_ref[c, t] for t in range(3)) for c in range(6)]

    def keep_elements(factors):
        for m in range(3):
            for t in range(7):
                elem_ref[m, t] = factors[m][t]

    def kept_elements():
        return [[elem_ref[m, t] for t in range(7)] for m in range(3)]

    def write_plane(before, after, i):
        weight = (time_step / 64.0) / split(mass_ref[i])
        for m, (a, b, c, e) in enumerate(gathered_x(before, after)):
            ab = edge_ref[m, 0, :, pl.ds(i, 1), :]
            ce = edge_ref[m, 1, :, pl.ds(i, 1), :]
            p = (a - b) + jnp.where(row == 0, ab, pltpu.roll(a + b, 1, 1))
            r = (c - e) + jnp.where(row == 0, ce, pltpu.roll(c + e, 1, 1))
            up = pltpu.roll(p + r, 1, 2)
            before_up = jnp.concatenate([jnp.zeros_like(up[:1]), up[:-1]], 0)
            force = jnp.where(lane == 0, before_up, up)
            last = (lane == LANES - 1) & (block == nb - 1)
            force = force + jnp.where(last, 0.0, p - r)
            result = split(v_ref[m, i]) - force * weight
            for k in range(nb):
                out_ref[m, i, :, k * LANES : (k + 1) * LANES] = result[k]

    def own_nodes(i):
        return [split(u_ref[c, i]) for c in range(3)] + [split(v_ref[c, i]) for c in range(3)]

    keep_nodes(node_plane([split(below(c)) for c in range(6)], 0))
    current = node_plane(own_nodes(0), 1)
    keep_elements(
        element_terms(
            kept_nodes(), current, [split(below(6 + c)) for c in range(6)], split(below(12))
        )
    )
    keep_nodes(current)

    def step(i, upper):
        factors = element_terms(
            kept_nodes(), upper, [split(stress_ref[c, i - 1]) for c in range(6)], split(hour_ref[i - 1])
        )
        write_plane(kept_elements(), factors, i - 1)
        keep_elements(factors)
        keep_nodes(upper)

    def loop(i, carry):
        step(i, node_plane(own_nodes(i), i + 1))
        return carry

    lax.fori_loop(1, planes, loop, 0)
    step(planes, node_plane([split(above(c)) for c in range(6)], planes + 1))


def final_body(
    nspace, capacity, pack, base_ref, mass_ref, table_ref, route_ref, out_hbm, rows_ref, out_ref, sems
):
    planes, columns, depth = base_ref.shape[1:]
    offset = (lax.axis_index("space") % pack) * capacity
    (contact,) = looked_up(table_ref, [route_ref[...]], capacity, offset, nspace)
    rows_ref[...] = jnp.zeros(rows_ref.shape, jnp.float32)
    lane = lax.broadcasted_iota(jnp.int32, (planes, columns, LANES), 2)
    low_weight = jnp.where(lane == 0, time_step / mass_ref[:, :, 0:LANES], 0.0)
    high_weight = jnp.where(
        lane == LANES - 1, time_step / mass_ref[:, :, depth - LANES : depth], 0.0
    )
    copies = []
    for m in range(3):
        rows_ref[m, 0:1, :] = contact[m][0:1]
        rows_ref[m, LANES - 1 : LANES, :] = contact[m][1:2]
        turned = rows_ref[m].T.reshape(planes, columns, LANES)
        for k in range(0, depth, LANES):
            value = base_ref[m, :, :, k : k + LANES]
            if k == 0:
                value = value + low_weight * turned
            if k == depth - LANES:
                value = value + high_weight * turned
            out_ref[m, :, :, k : k + LANES] = value
        copies.append(pltpu.make_async_copy(out_ref.at[m], out_hbm.at[m], sems.at[m]))
        copies[m].start()
    for copy in copies:
        copy.wait()


def local(
    displacement,
    velocity,
    stress,
    hourglass,
    mass,
    contact_route,
    pair_nodes,
    pair_diagonals,
    pair_gap,
    pair_stiffness,
):
    planes, columns, depth = displacement.shape[1:]
    nspace = lax.axis_size("space")
    surf_count = 2 * planes * columns
    pairs = pair_nodes.shape[1]
    capacity, pack, blocks = layout(nspace, surf_count)
    f32 = jnp.float32
    lines = pairs // LANES

    def sized(*shape):
        return jax.ShapeDtypeStruct(shape, f32)

    message = sized(nspace, 8, LANES)
    width = pack * capacity
    whole = jax.ShapeDtypeStruct((5, pairs), jnp.int32)
    place, block, nodes, diagonals, gap, stiffness = kernel_call(
        functools.partial(places_body, width, blocks),
        (
            pair_nodes,
            pair_diagonals,
            pair_gap.reshape(lines, LANES),
            pair_stiffness.reshape(lines, LANES),
        ),
        (
            jax.ShapeDtypeStruct(((width + 15) // 16 * 16, 5 * pairs), jnp.bfloat16),
            whole,
            jax.ShapeDtypeStruct((5, lines, LANES), jnp.int32),
            sized(6, lines, LANES),
            sized(lines, LANES),
            sized(lines, LANES),
        ),
        [
            pltpu.VMEM(whole.shape, jnp.int32),
            pltpu.VMEM((6, pairs), f32),
            pltpu.SemaphoreType.DMA((4,)),
        ],
        hbm_inputs=4,
    )
    fields = (displacement, velocity, stress, hourglass, mass)
    outgoing, ydn, yup, sides, *fields = kernel_call(
        functools.partial(first_body, capacity, pack, blocks),
        (*fields, contact_route.reshape(1, surf_count)),
        (
            message,
            sized(6, planes, depth),
            sized(13, planes, depth),
            jax.ShapeDtypeStruct((2, surf_count // 2), jnp.int32),
            *(sized(*field.shape) for field in fields),
        ),
        [
            pltpu.VMEM((8, surf_count), f32),
            pltpu.VMEM((1, surf_count), jnp.int32),
            pltpu.SemaphoreType.DMA((6,)),
        ],
        hbm_inputs=6,
    )
    yu = shifted(ydn, "slab", -1)
    yd = shifted(yup, "slab", 1)
    received = exchanged(outgoing)
    xdn, xup = kernel_call(
        second_body,
        (*fields[:4], yu, yd),
        (
            sized((6 * columns + 12 + 7) // 8 * 8, depth),
            sized((13 * columns + 19 + 7) // 8 * 8, depth),
        ),
    )
    xu = shifted(xdn, "space", -1)
    xd = shifted(xup, "space", 1)
    slot_force = kernel_call(
        functools.partial(pair_body, nspace, capacity, pack, blocks),
        (
            received,
            nodes,
            diagonals,
            gap,
            stiffness,
            place,
            block,
        ),
        message,
        [pltpu.VMEM((8, pairs), f32), pltpu.VMEM((24 * blocks, 5 * pairs), jnp.bfloat16)],
    )
    returned = exchanged(slot_force)

    nb = depth // LANES
    rows = (planes + 2 + 7) // 8 * 8
    base = kernel_call(
        element_body,
        (*fields, ydn, yu, yd, xu, xd),
        sized(*displacement.shape),
        [
            pltpu.VMEM((rows, depth), f32),
            pltpu.VMEM((6, nb, rows, LANES), f32),
            pltpu.VMEM((6, nb, rows, LANES), f32),
            pltpu.VMEM((3, 2, nb, rows, LANES), f32),
            pltpu.VMEM((6, 3, nb, columns, LANES), f32),
            pltpu.VMEM((3, 7, nb, columns, LANES), f32),
        ],
    )

    return kernel_call(
        functools.partial(final_body, nspace, capacity, pack),
        (base, fields[4], returned, sides),
        sized(*displacement.shape),
        [
            pltpu.VMEM((3, LANES, LANES), f32),
            pltpu.VMEM(displacement.shape, f32),
            pltpu.SemaphoreType.DMA((3,)),
        ],
        final=True,
    )


def solution(mesh):
    in_specs = (
        P(None, "space", "slab", None),
        P(None, "space", "slab", None),
        P(None, "space", "slab", None),
        P("space", "slab", None),
        P("space", "slab", None),
        P(("space", "slab")),
        P(None, ("space", "slab")),
        P(None, ("space", "slab")),
        P(("space", "slab")),
        P(("space", "slab")),
    )
    out_specs = P(None, "space", "slab", None)
    return jax.shard_map(local, mesh=mesh, in_specs=in_specs, out_specs=out_specs, check_vma=False)
```

```python
import functools

import jax
import jax.numpy as jnp
from jax import lax
from jax.experimental import pallas as pl
from jax.experimental.pallas import tpu as pltpu
from jax.sharding import PartitionSpec as P


time_step = 0.5
LANES = 128
VOIGT = [[0, 5, 4], [5, 1, 3], [4, 3, 2]]


def shifted(value, axis, steps):
    count = lax.axis_size(axis)
    return lax.ppermute(value, axis, [(at, (at + steps) % count) for at in range(count)])


def exchanged(value):
    return lax.all_to_all(value, "space", split_axis=0, concat_axis=0, tiled=True)


def kernel_call(body, inputs, outs, scratch=(), hbm_inputs=0):
    spaces = [pltpu.HBM if at < hbm_inputs else pltpu.VMEM for at in range(len(inputs))]
    inputs = [pltpu.with_memory_space_constraint(*pair) for pair in zip(inputs, spaces)]

    def placed(out):
        if isinstance(out, jax.ShapeDtypeStruct):
            return pltpu.VMEM(out.shape, out.dtype)
        return out

    outs = tuple(placed(out) for out in outs) if isinstance(outs, tuple) else placed(outs)
    return pl.pallas_call(
        body,
        out_shape=outs,
        in_specs=[pl.BlockSpec(memory_space=one) for one in spaces],
        out_specs=jax.tree.map(lambda out: pl.BlockSpec(memory_space=out.memory_space), outs),
        scratch_shapes=list(scratch),
        compiler_params=pltpu.CompilerParams(vmem_limit_bytes=16 << 20),
    )(*inputs)


def contract_lanes(lhs, rhs):
    return lax.dot_general(lhs, rhs, (((1,), (1,)), ((), ())), preferred_element_type=jnp.float32)


def layout(nspace, surf_count):
    capacity = max(2, (3 * surf_count // 2 + nspace - 1) // nspace)
    pack = max(1, min(LANES // capacity, nspace // 8))
    while nspace % pack:
        pack -= 1
    return capacity, pack, nspace // pack


def block_of(slots, width, blocks):
    block = jnp.zeros_like(slots)
    for b in range(1, blocks):
        block = block + jnp.where(slots >= b * width, 1, 0)
    return block, slots - block * width


def parts_of(rows):
    high = rows.astype(jnp.bfloat16).astype(jnp.float32)
    rest = rows - high
    middle = rest.astype(jnp.bfloat16).astype(jnp.float32)
    return [high, middle, rest - middle]


def places(place, width):
    rows = (width + 15) // 16 * 16
    count = place.shape[1]
    at = lax.broadcasted_iota(jnp.int32, (rows, count), 0)
    return jnp.where(at == place, 1.0, 0.0).astype(jnp.bfloat16)


def spread(parts, block, blocks):
    return [
        jnp.where(block == b, part, 0.0).astype(jnp.bfloat16)
        for part in parts
        for b in range(blocks)
    ]


def write_messages(out_ref, got, pack, blocks):
    for b in range(blocks):
        at = [(part * blocks + b) * 8 for part in range(3)]
        total = got[at[0] : at[0] + 8] + got[at[1] : at[1] + 8] + got[at[2] : at[2] + 8]
        for q in range(pack):
            out_ref[b * pack + q, :, 0 : total.shape[1]] = total


def first_body(
    capacity, pack, blocks, u_hbm, route_hbm, v_hbm, *rest,
):
    hbm, rest = (u_hbm, route_hbm, v_hbm) + rest[:7], rest[7:]
    message_hbm, ydn, sides_ref, u_ref, v_ref = rest[:5]
    out_ref, rows_ref, route_ref, sems, message_sem = rest[-5:]
    targets = (u_ref, route_ref, v_ref) + rest[5:-5]
    copies = [
        pltpu.make_async_copy(source, target, sems.at[at])
        for at, (source, target) in enumerate(zip(hbm, targets))
    ]
    for copy in copies:
        copy.start()
    out_ref[...] = jnp.zeros(out_ref.shape, jnp.float32)
    rows_ref[...] = jnp.zeros(rows_ref.shape, jnp.float32)
    copies[0].wait()
    copies[1].wait()
    planes, columns, depth = u_ref.shape[1:]
    side = planes * columns
    lane = lax.broadcasted_iota(jnp.int32, (side, LANES), 1)
    for c in range(3):
        bottom = u_ref[c, :, :, 0:LANES].reshape(side, LANES)
        top = u_ref[c, :, :, depth - LANES : depth].reshape(side, LANES)
        both = jnp.where(lane == LANES - 1, top, bottom).T
        rows_ref[c : c + 1, 0:side] = both[0:1]
        rows_ref[c : c + 1, side : 2 * side] = both[LANES - 1 : LANES]
    width = pack * capacity
    route = route_ref[...]
    block, place = block_of(route, width, blocks)
    entries = spread(parts_of(rows_ref[...]), block, blocks)
    got = contract_lanes(jnp.concatenate(entries, 0), places(place, width))
    write_messages(out_ref, got, pack, blocks)
    message = pltpu.make_async_copy(out_ref, message_hbm, message_sem)
    message.start()
    sides_ref[0:1, :] = route[:, 0:side]
    sides_ref[1:2, :] = route[:, side : 2 * side]
    for c in range(3):
        ydn[c] = u_ref[c, :, 0, :]
    copies[2].wait()
    for c in range(3):
        ydn[3 + c] = v_ref[c, :, 0, :]
    for copy in copies[3:]:
        copy.wait()
    message.wait()


def component(u_ref, v_ref, stress_ref, hour_ref, c):
    if c < 3:
        return u_ref.at[c]
    if c < 6:
        return v_ref.at[c - 3]
    if c < 12:
        return stress_ref.at[c - 6]
    return hour_ref


def second_body(u_ref, v_ref, stress_ref, hour_ref, yu, xdn, xup):
    planes, columns = u_ref.shape[1:3]
    for c in range(13):
        ref = component(u_ref, v_ref, stress_ref, hour_ref, c)
        xup[c * columns : (c + 1) * columns, :] = ref[planes - 1]
        if c < 6:
            at = 13 * columns + c
            xup[at : at + 1, :] = yu[c, planes - 1 : planes, :]
            xdn[c * columns : (c + 1) * columns, :] = ref[0]
            at = 6 * columns + c
            xdn[at : at + 1, :] = yu[c, 0:1, :]


def places_body(width, blocks, nodes_ref, diag_ref, place_ref, block_ref, lines_ref, diag_lines_ref):
    pairs = nodes_ref.shape[1]
    for j in range(5):
        nodes = nodes_ref[j : j + 1, :]
        block, place = block_of(nodes, width, blocks)
        block_ref[j : j + 1, :] = block
        place_ref[:, j * pairs : (j + 1) * pairs] = places(place, width)
        for r in range(pairs // LANES):
            lines_ref[j, r : r + 1, :] = nodes[:, r * LANES : (r + 1) * LANES]
    for c in range(6):
        for r in range(pairs // LANES):
            diag_lines_ref[c, r : r + 1, :] = diag_ref[c : c + 1, r * LANES : (r + 1) * LANES]


def looked_up(table_ref, slots, capacity, offset, count):
    shape = slots[0].shape

    def step(s, found):
        shift = s * capacity - offset
        result = []
        for slot, old in zip(slots, found):
            here = (slot >= s * capacity) & (slot < (s + 1) * capacity)
            index = (slot - shift) & (LANES - 1)
            new = []
            for c in range(3):
                row = jnp.broadcast_to(table_ref[s, c : c + 1, :], shape)
                new.append(jnp.where(here, jnp.take_along_axis(row, index, axis=1), old[c]))
            result.append(tuple(new))
        return tuple(result)

    zero = jnp.zeros(shape, jnp.float32)
    found = tuple((zero, zero, zero) for _ in slots)
    if count <= 16:
        for s in range(count):
            found = step(s, found)
        return found
    return lax.fori_loop(0, count, step, found)


def pair_body(
    nspace, capacity, pack, blocks, table_ref, nodes_ref, diag_ref, gap_ref, stiff_ref, place_ref,
    block_ref, out_ref, rows_ref, entry_ref,
):
    offset = (lax.axis_index("space") % pack) * capacity
    picked = looked_up(table_ref, [nodes_ref[j] for j in range(5)], capacity, offset, nspace)
    slave = picked[0]
    first = [diag_ref[c] + picked[3][c] - picked[1][c] for c in range(3)]
    second = [diag_ref[3 + c] + picked[4][c] - picked[2][c] for c in range(3)]
    normal = [
        first[(c + 1) % 3] * second[(c + 2) % 3] - first[(c + 2) % 3] * second[(c + 1) % 3]
        for c in range(3)
    ]
    gap = gap_ref[...]
    for c in range(3):
        centre = (picked[1][c] + picked[2][c] + picked[3][c] + picked[4][c]) * 0.25
        gap = gap + (slave[c] - centre) * normal[c]
    push = stiff_ref[...] * jnp.maximum(-gap, 0.0)
    pairs = rows_ref.shape[1]
    rows_ref[...] = jnp.zeros(rows_ref.shape, jnp.float32)
    for c in range(3):
        force = push * normal[c]
        for r in range(force.shape[0]):
            rows_ref[c : c + 1, r * LANES : (r + 1) * LANES] = force[r : r + 1]
    parts = parts_of(rows_ref[...])
    fourth = [part * -0.25 for part in parts]
    for j in range(5):
        entries = spread(fourth if j else parts, block_ref[j : j + 1, :], blocks)
        entry_ref[:, j * pairs : (j + 1) * pairs] = jnp.concatenate(entries, 0)
    out_ref[...] = jnp.zeros(out_ref.shape, jnp.float32)
    got = contract_lanes(entry_ref[...], place_ref[...])
    write_messages(out_ref, got, pack, blocks)


def split(value):
    return jnp.stack([value[:, at : at + LANES] for at in range(0, value.shape[1], LANES)])


def z_pair(f):
    lane = lax.broadcasted_iota(jnp.int32, f.shape, 2)
    turned = pltpu.roll(f, LANES - 1, 2)
    after = jnp.concatenate([turned[1:], turned[:1]], 0)
    upper = jnp.where(lane == LANES - 1, after, turned)
    return f + upper, upper - f


def node_terms(sums, diffs, sums_next, diffs_next):
    result = []
    for c in range(6):
        s0, s1, d0, d1 = sums[c], sums_next[c], diffs[c], diffs_next[c]
        if c < 3:
            result.append((s0 + s1, s1 - s0, d0 + d1))
        else:
            result.append((d1 - d0, d0 + d1, s1 - s0))
    return result


def element_terms(lower, upper, stress, hour):
    eight = []
    for m in range(3):
        row = [
            upper[m][0] - lower[m][0],
            lower[m][1] + upper[m][1],
            lower[m][2] + upper[m][2],
        ]
        row[m] = row[m] + 4.0
        eight.append(row)
    cof = [
        [
            eight[(m + 1) % 3][(n + 1) % 3] * eight[(m + 2) % 3][(n + 2) % 3]
            - eight[(m + 1) % 3][(n + 2) % 3] * eight[(m + 2) % 3][(n + 1) % 3]
            for n in range(3)
        ]
        for m in range(3)
    ]
    hour = hour * 64.0
    result = []
    for m in range(3):
        line = [
            stress[VOIGT[m][0]] * cof[0][n]
            + stress[VOIGT[m][1]] * cof[1][n]
            + stress[VOIGT[m][2]] * cof[2][n]
            for n in range(3)
        ]
        low, up = lower[3 + m], upper[3 + m]
        line.append(hour * (low[0] + up[0]))
        line.append(hour * (up[1] - low[1]))
        line.append(hour * (up[2] - low[2]))
        line.append(hour * (up[0] - low[0]))
        result.append(line)
    return result


def gathered_x(before, after):
    result = []
    for m in range(3):
        p, n = before[m], after[m]
        result.append(
            (
                p[0] - n[0],
                (p[1] + n[1]) + (p[5] - n[5]),
                (p[2] + n[2]) + (p[4] - n[4]),
                (p[3] + n[3]) + (p[6] - n[6]),
            )
        )
    return result


def element_body(
    u_ref, v_ref, stress_ref, hour_ref, mass_ref, yu, xu, xd,
    out_ref, beyond_ref, row_ref, halo_s, halo_d, last_ref, node_ref, elem_ref,
):
    planes, columns, depth = u_ref.shape[1:]
    nb = depth // LANES

    def below(c):
        return xd[c * columns : (c + 1) * columns, :]

    def above(c):
        return xu[c * columns : (c + 1) * columns, :]

    row_ref[...] = jnp.zeros(row_ref.shape, jnp.float32)
    for c in range(6):
        row_ref[0:1, :] = xd[13 * columns + c : 13 * columns + c + 1, :]
        row_ref[1 : planes + 1, :] = yu[c]
        row_ref[planes + 1 : planes + 2, :] = xu[6 * columns + c : 6 * columns + c + 1, :]
        halo_s[c], halo_d[c] = z_pair(split(row_ref[...]))

    row = lax.broadcasted_iota(jnp.int32, (nb, columns, LANES), 1)

    def node_plane(values, at):
        sums, diffs, sums_next, diffs_next = [], [], [], []
        for c in range(6):
            s, d = z_pair(values[c])
            sums.append(s)
            diffs.append(d)
            hs = halo_s[c, :, pl.ds(at, 1), :]
            hd = halo_d[c, :, pl.ds(at, 1), :]
            sums_next.append(jnp.where(row == columns - 1, hs, pltpu.roll(s, columns - 1, 1)))
            diffs_next.append(jnp.where(row == columns - 1, hd, pltpu.roll(d, columns - 1, 1)))
        return node_terms(sums, diffs, sums_next, diffs_next)

    def keep_nodes(terms):
        for c in range(6):
            for t in range(3):
                node_ref[c, t] = terms[c][t]

    def kept_nodes():
        return [tuple(node_ref[c, t] for t in range(3)) for c in range(6)]

    def keep_elements(factors):
        for m in range(3):
            for t in range(7):
                elem_ref[m, t] = factors[m][t]

    def kept_elements():
        return [[elem_ref[m, t] for t in range(7)] for m in range(3)]

    def along_z(p, r):
        lane = lax.broadcasted_iota(jnp.int32, p.shape, 2)
        block = lax.broadcasted_iota(jnp.int32, p.shape, 0)
        up = pltpu.roll(p + r, 1, 2)
        before_up = jnp.concatenate([jnp.zeros_like(up[:1]), up[:-1]], 0)
        last = (lane == LANES - 1) & (block == nb - 1)
        return jnp.where(lane == 0, before_up, up) + jnp.where(last, 0.0, p - r)

    def write_plane(before, after, i):
        weight = (time_step / 64.0) / split(mass_ref[i])
        for m, (a, b, c, e) in enumerate(gathered_x(before, after)):
            ab, ce = a + b, c + e
            last_ref[m, 0, :, pl.ds(i, 1), :] = ab[:, columns - 1 : columns]
            last_ref[m, 1, :, pl.ds(i, 1), :] = ce[:, columns - 1 : columns]
            p = (a - b) + jnp.where(row == 0, 0.0, pltpu.roll(ab, 1, 1))
            r = (c - e) + jnp.where(row == 0, 0.0, pltpu.roll(ce, 1, 1))
            result = split(v_ref[m, i]) - along_z(p, r) * weight
            for k in range(nb):
                out_ref[m, i, :, k * LANES : (k + 1) * LANES] = result[k]

    def own_nodes(i):
        return [split(u_ref[c, i]) for c in range(3)] + [split(v_ref[c, i]) for c in range(3)]

    keep_nodes(node_plane([split(below(c)) for c in range(6)], 0))
    current = node_plane(own_nodes(0), 1)
    keep_elements(
        element_terms(
            kept_nodes(), current, [split(below(6 + c)) for c in range(6)], split(below(12))
        )
    )
    keep_nodes(current)

    def step(i, upper):
        factors = element_terms(
            kept_nodes(), upper, [split(stress_ref[c, i - 1]) for c in range(6)], split(hour_ref[i - 1])
        )
        write_plane(kept_elements(), factors, i - 1)
        keep_elements(factors)
        keep_nodes(upper)

    def loop(i, carry):
        step(i, node_plane(own_nodes(i), i + 1))
        return carry

    lax.fori_loop(1, planes, loop, 0)
    step(planes, node_plane([split(above(c)) for c in range(6)], planes + 1))
    for m in range(3):
        force = along_z(last_ref[m, 0], last_ref[m, 1])
        for k in range(nb):
            beyond_ref[m, :, k * LANES : (k + 1) * LANES] = force[k]


def final_body(
    nspace, capacity, pack,
    base_ref, mass_ref, table_ref, route_ref, left_ref, out_hbm, rows_ref, out_ref, sems,
):
    planes, columns, depth = base_ref.shape[1:]
    offset = (lax.axis_index("space") % pack) * capacity
    (contact,) = looked_up(table_ref, [route_ref[...]], capacity, offset, nspace)
    rows_ref[...] = jnp.zeros(rows_ref.shape, jnp.float32)
    lane = lax.broadcasted_iota(jnp.int32, (planes, columns, LANES), 2)
    row = lax.broadcasted_iota(jnp.int32, (columns, LANES), 0)
    weights = [time_step / mass_ref[:, :, k : k + LANES] for k in range(0, depth, LANES)]
    low_weight = jnp.where(lane == 0, weights[0], 0.0)
    high_weight = jnp.where(lane == LANES - 1, weights[-1], 0.0)
    copies = []
    for m in range(3):
        rows_ref[m, 0:1, :] = contact[m][0:1]
        rows_ref[m, LANES - 1 : LANES, :] = contact[m][1:2]
        turned = rows_ref[m].T.reshape(planes, columns, LANES)
        for k in range(0, depth, LANES):
            left = jnp.stack(
                [
                    jnp.where(row == 0, left_ref[m, i : i + 1, k : k + LANES] * (1.0 / 64.0), 0.0)
                    for i in range(planes)
                ]
            )
            value = base_ref[m, :, :, k : k + LANES] - left * weights[k // LANES]
            if k == 0:
                value = value + low_weight * turned
            if k == depth - LANES:
                value = value + high_weight * turned
            out_ref[m, :, :, k : k + LANES] = value
        copies.append(pltpu.make_async_copy(out_ref.at[m], out_hbm.at[m], sems.at[m]))
        copies[m].start()
    for copy in copies:
        copy.wait()


def local(
    displacement,
    velocity,
    stress,
    hourglass,
    mass,
    contact_route,
    pair_nodes,
    pair_diagonals,
    pair_gap,
    pair_stiffness,
):
    planes, columns, depth = displacement.shape[1:]
    nspace = lax.axis_size("space")
    surf_count = 2 * planes * columns
    pairs = pair_nodes.shape[1]
    capacity, pack, blocks = layout(nspace, surf_count)
    f32 = jnp.float32
    lines = pairs // LANES

    def sized(*shape):
        return jax.ShapeDtypeStruct(shape, f32)

    message = sized(nspace, 8, LANES)
    width = pack * capacity
    small = (pair_nodes, pair_diagonals, pair_gap.reshape(lines, LANES))
    small += (pair_stiffness.reshape(lines, LANES),)
    kept = (displacement, velocity, stress, hourglass, mass) + small
    outgoing, ydn, sides, *kept = kernel_call(
        functools.partial(first_body, capacity, pack, blocks),
        (displacement, contact_route.reshape(1, surf_count)) + kept[1:],
        (
            pltpu.HBM(message.shape, f32),
            sized(6, planes, depth),
            jax.ShapeDtypeStruct((2, surf_count // 2), jnp.int32),
            *(jax.ShapeDtypeStruct(one.shape, one.dtype) for one in kept),
        ),
        [
            pltpu.VMEM(message.shape, f32),
            pltpu.VMEM((8, surf_count), f32),
            pltpu.VMEM((1, surf_count), jnp.int32),
            pltpu.SemaphoreType.DMA((len(kept) + 1,)),
            pltpu.SemaphoreType.DMA,
        ],
        hbm_inputs=len(kept) + 1,
    )
    fields, (pair_nodes, pair_diagonals, gap, stiffness) = kept[:5], kept[5:]
    yu = shifted(ydn, "slab", -1)
    received = exchanged(outgoing)
    xdn, xup = kernel_call(
        second_body,
        (*fields[:4], yu),
        (
            sized((6 * columns + 6 + 7) // 8 * 8, depth),
            sized((13 * columns + 6 + 7) // 8 * 8, depth),
        ),
    )
    xu = shifted(xdn, "space", -1)
    xd = shifted(xup, "space", 1)
    place, block, nodes, diagonals = kernel_call(
        functools.partial(places_body, width, blocks),
        (pair_nodes, pair_diagonals),
        (
            jax.ShapeDtypeStruct(((width + 15) // 16 * 16, 5 * pairs), jnp.bfloat16),
            jax.ShapeDtypeStruct((5, pairs), jnp.int32),
            jax.ShapeDtypeStruct((5, lines, LANES), jnp.int32),
            sized(6, lines, LANES),
        ),
    )
    slot_force = kernel_call(
        functools.partial(pair_body, nspace, capacity, pack, blocks),
        (received, nodes, diagonals, gap, stiffness, place, block),
        message,
        [pltpu.VMEM((8, pairs), f32), pltpu.VMEM((24 * blocks, 5 * pairs), jnp.bfloat16)],
    )
    returned = exchanged(slot_force)

    nb = depth // LANES
    rows = (planes + 2 + 7) // 8 * 8
    base, beyond = kernel_call(
        element_body,
        (*fields, yu, xu, xd),
        (sized(*displacement.shape), sized(3, planes, depth)),
        [
            pltpu.VMEM((rows, depth), f32),
            pltpu.VMEM((6, nb, rows, LANES), f32),
            pltpu.VMEM((6, nb, rows, LANES), f32),
            pltpu.VMEM((3, 2, nb, planes, LANES), f32),
            pltpu.VMEM((6, 3, nb, columns, LANES), f32),
            pltpu.VMEM((3, 7, nb, columns, LANES), f32),
        ],
    )
    left = shifted(beyond, "slab", 1)

    return kernel_call(
        functools.partial(final_body, nspace, capacity, pack),
        (base, fields[4], returned, sides, left),
        pltpu.HBM(displacement.shape, f32),
        [
            pltpu.VMEM((3, LANES, LANES), f32),
            pltpu.VMEM(displacement.shape, f32),
            pltpu.SemaphoreType.DMA((3,)),
        ],
    )


def solution(mesh):
    in_specs = (
        P(None, "space", "slab", None),
        P(None, "space", "slab", None),
        P(None, "space", "slab", None),
        P("space", "slab", None),
        P("space", "slab", None),
        P(("space", "slab")),
        P(None, ("space", "slab")),
        P(None, ("space", "slab")),
        P(("space", "slab")),
        P(("space", "slab")),
    )
    out_specs = P(None, "space", "slab", None)
    return jax.shard_map(local, mesh=mesh, in_specs=in_specs, out_specs=out_specs, check_vma=False)
```

```python
import functools

import jax
import jax.numpy as jnp
from jax import lax
from jax.experimental import pallas as pl
from jax.experimental.pallas import tpu as pltpu
from jax.sharding import PartitionSpec as P


time_step = 0.5
LANES = 128
VOIGT = [[0, 5, 4], [5, 1, 3], [4, 3, 2]]


def shifted(value, axis, steps):
    count = lax.axis_size(axis)
    return lax.ppermute(value, axis, [(at, (at + steps) % count) for at in range(count)])


def exchanged(value):
    return lax.all_to_all(value, "space", split_axis=0, concat_axis=0, tiled=True)


def kernel_call(body, inputs, outs, scratch=(), hbm_inputs=0):
    spaces = [pltpu.HBM if at < hbm_inputs else pltpu.VMEM for at in range(len(inputs))]
    inputs = [pltpu.with_memory_space_constraint(*pair) for pair in zip(inputs, spaces)]

    def placed(out):
        if isinstance(out, jax.ShapeDtypeStruct):
            return pltpu.VMEM(out.shape, out.dtype)
        return out

    outs = tuple(placed(out) for out in outs) if isinstance(outs, tuple) else placed(outs)
    return pl.pallas_call(
        body,
        out_shape=outs,
        in_specs=[pl.BlockSpec(memory_space=one) for one in spaces],
        out_specs=jax.tree.map(lambda out: pl.BlockSpec(memory_space=out.memory_space), outs),
        scratch_shapes=list(scratch),
        compiler_params=pltpu.CompilerParams(vmem_limit_bytes=16 << 20),
    )(*inputs)


def contract_lanes(lhs, rhs):
    return lax.dot_general(lhs, rhs, (((1,), (1,)), ((), ())), preferred_element_type=jnp.float32)


def layout(nspace, surf_count):
    capacity = max(2, (3 * surf_count // 2 + nspace - 1) // nspace)
    pack = max(1, min(LANES // capacity, nspace // 8))
    while nspace % pack:
        pack -= 1
    return capacity, pack, nspace // pack


def block_of(slots, width, blocks):
    block = jnp.zeros_like(slots)
    for b in range(1, blocks):
        block = block + jnp.where(slots >= b * width, 1, 0)
    return block, slots - block * width


def parts_of(rows):
    high = rows.astype(jnp.bfloat16).astype(jnp.float32)
    rest = rows - high
    middle = rest.astype(jnp.bfloat16).astype(jnp.float32)
    return [high, middle, rest - middle]


def places(place, width):
    rows = (width + 15) // 16 * 16
    count = place.shape[1]
    at = lax.broadcasted_iota(jnp.int32, (rows, count), 0)
    return jnp.where(at == place, 1.0, 0.0).astype(jnp.bfloat16)


def spread(parts, block, blocks):
    return [
        jnp.where(block == b, part, 0.0).astype(jnp.bfloat16)
        for part in parts
        for b in range(blocks)
    ]


def write_messages(out_ref, got, pack, blocks):
    for b in range(blocks):
        at = [(part * blocks + b) * 8 for part in range(3)]
        total = got[at[0] : at[0] + 8] + got[at[1] : at[1] + 8] + got[at[2] : at[2] + 8]
        for q in range(pack):
            out_ref[b * pack + q, :, 0 : total.shape[1]] = total


def first_body(
    capacity, pack, blocks, u_hbm, route_hbm, v_hbm, *rest,
):
    hbm, rest = (u_hbm, route_hbm, v_hbm) + rest[:7], rest[7:]
    message_hbm, ydn, sides_ref, u_ref, v_ref = rest[:5]
    out_ref, rows_ref, route_ref, sems, message_sem = rest[-5:]
    targets = (u_ref, route_ref, v_ref) + rest[5:-5]
    copies = [
        pltpu.make_async_copy(source, target, sems.at[at])
        for at, (source, target) in enumerate(zip(hbm, targets))
    ]
    for copy in copies:
        copy.start()
    out_ref[...] = jnp.zeros(out_ref.shape, jnp.float32)
    rows_ref[...] = jnp.zeros(rows_ref.shape, jnp.float32)
    copies[0].wait()
    copies[1].wait()
    planes, columns, depth = u_ref.shape[1:]
    side = planes * columns
    lane = lax.broadcasted_iota(jnp.int32, (side, LANES), 1)
    for c in range(3):
        bottom = u_ref[c, :, :, 0:LANES].reshape(side, LANES)
        top = u_ref[c, :, :, depth - LANES : depth].reshape(side, LANES)
        both = jnp.where(lane == LANES - 1, top, bottom).T
        rows_ref[c : c + 1, 0:side] = both[0:1]
        rows_ref[c : c + 1, side : 2 * side] = both[LANES - 1 : LANES]
    width = pack * capacity
    route = route_ref[...]
    block, place = block_of(route, width, blocks)
    entries = spread(parts_of(rows_ref[...]), block, blocks)
    got = contract_lanes(jnp.concatenate(entries, 0), places(place, width))
    write_messages(out_ref, got, pack, blocks)
    message = pltpu.make_async_copy(out_ref, message_hbm, message_sem)
    message.start()
    sides_ref[0:1, :] = route[:, 0:side]
    sides_ref[1:2, :] = route[:, side : 2 * side]
    for c in range(3):
        ydn[c] = u_ref[c, :, 0, :]
    copies[2].wait()
    for c in range(3):
        ydn[3 + c] = v_ref[c, :, 0, :]
    for copy in copies[3:]:
        copy.wait()
    message.wait()


def component(u_ref, v_ref, stress_ref, hour_ref, c):
    if c < 3:
        return u_ref.at[c]
    if c < 6:
        return v_ref.at[c - 3]
    if c < 12:
        return stress_ref.at[c - 6]
    return hour_ref


def second_body(u_ref, v_ref, stress_ref, hour_ref, yu, xdn, xup):
    planes, columns = u_ref.shape[1:3]
    for c in range(13):
        ref = component(u_ref, v_ref, stress_ref, hour_ref, c)
        xup[c * columns : (c + 1) * columns, :] = ref[planes - 1]
        if c < 6:
            at = 13 * columns + c
            xup[at : at + 1, :] = yu[c, planes - 1 : planes, :]
            xdn[c * columns : (c + 1) * columns, :] = ref[0]
            at = 6 * columns + c
            xdn[at : at + 1, :] = yu[c, 0:1, :]


def matrix_body(nodes_ref, diag_ref, matrix_ref, lines_ref, diag_lines_ref):
    pairs = nodes_ref.shape[1]
    group = 16

    def rows(g, carry):
        start = pl.multiple_of(g * group, group)
        slot = lax.broadcasted_iota(jnp.int32, (group, pairs), 0) + start
        total = jnp.where(nodes_ref[0:1, :] == slot, 1.0, 0.0)
        for j in range(1, 5):
            total = total - jnp.where(nodes_ref[j : j + 1, :] == slot, 0.25, 0.0)
        matrix_ref[pl.ds(start, group), :] = total.astype(jnp.bfloat16)
        return carry

    lax.fori_loop(0, matrix_ref.shape[0] // group, rows, 0)
    for r in range(pairs // LANES):
        for j in range(5):
            lines_ref[j, r : r + 1, :] = nodes_ref[j : j + 1, r * LANES : (r + 1) * LANES]
        for c in range(6):
            diag_lines_ref[c, r : r + 1, :] = diag_ref[c : c + 1, r * LANES : (r + 1) * LANES]


def looked_up(table_ref, slots, capacity, offset, count):
    shape = slots[0].shape

    def step(s, found):
        shift = s * capacity - offset
        result = []
        for slot, old in zip(slots, found):
            here = (slot >= s * capacity) & (slot < (s + 1) * capacity)
            index = (slot - shift) & (LANES - 1)
            new = []
            for c in range(3):
                row = jnp.broadcast_to(table_ref[s, c : c + 1, :], shape)
                new.append(jnp.where(here, jnp.take_along_axis(row, index, axis=1), old[c]))
            result.append(tuple(new))
        return tuple(result)

    zero = jnp.zeros(shape, jnp.float32)
    found = tuple((zero, zero, zero) for _ in slots)
    if count <= 16:
        for s in range(count):
            found = step(s, found)
        return found
    return lax.fori_loop(0, count, step, found)


def pair_body(
    nspace, capacity, pack, blocks,
    table_ref, nodes_ref, diag_ref, gap_ref, stiff_ref, matrix_ref, out_hbm, rows_ref, out_ref, sem,
):
    offset = (lax.axis_index("space") % pack) * capacity
    picked = looked_up(table_ref, [nodes_ref[j] for j in range(5)], capacity, offset, nspace)
    slave = picked[0]
    first = [diag_ref[c] + picked[3][c] - picked[1][c] for c in range(3)]
    second = [diag_ref[3 + c] + picked[4][c] - picked[2][c] for c in range(3)]
    normal = [
        first[(c + 1) % 3] * second[(c + 2) % 3] - first[(c + 2) % 3] * second[(c + 1) % 3]
        for c in range(3)
    ]
    gap = gap_ref[...]
    for c in range(3):
        centre = (picked[1][c] + picked[2][c] + picked[3][c] + picked[4][c]) * 0.25
        gap = gap + (slave[c] - centre) * normal[c]
    push = stiff_ref[...] * jnp.maximum(-gap, 0.0)
    out_ref[...] = jnp.zeros(out_ref.shape, jnp.float32)
    rows_ref[...] = jnp.zeros(rows_ref.shape, jnp.float32)
    for c in range(3):
        force = push * normal[c]
        for r in range(force.shape[0]):
            rows_ref[c : c + 1, r * LANES : (r + 1) * LANES] = force[r : r + 1]
    parts = [part.astype(jnp.bfloat16) for part in parts_of(rows_ref[...])]
    got = contract_lanes(jnp.concatenate(parts, 0), matrix_ref[...])
    total = got[0:8] + got[8:16] + got[16:24]
    width = pack * capacity
    for b in range(blocks):
        for q in range(pack):
            out_ref[b * pack + q, :, 0:width] = total[:, b * width : (b + 1) * width]
    copy = pltpu.make_async_copy(out_ref, out_hbm, sem)
    copy.start()
    copy.wait()


def split(value):
    return jnp.stack([value[:, at : at + LANES] for at in range(0, value.shape[1], LANES)])


def z_pair(f):
    lane = lax.broadcasted_iota(jnp.int32, f.shape, 2)
    turned = pltpu.roll(f, LANES - 1, 2)
    after = jnp.concatenate([turned[1:], turned[:1]], 0)
    upper = jnp.where(lane == LANES - 1, after, turned)
    return f + upper, upper - f


def node_terms(sums, diffs, sums_next, diffs_next):
    result = []
    for c in range(6):
        s0, s1, d0, d1 = sums[c], sums_next[c], diffs[c], diffs_next[c]
        if c < 3:
            result.append((s0 + s1, s1 - s0, d0 + d1))
        else:
            result.append((d1 - d0, d0 + d1, s1 - s0))
    return result


def element_terms(lower, upper, stress, hour):
    eight = []
    for m in range(3):
        row = [
            upper[m][0] - lower[m][0],
            lower[m][1] + upper[m][1],
            lower[m][2] + upper[m][2],
        ]
        row[m] = row[m] + 4.0
        eight.append(row)
    cof = [
        [
            eight[(m + 1) % 3][(n + 1) % 3] * eight[(m + 2) % 3][(n + 2) % 3]
            - eight[(m + 1) % 3][(n + 2) % 3] * eight[(m + 2) % 3][(n + 1) % 3]
            for n in range(3)
        ]
        for m in range(3)
    ]
    hour = hour * 64.0
    result = []
    for m in range(3):
        line = [
            stress[VOIGT[m][0]] * cof[0][n]
            + stress[VOIGT[m][1]] * cof[1][n]
            + stress[VOIGT[m][2]] * cof[2][n]
            for n in range(3)
        ]
        low, up = lower[3 + m], upper[3 + m]
        line.append(hour * (low[0] + up[0]))
        line.append(hour * (up[1] - low[1]))
        line.append(hour * (up[2] - low[2]))
        line.append(hour * (up[0] - low[0]))
        result.append(line)
    return result


def gathered_x(before, after):
    result = []
    for m in range(3):
        p, n = before[m], after[m]
        result.append(
            (
                p[0] - n[0],
                (p[1] + n[1]) + (p[5] - n[5]),
                (p[2] + n[2]) + (p[4] - n[4]),
                (p[3] + n[3]) + (p[6] - n[6]),
            )
        )
    return result


def along_z(p, r):
    lane = lax.broadcasted_iota(jnp.int32, p.shape, 2)
    block = lax.broadcasted_iota(jnp.int32, p.shape, 0)
    nb = p.shape[0]
    up = pltpu.roll(p + r, 1, 2)
    before_up = jnp.concatenate([jnp.zeros_like(up[:1]), up[:-1]], 0)
    last = (lane == LANES - 1) & (block == nb - 1)
    return jnp.where(lane == 0, before_up, up) + jnp.where(last, 0.0, p - r)


def edge_body(u_ref, v_ref, stress_ref, hour_ref, yu, xu, xd, beyond_ref, row_ref):
    planes, columns, _ = u_ref.shape[1:]
    rows = row_ref.shape[0]
    row_ref[...] = jnp.zeros(row_ref.shape, jnp.float32)

    def assembled(first, middle, last):
        row_ref[0:1, :] = first
        row_ref[1 : planes + 1, :] = middle
        if last is not None:
            row_ref[planes + 1 : planes + 2, :] = last
        return split(row_ref[...])

    def line(ref, at):
        return ref[at : at + 1, :]

    def following(q):
        return pltpu.roll(q, rows - 1, 1)

    def own(c):
        middle = component(u_ref, v_ref, stress_ref, hour_ref, c)[:, columns - 1, :]
        at = c * columns + columns - 1
        return assembled(line(xd, at), middle, line(xu, at) if c < 6 else None)

    own_s, own_d, next_s, next_d = [], [], [], []
    for c in range(6):
        s, d = z_pair(own(c))
        own_s.append(s)
        own_d.append(d)
        last = line(xu, 6 * columns + c)
        s, d = z_pair(assembled(line(xd, 13 * columns + c), yu[c], last))
        next_s.append(s)
        next_d.append(d)
    lower = node_terms(own_s, own_d, next_s, next_d)
    upper = [tuple(following(q) for q in terms) for terms in lower]
    factors = element_terms(lower, upper, [own(6 + c) for c in range(6)], own(12))
    after = [[following(q) for q in terms] for terms in factors]
    for m, (a, b, c, e) in enumerate(gathered_x(factors, after)):
        force = along_z(a + b, c + e)[:, 0:planes]
        for k in range(force.shape[0]):
            beyond_ref[m, :, k * LANES : (k + 1) * LANES] = force[k]


def element_body(
    u_ref, v_ref, stress_ref, hour_ref, mass_ref, yu, xu, xd,
    out_ref, row_ref, halo_s, halo_d, node_ref, elem_ref,
):
    planes, columns, depth = u_ref.shape[1:]
    nb = depth // LANES

    def below(c):
        return xd[c * columns : (c + 1) * columns, :]

    def above(c):
        return xu[c * columns : (c + 1) * columns, :]

    row_ref[...] = jnp.zeros(row_ref.shape, jnp.float32)
    for c in range(6):
        row_ref[0:1, :] = xd[13 * columns + c : 13 * columns + c + 1, :]
        row_ref[1 : planes + 1, :] = yu[c]
        row_ref[planes + 1 : planes + 2, :] = xu[6 * columns + c : 6 * columns + c + 1, :]
        halo_s[c], halo_d[c] = z_pair(split(row_ref[...]))

    row = lax.broadcasted_iota(jnp.int32, (nb, columns, LANES), 1)

    def node_plane(values, at):
        sums, diffs, sums_next, diffs_next = [], [], [], []
        for c in range(6):
            s, d = z_pair(values[c])
            sums.append(s)
            diffs.append(d)
            hs = halo_s[c, :, pl.ds(at, 1), :]
            hd = halo_d[c, :, pl.ds(at, 1), :]
            sums_next.append(jnp.where(row == columns - 1, hs, pltpu.roll(s, columns - 1, 1)))
            diffs_next.append(jnp.where(row == columns - 1, hd, pltpu.roll(d, columns - 1, 1)))
        return node_terms(sums, diffs, sums_next, diffs_next)

    def keep_nodes(terms):
        for c in range(6):
            for t in range(3):
                node_ref[c, t] = terms[c][t]

    def kept_nodes():
        return [tuple(node_ref[c, t] for t in range(3)) for c in range(6)]

    def keep_elements(factors):
        for m in range(3):
            for t in range(7):
                elem_ref[m, t] = factors[m][t]

    def kept_elements():
        return [[elem_ref[m, t] for t in range(7)] for m in range(3)]

    def write_plane(before, after, i):
        weight = (time_step / 64.0) / split(mass_ref[i])
        for m, (a, b, c, e) in enumerate(gathered_x(before, after)):
            ab, ce = a + b, c + e
            p = (a - b) + jnp.where(row == 0, 0.0, pltpu.roll(ab, 1, 1))
            r = (c - e) + jnp.where(row == 0, 0.0, pltpu.roll(ce, 1, 1))
            result = split(v_ref[m, i]) - along_z(p, r) * weight
            for k in range(nb):
                out_ref[m, i, :, k * LANES : (k + 1) * LANES] = result[k]

    def own_nodes(i):
        return [split(u_ref[c, i]) for c in range(3)] + [split(v_ref[c, i]) for c in range(3)]

    keep_nodes(node_plane([split(below(c)) for c in range(6)], 0))
    current = node_plane(own_nodes(0), 1)
    keep_elements(
        element_terms(
            kept_nodes(), current, [split(below(6 + c)) for c in range(6)], split(below(12))
        )
    )
    keep_nodes(current)

    def step(i, upper):
        factors = element_terms(
            kept_nodes(), upper, [split(stress_ref[c, i - 1]) for c in range(6)], split(hour_ref[i - 1])
        )
        write_plane(kept_elements(), factors, i - 1)
        keep_elements(factors)
        keep_nodes(upper)

    def loop(i, carry):
        step(i, node_plane(own_nodes(i), i + 1))
        return carry

    lax.fori_loop(1, planes, loop, 0)
    step(planes, node_plane([split(above(c)) for c in range(6)], planes + 1))


def final_body(
    nspace, capacity, pack,
    base_ref, mass_ref, table_ref, route_ref, left_ref, out_hbm, rows_ref, out_ref, sems,
):
    planes, columns, depth = base_ref.shape[1:]
    offset = (lax.axis_index("space") % pack) * capacity
    (contact,) = looked_up(table_ref, [route_ref[...]], capacity, offset, nspace)
    rows_ref[...] = jnp.zeros(rows_ref.shape, jnp.float32)
    lane = lax.broadcasted_iota(jnp.int32, (planes, columns, LANES), 2)
    row = lax.broadcasted_iota(jnp.int32, (columns, LANES), 0)
    weights = [time_step / mass_ref[:, :, k : k + LANES] for k in range(0, depth, LANES)]
    low_weight = jnp.where(lane == 0, weights[0], 0.0)
    high_weight = jnp.where(lane == LANES - 1, weights[-1], 0.0)
    copies = []
    for m in range(3):
        rows_ref[m, 0:1, :] = contact[m][0:1]
        rows_ref[m, LANES - 1 : LANES, :] = contact[m][1:2]
        turned = rows_ref[m].T.reshape(planes, columns, LANES)
        for k in range(0, depth, LANES):
            left = jnp.stack(
                [
                    jnp.where(row == 0, left_ref[m, i : i + 1, k : k + LANES] * (1.0 / 64.0), 0.0)
                    for i in range(planes)
                ]
            )
            value = base_ref[m, :, :, k : k + LANES] - left * weights[k // LANES]
            if k == 0:
                value = value + low_weight * turned
            if k == depth - LANES:
                value = value + high_weight * turned
            out_ref[m, :, :, k : k + LANES] = value
        copies.append(pltpu.make_async_copy(out_ref.at[m], out_hbm.at[m], sems.at[m]))
        copies[m].start()
    for copy in copies:
        copy.wait()


def local(
    displacement,
    velocity,
    stress,
    hourglass,
    mass,
    contact_route,
    pair_nodes,
    pair_diagonals,
    pair_gap,
    pair_stiffness,
):
    planes, columns, depth = displacement.shape[1:]
    nspace = lax.axis_size("space")
    surf_count = 2 * planes * columns
    pairs = pair_nodes.shape[1]
    capacity, pack, blocks = layout(nspace, surf_count)
    f32 = jnp.float32
    lines = pairs // LANES

    def sized(*shape):
        return jax.ShapeDtypeStruct(shape, f32)

    message = sized(nspace, 8, LANES)
    small = (pair_nodes, pair_diagonals, pair_gap.reshape(lines, LANES))
    small += (pair_stiffness.reshape(lines, LANES),)
    kept = (displacement, velocity, stress, hourglass, mass) + small
    outgoing, ydn, sides, *kept = kernel_call(
        functools.partial(first_body, capacity, pack, blocks),
        (displacement, contact_route.reshape(1, surf_count)) + kept[1:],
        (
            pltpu.HBM(message.shape, f32),
            sized(6, planes, depth),
            jax.ShapeDtypeStruct((2, surf_count // 2), jnp.int32),
            *(jax.ShapeDtypeStruct(one.shape, one.dtype) for one in kept),
        ),
        [
            pltpu.VMEM(message.shape, f32),
            pltpu.VMEM((8, surf_count), f32),
            pltpu.VMEM((1, surf_count), jnp.int32),
            pltpu.SemaphoreType.DMA((len(kept) + 1,)),
            pltpu.SemaphoreType.DMA,
        ],
        hbm_inputs=len(kept) + 1,
    )
    fields, (pair_nodes, pair_diagonals, gap, stiffness) = kept[:5], kept[5:]
    yu = shifted(ydn, "slab", -1)
    received = exchanged(outgoing)
    xdn, xup = kernel_call(
        second_body,
        (*fields[:4], yu),
        (
            sized((6 * columns + 6 + 7) // 8 * 8, depth),
            sized((13 * columns + 6 + 7) // 8 * 8, depth),
        ),
    )
    xu = shifted(xdn, "space", -1)
    xd = shifted(xup, "space", 1)
    slots = (nspace * capacity + 15) // 16 * 16
    matrix, nodes, diagonals = kernel_call(
        matrix_body,
        (pair_nodes, pair_diagonals),
        (
            jax.ShapeDtypeStruct((slots, pairs), jnp.bfloat16),
            jax.ShapeDtypeStruct((5, lines, LANES), jnp.int32),
            sized(6, lines, LANES),
        ),
    )
    slot_force = kernel_call(
        functools.partial(pair_body, nspace, capacity, pack, blocks),
        (received, nodes, diagonals, gap, stiffness, matrix),
        pltpu.HBM(message.shape, f32),
        [
            pltpu.VMEM((8, pairs), f32),
            pltpu.VMEM(message.shape, f32),
            pltpu.SemaphoreType.DMA,
        ],
    )
    returned = exchanged(slot_force)

    nb = depth // LANES
    rows = (planes + 2 + 7) // 8 * 8
    beyond = kernel_call(
        edge_body,
        (*fields[:4], yu, xu, xd),
        sized(3, planes, depth),
        [pltpu.VMEM((rows, depth), f32)],
    )
    left = shifted(beyond, "slab", 1)
    base = kernel_call(
        element_body,
        (*fields, yu, xu, xd),
        sized(*displacement.shape),
        [
            pltpu.VMEM((rows, depth), f32),
            pltpu.VMEM((6, nb, rows, LANES), f32),
            pltpu.VMEM((6, nb, rows, LANES), f32),
            pltpu.VMEM((6, 3, nb, columns, LANES), f32),
            pltpu.VMEM((3, 7, nb, columns, LANES), f32),
        ],
    )

    return kernel_call(
        functools.partial(final_body, nspace, capacity, pack),
        (base, fields[4], returned, sides, left),
        pltpu.HBM(displacement.shape, f32),
        [
            pltpu.VMEM((3, LANES, LANES), f32),
            pltpu.VMEM(displacement.shape, f32),
            pltpu.SemaphoreType.DMA((3,)),
        ],
    )


def solution(mesh):
    in_specs = (
        P(None, "space", "slab", None),
        P(None, "space", "slab", None),
        P(None, "space", "slab", None),
        P("space", "slab", None),
        P("space", "slab", None),
        P(("space", "slab")),
        P(None, ("space", "slab")),
        P(None, ("space", "slab")),
        P(("space", "slab")),
        P(("space", "slab")),
    )
    out_specs = P(None, "space", "slab", None)
    return jax.shard_map(local, mesh=mesh, in_specs=in_specs, out_specs=out_specs, check_vma=False)
```

```python
import functools

import jax
import jax.numpy as jnp
from jax import lax
from jax.experimental import pallas as pl
from jax.experimental.pallas import tpu as pltpu
from jax.sharding import PartitionSpec as P


time_step = 0.5
LANES = 128
VOIGT = [[0, 5, 4], [5, 1, 3], [4, 3, 2]]


def shifted(value, axis, steps):
    count = lax.axis_size(axis)
    return lax.ppermute(value, axis, [(at, (at + steps) % count) for at in range(count)])


def exchanged(value):
    return lax.all_to_all(value, "space", split_axis=0, concat_axis=0, tiled=True)


def kernel_call(body, inputs, outs, scratch=(), hbm_inputs=0):
    spaces = [pltpu.HBM if at < hbm_inputs else pltpu.VMEM for at in range(len(inputs))]
    inputs = [pltpu.with_memory_space_constraint(*pair) for pair in zip(inputs, spaces)]

    def placed(out):
        if isinstance(out, jax.ShapeDtypeStruct):
            return pltpu.VMEM(out.shape, out.dtype)
        return out

    outs = tuple(placed(out) for out in outs) if isinstance(outs, tuple) else placed(outs)
    return pl.pallas_call(
        body,
        out_shape=outs,
        in_specs=[pl.BlockSpec(memory_space=one) for one in spaces],
        out_specs=jax.tree.map(lambda out: pl.BlockSpec(memory_space=out.memory_space), outs),
        scratch_shapes=list(scratch),
        compiler_params=pltpu.CompilerParams(vmem_limit_bytes=16 << 20),
    )(*inputs)


def contract_lanes(lhs, rhs):
    return lax.dot_general(lhs, rhs, (((1,), (1,)), ((), ())), preferred_element_type=jnp.float32)


def layout(nspace, surf_count):
    capacity = max(2, (3 * surf_count // 2 + nspace - 1) // nspace)
    pack = max(1, min(LANES // capacity, nspace // 8))
    while nspace % pack:
        pack -= 1
    return capacity, pack, nspace // pack


def block_of(slots, width, blocks):
    block = jnp.zeros_like(slots)
    for b in range(1, blocks):
        block = block + jnp.where(slots >= b * width, 1, 0)
    return block, slots - block * width


def parts_of(rows):
    high = rows.astype(jnp.bfloat16).astype(jnp.float32)
    rest = rows - high
    middle = rest.astype(jnp.bfloat16).astype(jnp.float32)
    return [high, middle, rest - middle]


def places(place, width):
    rows = (width + 15) // 16 * 16
    count = place.shape[1]
    at = lax.broadcasted_iota(jnp.int32, (rows, count), 0)
    return jnp.where(at == place, 1.0, 0.0).astype(jnp.bfloat16)


def spread(parts, block, blocks):
    return [
        jnp.where(block == b, part, 0.0).astype(jnp.bfloat16)
        for part in parts
        for b in range(blocks)
    ]


def write_messages(out_ref, got, pack, blocks):
    for b in range(blocks):
        at = [(part * blocks + b) * 8 for part in range(3)]
        total = got[at[0] : at[0] + 8] + got[at[1] : at[1] + 8] + got[at[2] : at[2] + 8]
        for q in range(pack):
            out_ref[b * pack + q, :, 0 : total.shape[1]] = total


def first_body(
    capacity, pack, blocks, u_hbm, route_hbm, v_hbm, *rest,
):
    hbm, rest = (u_hbm, route_hbm, v_hbm) + rest[:7], rest[7:]
    message_hbm, ydn, xdn, xup, sides_ref, u_ref, v_ref, stress_ref, hour_ref = rest[:9]
    out_ref, rows_ref, route_ref, sems, message_sem = rest[-5:]
    targets = (u_ref, route_ref, v_ref, stress_ref, hour_ref) + rest[9:-5]
    copies = [
        pltpu.make_async_copy(source, target, sems.at[at])
        for at, (source, target) in enumerate(zip(hbm, targets))
    ]
    for copy in copies:
        copy.start()
    out_ref[...] = jnp.zeros(out_ref.shape, jnp.float32)
    rows_ref[...] = jnp.zeros(rows_ref.shape, jnp.float32)
    copies[0].wait()
    copies[1].wait()
    planes, columns, depth = u_ref.shape[1:]
    side = planes * columns
    lane = lax.broadcasted_iota(jnp.int32, (side, LANES), 1)
    for c in range(3):
        bottom = u_ref[c, :, :, 0:LANES].reshape(side, LANES)
        top = u_ref[c, :, :, depth - LANES : depth].reshape(side, LANES)
        both = jnp.where(lane == LANES - 1, top, bottom).T
        rows_ref[c : c + 1, 0:side] = both[0:1]
        rows_ref[c : c + 1, side : 2 * side] = both[LANES - 1 : LANES]
    width = pack * capacity
    route = route_ref[...]
    block, place = block_of(route, width, blocks)
    entries = spread(parts_of(rows_ref[...]), block, blocks)
    got = contract_lanes(jnp.concatenate(entries, 0), places(place, width))
    write_messages(out_ref, got, pack, blocks)
    message = pltpu.make_async_copy(out_ref, message_hbm, message_sem)
    message.start()
    sides_ref[0:1, :] = route[:, 0:side]
    sides_ref[1:2, :] = route[:, side : 2 * side]
    for copy in copies[2:5]:
        copy.wait()
    for c in range(13):
        ref = component(u_ref, v_ref, stress_ref, hour_ref, c)
        xup[c * columns : (c + 1) * columns, :] = ref[planes - 1]
        if c < 6:
            xdn[c * columns : (c + 1) * columns, :] = ref[0]
            ydn[c] = ref[:, 0, :]
    for copy in copies[5:]:
        copy.wait()
    message.wait()


def component(u_ref, v_ref, stress_ref, hour_ref, c):
    if c < 3:
        return u_ref.at[c]
    if c < 6:
        return v_ref.at[c - 3]
    if c < 12:
        return stress_ref.at[c - 6]
    return hour_ref


def corner_body(columns, xu, xd, out_ref):
    out_ref[...] = jnp.zeros(out_ref.shape, jnp.float32)
    for c in range(6):
        out_ref[c : c + 1, :] = xd[c * columns : c * columns + 1, :]
        out_ref[8 + c : 9 + c, :] = xu[c * columns : c * columns + 1, :]


def matrix_body(nodes_ref, diag_ref, matrix_ref, lines_ref, diag_lines_ref):
    pairs = nodes_ref.shape[1]
    group = 16

    def rows(g, carry):
        start = pl.multiple_of(g * group, group)
        slot = lax.broadcasted_iota(jnp.int32, (group, pairs), 0) + start
        total = jnp.where(nodes_ref[0:1, :] == slot, 1.0, 0.0)
        for j in range(1, 5):
            total = total - jnp.where(nodes_ref[j : j + 1, :] == slot, 0.25, 0.0)
        matrix_ref[pl.ds(start, group), :] = total.astype(jnp.bfloat16)
        return carry

    lax.fori_loop(0, matrix_ref.shape[0] // group, rows, 0)
    for r in range(pairs // LANES):
        for j in range(5):
            lines_ref[j, r : r + 1, :] = nodes_ref[j : j + 1, r * LANES : (r + 1) * LANES]
        for c in range(6):
            diag_lines_ref[c, r : r + 1, :] = diag_ref[c : c + 1, r * LANES : (r + 1) * LANES]


def looked_up(table_ref, slots, capacity, offset, count):
    shape = slots[0].shape

    def step(s, found):
        shift = s * capacity - offset
        result = []
        for slot, old in zip(slots, found):
            here = (slot >= s * capacity) & (slot < (s + 1) * capacity)
            index = (slot - shift) & (LANES - 1)
            new = []
            for c in range(3):
                row = jnp.broadcast_to(table_ref[s, c : c + 1, :], shape)
                new.append(jnp.where(here, jnp.take_along_axis(row, index, axis=1), old[c]))
            result.append(tuple(new))
        return tuple(result)

    zero = jnp.zeros(shape, jnp.float32)
    found = tuple((zero, zero, zero) for _ in slots)
    if count <= 16:
        for s in range(count):
            found = step(s, found)
        return found
    return lax.fori_loop(0, count, step, found)


def pair_body(
    nspace, capacity, pack, blocks,
    table_ref, nodes_ref, diag_ref, gap_ref, stiff_ref, matrix_ref, out_hbm, rows_ref, out_ref, sem,
):
    offset = (lax.axis_index("space") % pack) * capacity
    picked = looked_up(table_ref, [nodes_ref[j] for j in range(5)], capacity, offset, nspace)
    slave = picked[0]
    first = [diag_ref[c] + picked[3][c] - picked[1][c] for c in range(3)]
    second = [diag_ref[3 + c] + picked[4][c] - picked[2][c] for c in range(3)]
    normal = [
        first[(c + 1) % 3] * second[(c + 2) % 3] - first[(c + 2) % 3] * second[(c + 1) % 3]
        for c in range(3)
    ]
    gap = gap_ref[...]
    for c in range(3):
        centre = (picked[1][c] + picked[2][c] + picked[3][c] + picked[4][c]) * 0.25
        gap = gap + (slave[c] - centre) * normal[c]
    push = stiff_ref[...] * jnp.maximum(-gap, 0.0)
    out_ref[...] = jnp.zeros(out_ref.shape, jnp.float32)
    rows_ref[...] = jnp.zeros(rows_ref.shape, jnp.float32)
    for c in range(3):
        force = push * normal[c]
        for r in range(force.shape[0]):
            rows_ref[c : c + 1, r * LANES : (r + 1) * LANES] = force[r : r + 1]
    parts = [part.astype(jnp.bfloat16) for part in parts_of(rows_ref[...])]
    got = contract_lanes(jnp.concatenate(parts, 0), matrix_ref[...])
    total = got[0:8] + got[8:16] + got[16:24]
    width = pack * capacity
    for b in range(blocks):
        for q in range(pack):
            out_ref[b * pack + q, :, 0:width] = total[:, b * width : (b + 1) * width]
    copy = pltpu.make_async_copy(out_ref, out_hbm, sem)
    copy.start()
    copy.wait()


def split(value):
    return jnp.stack([value[:, at : at + LANES] for at in range(0, value.shape[1], LANES)])


def z_pair(f):
    lane = lax.broadcasted_iota(jnp.int32, f.shape, 2)
    turned = pltpu.roll(f, LANES - 1, 2)
    after = jnp.concatenate([turned[1:], turned[:1]], 0)
    upper = jnp.where(lane == LANES - 1, after, turned)
    return f + upper, upper - f


def node_terms(sums, diffs, sums_next, diffs_next):
    result = []
    for c in range(6):
        s0, s1, d0, d1 = sums[c], sums_next[c], diffs[c], diffs_next[c]
        if c < 3:
            result.append((s0 + s1, s1 - s0, d0 + d1))
        else:
            result.append((d1 - d0, d0 + d1, s1 - s0))
    return result


def element_terms(lower, upper, stress, hour):
    eight = []
    for m in range(3):
        row = [
            upper[m][0] - lower[m][0],
            lower[m][1] + upper[m][1],
            lower[m][2] + upper[m][2],
        ]
        row[m] = row[m] + 4.0
        eight.append(row)
    cof = [
        [
            eight[(m + 1) % 3][(n + 1) % 3] * eight[(m + 2) % 3][(n + 2) % 3]
            - eight[(m + 1) % 3][(n + 2) % 3] * eight[(m + 2) % 3][(n + 1) % 3]
            for n in range(3)
        ]
        for m in range(3)
    ]
    hour = hour * 64.0
    result = []
    for m in range(3):
        line = [
            stress[VOIGT[m][0]] * cof[0][n]
            + stress[VOIGT[m][1]] * cof[1][n]
            + stress[VOIGT[m][2]] * cof[2][n]
            for n in range(3)
        ]
        low, up = lower[3 + m], upper[3 + m]
        line.append(hour * (low[0] + up[0]))
        line.append(hour * (up[1] - low[1]))
        line.append(hour * (up[2] - low[2]))
        line.append(hour * (up[0] - low[0]))
        result.append(line)
    return result


def gathered_x(before, after):
    result = []
    for m in range(3):
        p, n = before[m], after[m]
        result.append(
            (
                p[0] - n[0],
                (p[1] + n[1]) + (p[5] - n[5]),
                (p[2] + n[2]) + (p[4] - n[4]),
                (p[3] + n[3]) + (p[6] - n[6]),
            )
        )
    return result


def along_z(p, r):
    lane = lax.broadcasted_iota(jnp.int32, p.shape, 2)
    block = lax.broadcasted_iota(jnp.int32, p.shape, 0)
    nb = p.shape[0]
    up = pltpu.roll(p + r, 1, 2)
    before_up = jnp.concatenate([jnp.zeros_like(up[:1]), up[:-1]], 0)
    last = (lane == LANES - 1) & (block == nb - 1)
    return jnp.where(lane == 0, before_up, up) + jnp.where(last, 0.0, p - r)


def edge_body(u_ref, v_ref, stress_ref, hour_ref, yu, xu, xd, corner, beyond_ref, row_ref):
    planes, columns, _ = u_ref.shape[1:]
    rows = row_ref.shape[0]
    row_ref[...] = jnp.zeros(row_ref.shape, jnp.float32)

    def assembled(first, middle, last):
        row_ref[0:1, :] = first
        row_ref[1 : planes + 1, :] = middle
        if last is not None:
            row_ref[planes + 1 : planes + 2, :] = last
        return split(row_ref[...])

    def line(ref, at):
        return ref[at : at + 1, :]

    def following(q):
        return pltpu.roll(q, rows - 1, 1)

    def own(c):
        middle = component(u_ref, v_ref, stress_ref, hour_ref, c)[:, columns - 1, :]
        at = c * columns + columns - 1
        return assembled(line(xd, at), middle, line(xu, at) if c < 6 else None)

    own_s, own_d, next_s, next_d = [], [], [], []
    for c in range(6):
        s, d = z_pair(own(c))
        own_s.append(s)
        own_d.append(d)
        s, d = z_pair(assembled(line(corner, c), yu[c], line(corner, 8 + c)))
        next_s.append(s)
        next_d.append(d)
    lower = node_terms(own_s, own_d, next_s, next_d)
    upper = [tuple(following(q) for q in terms) for terms in lower]
    factors = element_terms(lower, upper, [own(6 + c) for c in range(6)], own(12))
    after = [[following(q) for q in terms] for terms in factors]
    for m, (a, b, c, e) in enumerate(gathered_x(factors, after)):
        force = along_z(a + b, c + e)[:, 0:planes]
        for k in range(force.shape[0]):
            beyond_ref[m, :, k * LANES : (k + 1) * LANES] = force[k]


def node_plane(values, halo_s, halo_d):
    row = lax.broadcasted_iota(jnp.int32, values[0].shape, 1)
    end = values[0].shape[1] - 1
    sums, diffs, sums_next, diffs_next = [], [], [], []
    for c in range(6):
        s, d = z_pair(values[c])
        sums.append(s)
        diffs.append(d)
        sums_next.append(jnp.where(row == end, halo_s[c], pltpu.roll(s, end, 1)))
        diffs_next.append(jnp.where(row == end, halo_d[c], pltpu.roll(d, end, 1)))
    return node_terms(sums, diffs, sums_next, diffs_next)


def kept_nodes(node_ref, i):
    return [tuple(node_ref[i, c, t] for t in range(3)) for c in range(6)]


def kept_elements(elem_ref, i):
    return [[elem_ref[i, m, t] for t in range(7)] for m in range(3)]


def new_velocity(before, after, velocity, mass):
    row = lax.broadcasted_iota(jnp.int32, mass.shape, 1)
    weight = (time_step / 64.0) / mass
    result = []
    for m, (a, b, c, e) in enumerate(gathered_x(before, after)):
        p = (a - b) + jnp.where(row == 0, 0.0, pltpu.roll(a + b, 1, 1))
        r = (c - e) + jnp.where(row == 0, 0.0, pltpu.roll(c + e, 1, 1))
        result.append(velocity[m] - along_z(p, r) * weight)
    return result


def steps(start, stop, unroll, body):
    count = (stop - start) // unroll

    def several(t, carry):
        for k in range(unroll):
            body(start + t * unroll + k)
        return carry

    lax.fori_loop(0, count, several, 0)
    for i in range(start + count * unroll, stop):
        body(i)


def inner_body(
    unroll, u_ref, v_ref, stress_ref, hour_ref, mass_ref, yu, out_ref, node_ref, elem_ref, halo_s, halo_d
):
    planes, _, depth = u_ref.shape[1:]
    nb = depth // LANES
    for c in range(6):
        halo_s[c], halo_d[c] = z_pair(split(yu[c]))

    def nodes(i):
        values = [split(u_ref[c, i]) for c in range(3)] + [split(v_ref[c, i]) for c in range(3)]
        terms = node_plane(
            values,
            [halo_s[c, :, pl.ds(i, 1), :] for c in range(6)],
            [halo_d[c, :, pl.ds(i, 1), :] for c in range(6)],
        )
        for c in range(6):
            for t in range(3):
                node_ref[i, c, t] = terms[c][t]

    def elements(i):
        factors = element_terms(
            kept_nodes(node_ref, i),
            kept_nodes(node_ref, i + 1),
            [split(stress_ref[c, i]) for c in range(6)],
            split(hour_ref[i]),
        )
        for m in range(3):
            for t in range(7):
                elem_ref[i, m, t] = factors[m][t]

    def forces(i):
        result = new_velocity(
            kept_elements(elem_ref, i - 1),
            kept_elements(elem_ref, i),
            [split(v_ref[m, i]) for m in range(3)],
            split(mass_ref[i]),
        )
        for m in range(3):
            for k in range(nb):
                out_ref[m, i, :, k * LANES : (k + 1) * LANES] = result[m][k]

    steps(0, planes, unroll, nodes)
    steps(0, planes - 1, unroll, elements)
    steps(1, planes - 1, unroll, forces)


def outer_body(
    v_ref, stress_ref, hour_ref, mass_ref, node_ref, elem_ref, xu, xd, corner, out_ref
):
    planes, columns, depth = v_ref.shape[1:]
    last = planes - 1

    def part(ref, c):
        return split(ref[c * columns : (c + 1) * columns, :])

    def plane_terms(ref, at):
        halo_s, halo_d = z_pair(split(corner[at : at + 8, :]))
        return node_plane(
            [part(ref, c) for c in range(6)],
            [halo_s[:, c : c + 1] for c in range(6)],
            [halo_d[:, c : c + 1] for c in range(6)],
        )

    below = element_terms(
        plane_terms(xd, 0),
        kept_nodes(node_ref, 0),
        [part(xd, 6 + c) for c in range(6)],
        part(xd, 12),
    )
    above = element_terms(
        kept_nodes(node_ref, last),
        plane_terms(xu, 8),
        [split(stress_ref[c, last]) for c in range(6)],
        split(hour_ref[last]),
    )
    ends = (
        (0, below, kept_elements(elem_ref, 0)),
        (last, kept_elements(elem_ref, last - 1), above),
    )
    for at, (i, before, after) in enumerate(ends):
        velocity = [split(v_ref[m, i]) for m in range(3)]
        result = new_velocity(before, after, velocity, split(mass_ref[i]))
        for m in range(3):
            for k in range(depth // LANES):
                out_ref[m, at, :, k * LANES : (k + 1) * LANES] = result[m][k]


def final_body(
    nspace, capacity, pack,
    base_ref, outer_ref, mass_ref, table_ref, route_ref, left_ref, out_hbm, rows_ref, out_ref, sems,
):
    planes, columns, depth = base_ref.shape[1:]
    offset = (lax.axis_index("space") % pack) * capacity
    (contact,) = looked_up(table_ref, [route_ref[...]], capacity, offset, nspace)
    rows_ref[...] = jnp.zeros(rows_ref.shape, jnp.float32)
    lane = lax.broadcasted_iota(jnp.int32, (planes, columns, LANES), 2)
    row = lax.broadcasted_iota(jnp.int32, (columns, LANES), 0)
    weights = [time_step / mass_ref[:, :, k : k + LANES] for k in range(0, depth, LANES)]
    low_weight = jnp.where(lane == 0, weights[0], 0.0)
    high_weight = jnp.where(lane == LANES - 1, weights[-1], 0.0)
    copies = []
    for m in range(3):
        rows_ref[m, 0:1, :] = contact[m][0:1]
        rows_ref[m, LANES - 1 : LANES, :] = contact[m][1:2]
        turned = rows_ref[m].T.reshape(planes, columns, LANES)
        for k in range(0, depth, LANES):
            left = jnp.stack(
                [
                    jnp.where(row == 0, left_ref[m, i : i + 1, k : k + LANES] * (1.0 / 64.0), 0.0)
                    for i in range(planes)
                ]
            )
            value = jnp.concatenate(
                [
                    outer_ref[m, 0:1, :, k : k + LANES],
                    base_ref[m, 1 : planes - 1, :, k : k + LANES],
                    outer_ref[m, 1:2, :, k : k + LANES],
                ]
            )
            value = value - left * weights[k // LANES]
            if k == 0:
                value = value + low_weight * turned
            if k == depth - LANES:
                value = value + high_weight * turned
            out_ref[m, :, :, k : k + LANES] = value
        copies.append(pltpu.make_async_copy(out_ref.at[m], out_hbm.at[m], sems.at[m]))
        copies[m].start()
    for copy in copies:
        copy.wait()


def local(
    displacement,
    velocity,
    stress,
    hourglass,
    mass,
    contact_route,
    pair_nodes,
    pair_diagonals,
    pair_gap,
    pair_stiffness,
):
    planes, columns, depth = displacement.shape[1:]
    nspace = lax.axis_size("space")
    surf_count = 2 * planes * columns
    pairs = pair_nodes.shape[1]
    capacity, pack, blocks = layout(nspace, surf_count)
    f32 = jnp.float32
    lines = pairs // LANES

    def sized(*shape):
        return jax.ShapeDtypeStruct(shape, f32)

    message = sized(nspace, 8, LANES)
    small = (pair_nodes, pair_diagonals, pair_gap.reshape(lines, LANES))
    small += (pair_stiffness.reshape(lines, LANES),)
    kept = (displacement, velocity, stress, hourglass, mass) + small
    outgoing, ydn, xdn, xup, sides, *kept = kernel_call(
        functools.partial(first_body, capacity, pack, blocks),
        (displacement, contact_route.reshape(1, surf_count)) + kept[1:],
        (
            pltpu.HBM(message.shape, f32),
            sized(6, planes, depth),
            sized(6 * columns, depth),
            sized(13 * columns, depth),
            jax.ShapeDtypeStruct((2, surf_count // 2), jnp.int32),
            *(jax.ShapeDtypeStruct(one.shape, one.dtype) for one in kept),
        ),
        [
            pltpu.VMEM(message.shape, f32),
            pltpu.VMEM((8, surf_count), f32),
            pltpu.VMEM((1, surf_count), jnp.int32),
            pltpu.SemaphoreType.DMA((len(kept) + 1,)),
            pltpu.SemaphoreType.DMA,
        ],
        hbm_inputs=len(kept) + 1,
    )
    fields, (pair_nodes, pair_diagonals, gap, stiffness) = kept[:5], kept[5:]
    received = exchanged(outgoing)
    yu = shifted(ydn, "slab", -1)
    xu = shifted(xdn, "space", -1)
    xd = shifted(xup, "space", 1)
    slots = (nspace * capacity + 15) // 16 * 16
    matrix, nodes, diagonals = kernel_call(
        matrix_body,
        (pair_nodes, pair_diagonals),
        (
            jax.ShapeDtypeStruct((slots, pairs), jnp.bfloat16),
            jax.ShapeDtypeStruct((5, lines, LANES), jnp.int32),
            sized(6, lines, LANES),
        ),
    )
    slot_force = kernel_call(
        functools.partial(pair_body, nspace, capacity, pack, blocks),
        (received, nodes, diagonals, gap, stiffness, matrix),
        pltpu.HBM(message.shape, f32),
        [
            pltpu.VMEM((8, pairs), f32),
            pltpu.VMEM(message.shape, f32),
            pltpu.SemaphoreType.DMA,
        ],
    )
    returned = exchanged(slot_force)

    corner = kernel_call(functools.partial(corner_body, columns), (xu, xd), sized(16, depth))
    corner = shifted(corner, "slab", -1)
    nb = depth // LANES
    base, node, elem = kernel_call(
        functools.partial(inner_body, 2),
        (*fields, yu),
        (
            sized(*displacement.shape),
            sized(planes, 6, 3, nb, columns, LANES),
            sized(planes - 1, 3, 7, nb, columns, LANES),
        ),
        [
            pltpu.VMEM((6, nb, planes, LANES), f32),
            pltpu.VMEM((6, nb, planes, LANES), f32),
        ],
    )
    rows = (planes + 2 + 7) // 8 * 8
    beyond = kernel_call(
        edge_body,
        (*fields[:4], yu, xu, xd, corner),
        sized(3, planes, depth),
        [pltpu.VMEM((rows, depth), f32)],
    )
    left = shifted(beyond, "slab", 1)
    outer = kernel_call(
        outer_body, (*fields[1:], node, elem, xu, xd, corner), sized(3, 2, columns, depth)
    )

    return kernel_call(
        functools.partial(final_body, nspace, capacity, pack),
        (base, outer, fields[4], returned, sides, left),
        pltpu.HBM(displacement.shape, f32),
        [
            pltpu.VMEM((3, LANES, LANES), f32),
            pltpu.VMEM(displacement.shape, f32),
            pltpu.SemaphoreType.DMA((3,)),
        ],
    )


def solution(mesh):
    in_specs = (
        P(None, "space", "slab", None),
        P(None, "space", "slab", None),
        P(None, "space", "slab", None),
        P("space", "slab", None),
        P("space", "slab", None),
        P(("space", "slab")),
        P(None, ("space", "slab")),
        P(None, ("space", "slab")),
        P(("space", "slab")),
        P(("space", "slab")),
    )
    out_specs = P(None, "space", "slab", None)
    return jax.shard_map(local, mesh=mesh, in_specs=in_specs, out_specs=out_specs, check_vma=False)
```

```python
import functools

import jax
import jax.numpy as jnp
from jax import lax
from jax.experimental import pallas as pl
from jax.experimental.pallas import tpu as pltpu
from jax.sharding import PartitionSpec as P


time_step = 0.5
LANES = 128
VOIGT = [[0, 5, 4], [5, 1, 3], [4, 3, 2]]


def shifted(value, axis, steps):
    count = lax.axis_size(axis)
    return lax.ppermute(value, axis, [(at, (at + steps) % count) for at in range(count)])


def exchanged(value):
    return lax.all_to_all(value, "space", split_axis=0, concat_axis=0, tiled=True)


def kernel_call(body, inputs, outs, scratch=(), hbm_inputs=0):
    spaces = [pltpu.HBM if at < hbm_inputs else pltpu.VMEM for at in range(len(inputs))]
    inputs = [pltpu.with_memory_space_constraint(*pair) for pair in zip(inputs, spaces)]

    def placed(out):
        if isinstance(out, jax.ShapeDtypeStruct):
            return pltpu.VMEM(out.shape, out.dtype)
        return out

    outs = tuple(placed(out) for out in outs) if isinstance(outs, tuple) else placed(outs)
    return pl.pallas_call(
        body,
        out_shape=outs,
        in_specs=[pl.BlockSpec(memory_space=one) for one in spaces],
        out_specs=jax.tree.map(lambda out: pl.BlockSpec(memory_space=out.memory_space), outs),
        scratch_shapes=list(scratch),
        compiler_params=pltpu.CompilerParams(vmem_limit_bytes=16 << 20),
    )(*inputs)


def contract_lanes(lhs, rhs):
    return lax.dot_general(lhs, rhs, (((1,), (1,)), ((), ())), preferred_element_type=jnp.float32)


def layout(nspace, surf_count):
    capacity = max(2, (3 * surf_count // 2 + nspace - 1) // nspace)
    pack = max(1, min(LANES // capacity, nspace // 8))
    while nspace % pack:
        pack -= 1
    return capacity, pack, nspace // pack


def block_of(slots, width, blocks):
    block = jnp.zeros_like(slots)
    for b in range(1, blocks):
        block = block + jnp.where(slots >= b * width, 1, 0)
    return block, slots - block * width


def parts_of(rows):
    high = rows.astype(jnp.bfloat16).astype(jnp.float32)
    rest = rows - high
    middle = rest.astype(jnp.bfloat16).astype(jnp.float32)
    return [high, middle, rest - middle]


def places(place, width):
    rows = (width + 15) // 16 * 16
    count = place.shape[1]
    at = lax.broadcasted_iota(jnp.int32, (rows, count), 0)
    return jnp.where(at == place, 1.0, 0.0).astype(jnp.bfloat16)


def spread(parts, block, blocks):
    return [
        jnp.where(block == b, part, 0.0).astype(jnp.bfloat16)
        for part in parts
        for b in range(blocks)
    ]


def write_messages(out_ref, got, pack, blocks):
    for b in range(blocks):
        at = [(part * blocks + b) * 8 for part in range(3)]
        total = got[at[0] : at[0] + 8] + got[at[1] : at[1] + 8] + got[at[2] : at[2] + 8]
        for q in range(pack):
            out_ref[b * pack + q, :, 0 : total.shape[1]] = total


def first_body(
    capacity, pack, blocks, u_hbm, route_hbm, v_hbm, *rest,
):
    hbm, rest = (u_hbm, route_hbm, v_hbm) + rest[:7], rest[7:]
    message_hbm, ydn, xdn, xup, sides_ref, u_ref, v_ref, stress_ref, hour_ref = rest[:9]
    out_ref, rows_ref, route_ref, sems, message_sem = rest[-5:]
    targets = (u_ref, route_ref, v_ref, stress_ref, hour_ref) + rest[9:-5]
    copies = [
        pltpu.make_async_copy(source, target, sems.at[at])
        for at, (source, target) in enumerate(zip(hbm, targets))
    ]
    for copy in copies:
        copy.start()
    out_ref[...] = jnp.zeros(out_ref.shape, jnp.float32)
    rows_ref[...] = jnp.zeros(rows_ref.shape, jnp.float32)
    copies[0].wait()
    copies[1].wait()
    planes, columns, depth = u_ref.shape[1:]
    side = planes * columns
    lane = lax.broadcasted_iota(jnp.int32, (side, LANES), 1)
    for c in range(3):
        bottom = u_ref[c, :, :, 0:LANES].reshape(side, LANES)
        top = u_ref[c, :, :, depth - LANES : depth].reshape(side, LANES)
        both = jnp.where(lane == LANES - 1, top, bottom).T
        rows_ref[c : c + 1, 0:side] = both[0:1]
        rows_ref[c : c + 1, side : 2 * side] = both[LANES - 1 : LANES]
    width = pack * capacity
    route = route_ref[...]
    block, place = block_of(route, width, blocks)
    entries = spread(parts_of(rows_ref[...]), block, blocks)
    got = contract_lanes(jnp.concatenate(entries, 0), places(place, width))
    write_messages(out_ref, got, pack, blocks)
    message = pltpu.make_async_copy(out_ref, message_hbm, message_sem)
    message.start()
    sides_ref[0:1, :] = route[:, 0:side]
    sides_ref[1:2, :] = route[:, side : 2 * side]
    for copy in copies[2:5]:
        copy.wait()
    for c in range(13):
        ref = component(u_ref, v_ref, stress_ref, hour_ref, c)
        xup[c * columns : (c + 1) * columns, :] = ref[planes - 1]
        if c < 6:
            xdn[c * columns : (c + 1) * columns, :] = ref[0]
            ydn[c] = ref[:, 0, :]
    for copy in copies[5:]:
        copy.wait()
    message.wait()


def component(u_ref, v_ref, stress_ref, hour_ref, c):
    if c < 3:
        return u_ref.at[c]
    if c < 6:
        return v_ref.at[c - 3]
    if c < 12:
        return stress_ref.at[c - 6]
    return hour_ref


def corner_body(columns, xu, xd, out_ref):
    out_ref[...] = jnp.zeros(out_ref.shape, jnp.float32)
    for c in range(6):
        out_ref[c : c + 1, :] = xd[c * columns : c * columns + 1, :]
        out_ref[8 + c : 9 + c, :] = xu[c * columns : c * columns + 1, :]


def matrix_body(nodes_ref, diag_ref, matrix_ref, lines_ref, diag_lines_ref, square_ref, column_ref):
    pairs, slots = matrix_ref.shape
    group = 16
    square_ref[...] = jnp.zeros(square_ref.shape, jnp.int32)
    for r in range(pairs // LANES):
        chunk = nodes_ref[:, r * LANES : (r + 1) * LANES]
        for j in range(5):
            lines_ref[j, r : r + 1, :] = chunk[j : j + 1]
        square_ref[0:5, :] = chunk
        column_ref[r * LANES : (r + 1) * LANES, :] = square_ref[...].T
        for c in range(6):
            diag_lines_ref[c, r : r + 1, :] = diag_ref[c : c + 1, r * LANES : (r + 1) * LANES]

    def rows(start):
        columns = column_ref[pl.ds(start, group), :]
        slot = lax.broadcasted_iota(jnp.int32, (group, slots), 1)
        total = jnp.where(columns[:, 0:1] == slot, 1.0, 0.0)
        for j in range(1, 5):
            total = total - jnp.where(columns[:, j : j + 1] == slot, 0.25, 0.0)
        matrix_ref[pl.ds(start, group), :] = total.astype(jnp.bfloat16)

    steps(0, pairs // group, 4, lambda g: rows(pl.multiple_of(g * group, group)))


def dense_rows(table_ref, rows_ref, capacity, pack, offset):
    together = LANES // capacity
    lane = lax.broadcasted_iota(jnp.int32, (8, LANES), 1)
    for b in range(rows_ref.shape[0]):
        total = None
        for q in range(min(together, table_ref.shape[0] - b * together)):
            tile = table_ref[b * together + q]
            if pack > 1:
                tile = jnp.where((lane >= offset) & (lane < offset + capacity), tile, 0.0)
                tile = pltpu.roll(tile, (q * capacity - offset) & (LANES - 1), 1)
            elif q:
                tile = pltpu.roll(tile, q * capacity, 1)
            total = tile if total is None else total + tile
        rows_ref[b] = total
    return together * capacity


def looked_up(rows_ref, slots, width):
    shape = slots[0].shape
    found = [[None] * 3 for _ in slots]
    for b in range(rows_ref.shape[0]):
        rows = [jnp.broadcast_to(rows_ref[b, c : c + 1, :], shape) for c in range(3)]
        for slot, old in zip(slots, found):
            place = slot - b * width
            here = place >= 0
            for c in range(3):
                new = jnp.take_along_axis(rows[c], place & (LANES - 1), axis=1)
                old[c] = jnp.where(here, new, old[c]) if b else new
    return found


def pair_body(
    capacity, pack, blocks,
    table_ref, nodes_ref, diag_ref, gap_ref, stiff_ref, matrix_ref,
    out_hbm, rows_ref, out_ref, dense_ref, sem,
):
    offset = (lax.axis_index("space") % pack) * capacity
    dense = dense_rows(table_ref, dense_ref, capacity, pack, offset)
    picked = looked_up(dense_ref, [nodes_ref[j] for j in range(5)], dense)
    slave = picked[0]
    first = [diag_ref[c] + picked[3][c] - picked[1][c] for c in range(3)]
    second = [diag_ref[3 + c] + picked[4][c] - picked[2][c] for c in range(3)]
    normal = [
        first[(c + 1) % 3] * second[(c + 2) % 3] - first[(c + 2) % 3] * second[(c + 1) % 3]
        for c in range(3)
    ]
    gap = gap_ref[...]
    for c in range(3):
        centre = (picked[1][c] + picked[2][c] + picked[3][c] + picked[4][c]) * 0.25
        gap = gap + (slave[c] - centre) * normal[c]
    push = stiff_ref[...] * jnp.maximum(-gap, 0.0)
    out_ref[...] = jnp.zeros(out_ref.shape, jnp.float32)
    rows_ref[...] = jnp.zeros(rows_ref.shape, jnp.float32)
    for c in range(3):
        force = push * normal[c]
        for r in range(force.shape[0]):
            rows_ref[c : c + 1, r * LANES : (r + 1) * LANES] = force[r : r + 1]
    parts = [part.astype(jnp.bfloat16) for part in parts_of(rows_ref[...])]
    got = jnp.dot(
        jnp.concatenate(parts, 0), matrix_ref[...], preferred_element_type=jnp.float32
    )
    total = got[0:8] + got[8:16] + got[16:24]
    width = pack * capacity
    for b in range(blocks):
        for q in range(pack):
            out_ref[b * pack + q, :, 0:width] = total[:, b * width : (b + 1) * width]
    copy = pltpu.make_async_copy(out_ref, out_hbm, sem)
    copy.start()
    copy.wait()


def split(value):
    return jnp.stack([value[:, at : at + LANES] for at in range(0, value.shape[1], LANES)])


def z_pair(f):
    lane = lax.broadcasted_iota(jnp.int32, f.shape, 2)
    turned = pltpu.roll(f, LANES - 1, 2)
    after = jnp.concatenate([turned[1:], turned[:1]], 0)
    upper = jnp.where(lane == LANES - 1, after, turned)
    return f + upper, upper - f


def node_terms(sums, diffs, sums_next, diffs_next):
    result = []
    for c in range(6):
        s0, s1, d0, d1 = sums[c], sums_next[c], diffs[c], diffs_next[c]
        if c < 3:
            result.append((s0 + s1, s1 - s0, d0 + d1))
        else:
            result.append((d1 - d0, d0 + d1, s1 - s0))
    return result


def element_terms(lower, upper, stress, hour):
    eight = []
    for m in range(3):
        row = [
            upper[m][0] - lower[m][0],
            lower[m][1] + upper[m][1],
            lower[m][2] + upper[m][2],
        ]
        row[m] = row[m] + 4.0
        eight.append(row)
    cof = [
        [
            eight[(m + 1) % 3][(n + 1) % 3] * eight[(m + 2) % 3][(n + 2) % 3]
            - eight[(m + 1) % 3][(n + 2) % 3] * eight[(m + 2) % 3][(n + 1) % 3]
            for n in range(3)
        ]
        for m in range(3)
    ]
    hour = hour * 64.0
    result = []
    for m in range(3):
        line = [
            stress[VOIGT[m][0]] * cof[0][n]
            + stress[VOIGT[m][1]] * cof[1][n]
            + stress[VOIGT[m][2]] * cof[2][n]
            for n in range(3)
        ]
        low, up = lower[3 + m], upper[3 + m]
        line.append(hour * (low[0] + up[0]))
        line.append(hour * (up[1] - low[1]))
        line.append(hour * (up[2] - low[2]))
        line.append(hour * (up[0] - low[0]))
        result.append(line)
    return result


def gathered_x(before, after):
    result = []
    for m in range(3):
        p, n = before[m], after[m]
        result.append(
            (
                p[0] - n[0],
                (p[1] + n[1]) + (p[5] - n[5]),
                (p[2] + n[2]) + (p[4] - n[4]),
                (p[3] + n[3]) + (p[6] - n[6]),
            )
        )
    return result


def along_z(p, r):
    lane = lax.broadcasted_iota(jnp.int32, p.shape, 2)
    block = lax.broadcasted_iota(jnp.int32, p.shape, 0)
    nb = p.shape[0]
    up = pltpu.roll(p + r, 1, 2)
    before_up = jnp.concatenate([jnp.zeros_like(up[:1]), up[:-1]], 0)
    last = (lane == LANES - 1) & (block == nb - 1)
    return jnp.where(lane == 0, before_up, up) + jnp.where(last, 0.0, p - r)


def edge_body(u_ref, v_ref, stress_ref, hour_ref, yu, xu, xd, corner, beyond_ref, row_ref):
    planes, columns, _ = u_ref.shape[1:]
    rows = row_ref.shape[0]
    row_ref[...] = jnp.zeros(row_ref.shape, jnp.float32)

    def assembled(first, middle, last):
        row_ref[0:1, :] = first
        row_ref[1 : planes + 1, :] = middle
        if last is not None:
            row_ref[planes + 1 : planes + 2, :] = last
        return split(row_ref[...])

    def line(ref, at):
        return ref[at : at + 1, :]

    def following(q):
        return pltpu.roll(q, rows - 1, 1)

    def own(c):
        middle = component(u_ref, v_ref, stress_ref, hour_ref, c)[:, columns - 1, :]
        at = c * columns + columns - 1
        return assembled(line(xd, at), middle, line(xu, at) if c < 6 else None)

    own_s, own_d, next_s, next_d = [], [], [], []
    for c in range(6):
        s, d = z_pair(own(c))
        own_s.append(s)
        own_d.append(d)
        s, d = z_pair(assembled(line(corner, c), yu[c], line(corner, 8 + c)))
        next_s.append(s)
        next_d.append(d)
    lower = node_terms(own_s, own_d, next_s, next_d)
    upper = [tuple(following(q) for q in terms) for terms in lower]
    factors = element_terms(lower, upper, [own(6 + c) for c in range(6)], own(12))
    after = [[following(q) for q in terms] for terms in factors]
    for m, (a, b, c, e) in enumerate(gathered_x(factors, after)):
        force = along_z(a + b, c + e)[:, 0:planes]
        for k in range(force.shape[0]):
            beyond_ref[m, :, k * LANES : (k + 1) * LANES] = force[k]


def node_plane(values, halo_s, halo_d):
    row = lax.broadcasted_iota(jnp.int32, values[0].shape, 1)
    end = values[0].shape[1] - 1
    sums, diffs, sums_next, diffs_next = [], [], [], []
    for c in range(6):
        s, d = z_pair(values[c])
        sums.append(s)
        diffs.append(d)
        sums_next.append(jnp.where(row == end, halo_s[c], pltpu.roll(s, end, 1)))
        diffs_next.append(jnp.where(row == end, halo_d[c], pltpu.roll(d, end, 1)))
    return node_terms(sums, diffs, sums_next, diffs_next)


def kept_nodes(node_ref, i):
    return [tuple(node_ref[i, c, t] for t in range(3)) for c in range(6)]


def kept_elements(elem_ref, i):
    return [[elem_ref[i, m, t] for t in range(7)] for m in range(3)]


def new_velocity(before, after, velocity, mass):
    row = lax.broadcasted_iota(jnp.int32, mass.shape, 1)
    weight = (time_step / 64.0) / mass
    result = []
    for m, (a, b, c, e) in enumerate(gathered_x(before, after)):
        p = (a - b) + jnp.where(row == 0, 0.0, pltpu.roll(a + b, 1, 1))
        r = (c - e) + jnp.where(row == 0, 0.0, pltpu.roll(c + e, 1, 1))
        result.append(velocity[m] - along_z(p, r) * weight)
    return result


def steps(start, stop, unroll, body):
    count = (stop - start) // unroll

    def several(t, carry):
        for k in range(unroll):
            body(start + t * unroll + k)
        return carry

    lax.fori_loop(0, count, several, 0)
    for i in range(start + count * unroll, stop):
        body(jnp.int32(i))


def inner_body(
    unroll, u_ref, v_ref, stress_ref, hour_ref, mass_ref, yu, out_ref, node_ref, elem_ref, halo_s, halo_d
):
    planes, _, depth = u_ref.shape[1:]
    nb = depth // LANES
    for c in range(6):
        halo_s[c], halo_d[c] = z_pair(split(yu[c]))

    def nodes(i):
        values = [split(u_ref[c, i]) for c in range(3)] + [split(v_ref[c, i]) for c in range(3)]
        terms = node_plane(
            values,
            [halo_s[c, :, pl.ds(i, 1), :] for c in range(6)],
            [halo_d[c, :, pl.ds(i, 1), :] for c in range(6)],
        )
        for c in range(6):
            for t in range(3):
                node_ref[i, c, t] = terms[c][t]

    def elements(i):
        factors = element_terms(
            kept_nodes(node_ref, i),
            kept_nodes(node_ref, i + 1),
            [split(stress_ref[c, i]) for c in range(6)],
            split(hour_ref[i]),
        )
        for m in range(3):
            for t in range(7):
                elem_ref[i, m, t] = factors[m][t]

    def forces(i):
        result = new_velocity(
            kept_elements(elem_ref, i - 1),
            kept_elements(elem_ref, i),
            [split(v_ref[m, i]) for m in range(3)],
            split(mass_ref[i]),
        )
        for m in range(3):
            for k in range(nb):
                out_ref[m, i, :, k * LANES : (k + 1) * LANES] = result[m][k]

    steps(0, planes, unroll, nodes)
    steps(0, planes - 1, unroll, elements)
    steps(1, planes - 1, unroll, forces)


def outer_body(
    v_ref, stress_ref, hour_ref, mass_ref, node_ref, elem_ref, xu, xd, corner, out_ref
):
    planes, columns, depth = v_ref.shape[1:]
    last = planes - 1

    def part(ref, c):
        return split(ref[c * columns : (c + 1) * columns, :])

    def plane_terms(ref, at):
        halo_s, halo_d = z_pair(split(corner[at : at + 8, :]))
        return node_plane(
            [part(ref, c) for c in range(6)],
            [halo_s[:, c : c + 1] for c in range(6)],
            [halo_d[:, c : c + 1] for c in range(6)],
        )

    below = element_terms(
        plane_terms(xd, 0),
        kept_nodes(node_ref, 0),
        [part(xd, 6 + c) for c in range(6)],
        part(xd, 12),
    )
    above = element_terms(
        kept_nodes(node_ref, last),
        plane_terms(xu, 8),
        [split(stress_ref[c, last]) for c in range(6)],
        split(hour_ref[last]),
    )
    ends = (
        (0, below, kept_elements(elem_ref, 0)),
        (last, kept_elements(elem_ref, last - 1), above),
    )
    for at, (i, before, after) in enumerate(ends):
        velocity = [split(v_ref[m, i]) for m in range(3)]
        result = new_velocity(before, after, velocity, split(mass_ref[i]))
        for m in range(3):
            for k in range(depth // LANES):
                out_ref[m, at, :, k * LANES : (k + 1) * LANES] = result[m][k]


def final_body(
    capacity, pack,
    base_ref, outer_ref, mass_ref, table_ref, route_ref, left_ref,
    out_hbm, rows_ref, out_ref, dense_ref, sems,
):
    planes, columns, depth = base_ref.shape[1:]
    offset = (lax.axis_index("space") % pack) * capacity
    dense = dense_rows(table_ref, dense_ref, capacity, pack, offset)
    (contact,) = looked_up(dense_ref, [route_ref[...]], dense)
    rows_ref[...] = jnp.zeros(rows_ref.shape, jnp.float32)
    lane = lax.broadcasted_iota(jnp.int32, (planes, columns, LANES), 2)
    row = lax.broadcasted_iota(jnp.int32, (columns, LANES), 0)
    weights = [time_step / mass_ref[:, :, k : k + LANES] for k in range(0, depth, LANES)]
    low_weight = jnp.where(lane == 0, weights[0], 0.0)
    high_weight = jnp.where(lane == LANES - 1, weights[-1], 0.0)
    copies = []
    for m in range(3):
        rows_ref[m, 0:1, :] = contact[m][0:1]
        rows_ref[m, LANES - 1 : LANES, :] = contact[m][1:2]
        turned = rows_ref[m].T.reshape(planes, columns, LANES)
        for k in range(0, depth, LANES):
            left = jnp.stack(
                [
                    jnp.where(row == 0, left_ref[m, i : i + 1, k : k + LANES] * (1.0 / 64.0), 0.0)
                    for i in range(planes)
                ]
            )
            value = jnp.concatenate(
                [
                    outer_ref[m, 0:1, :, k : k + LANES],
                    base_ref[m, 1 : planes - 1, :, k : k + LANES],
                    outer_ref[m, 1:2, :, k : k + LANES],
                ]
            )
            value = value - left * weights[k // LANES]
            if k == 0:
                value = value + low_weight * turned
            if k == depth - LANES:
                value = value + high_weight * turned
            out_ref[m, :, :, k : k + LANES] = value
        copies.append(pltpu.make_async_copy(out_ref.at[m], out_hbm.at[m], sems.at[m]))
        copies[m].start()
    for copy in copies:
        copy.wait()


def local(
    displacement,
    velocity,
    stress,
    hourglass,
    mass,
    contact_route,
    pair_nodes,
    pair_diagonals,
    pair_gap,
    pair_stiffness,
):
    planes, columns, depth = displacement.shape[1:]
    nspace = lax.axis_size("space")
    surf_count = 2 * planes * columns
    pairs = pair_nodes.shape[1]
    capacity, pack, blocks = layout(nspace, surf_count)
    f32 = jnp.float32
    lines = pairs // LANES

    def sized(*shape):
        return jax.ShapeDtypeStruct(shape, f32)

    message = sized(nspace, 8, LANES)
    small = (pair_nodes, pair_diagonals, pair_gap.reshape(lines, LANES))
    small += (pair_stiffness.reshape(lines, LANES),)
    kept = (displacement, velocity, stress, hourglass, mass) + small
    outgoing, ydn, xdn, xup, sides, *kept = kernel_call(
        functools.partial(first_body, capacity, pack, blocks),
        (displacement, contact_route.reshape(1, surf_count)) + kept[1:],
        (
            pltpu.HBM(message.shape, f32),
            sized(6, planes, depth),
            sized(6 * columns, depth),
            sized(13 * columns, depth),
            jax.ShapeDtypeStruct((2, surf_count // 2), jnp.int32),
            *(jax.ShapeDtypeStruct(one.shape, one.dtype) for one in kept),
        ),
        [
            pltpu.VMEM(message.shape, f32),
            pltpu.VMEM((8, surf_count), f32),
            pltpu.VMEM((1, surf_count), jnp.int32),
            pltpu.SemaphoreType.DMA((len(kept) + 1,)),
            pltpu.SemaphoreType.DMA,
        ],
        hbm_inputs=len(kept) + 1,
    )
    fields, (pair_nodes, pair_diagonals, gap, stiffness) = kept[:5], kept[5:]
    received = exchanged(outgoing)
    yu = shifted(ydn, "slab", -1)
    xu = shifted(xdn, "space", -1)
    xd = shifted(xup, "space", 1)
    slots = nspace * capacity
    matrix, nodes, diagonals = kernel_call(
        matrix_body,
        (pair_nodes, pair_diagonals),
        (
            jax.ShapeDtypeStruct((pairs, slots), jnp.bfloat16),
            jax.ShapeDtypeStruct((5, lines, LANES), jnp.int32),
            sized(6, lines, LANES),
        ),
        [pltpu.VMEM((LANES, LANES), jnp.int32), pltpu.VMEM((pairs, LANES), jnp.int32)],
    )
    dense = pltpu.VMEM((pl.cdiv(nspace, LANES // capacity), 8, LANES), f32)
    slot_force = kernel_call(
        functools.partial(pair_body, capacity, pack, blocks),
        (received, nodes, diagonals, gap, stiffness, matrix),
        pltpu.HBM(message.shape, f32),
        [
            pltpu.VMEM((8, pairs), f32),
            pltpu.VMEM(message.shape, f32),
            dense,
            pltpu.SemaphoreType.DMA,
        ],
    )
    returned = exchanged(slot_force)

    corner = kernel_call(functools.partial(corner_body, columns), (xu, xd), sized(16, depth))
    corner = shifted(corner, "slab", -1)
    nb = depth // LANES
    base, node, elem = kernel_call(
        functools.partial(inner_body, 2),
        (*fields, yu),
        (
            sized(*displacement.shape),
            sized(planes, 6, 3, nb, columns, LANES),
            sized(planes - 1, 3, 7, nb, columns, LANES),
        ),
        [
            pltpu.VMEM((6, nb, planes, LANES), f32),
            pltpu.VMEM((6, nb, planes, LANES), f32),
        ],
    )
    rows = (planes + 2 + 7) // 8 * 8
    beyond = kernel_call(
        edge_body,
        (*fields[:4], yu, xu, xd, corner),
        sized(3, planes, depth),
        [pltpu.VMEM((rows, depth), f32)],
    )
    left = shifted(beyond, "slab", 1)
    outer = kernel_call(
        outer_body, (*fields[1:], node, elem, xu, xd, corner), sized(3, 2, columns, depth)
    )

    return kernel_call(
        functools.partial(final_body, capacity, pack),
        (base, outer, fields[4], returned, sides, left),
        pltpu.HBM(displacement.shape, f32),
        [
            pltpu.VMEM((3, LANES, LANES), f32),
            pltpu.VMEM(displacement.shape, f32),
            dense,
            pltpu.SemaphoreType.DMA((3,)),
        ],
    )


def solution(mesh):
    in_specs = (
        P(None, "space", "slab", None),
        P(None, "space", "slab", None),
        P(None, "space", "slab", None),
        P("space", "slab", None),
        P("space", "slab", None),
        P(("space", "slab")),
        P(None, ("space", "slab")),
        P(None, ("space", "slab")),
        P(("space", "slab")),
        P(("space", "slab")),
    )
    out_specs = P(None, "space", "slab", None)
    return jax.shard_map(local, mesh=mesh, in_specs=in_specs, out_specs=out_specs, check_vma=False)
```

```python
import functools

import jax
import jax.numpy as jnp
from jax import lax
from jax.experimental import pallas as pl
from jax.experimental.pallas import tpu as pltpu
from jax.sharding import PartitionSpec as P


time_step = 0.5
LANES = 128
VOIGT = [[0, 5, 4], [5, 1, 3], [4, 3, 2]]


def shifted(value, axis, steps):
    count = lax.axis_size(axis)
    return lax.ppermute(value, axis, [(at, (at + steps) % count) for at in range(count)])


def exchanged(value):
    return lax.all_to_all(value, "space", split_axis=0, concat_axis=0, tiled=True)


def kernel_call(body, inputs, outs, scratch=(), hbm_inputs=0):
    spaces = [pltpu.HBM if at < hbm_inputs else pltpu.VMEM for at in range(len(inputs))]
    inputs = [pltpu.with_memory_space_constraint(*pair) for pair in zip(inputs, spaces)]

    def placed(out):
        if isinstance(out, jax.ShapeDtypeStruct):
            return pltpu.VMEM(out.shape, out.dtype)
        return out

    outs = tuple(placed(out) for out in outs) if isinstance(outs, tuple) else placed(outs)
    return pl.pallas_call(
        body,
        out_shape=outs,
        in_specs=[pl.BlockSpec(memory_space=one) for one in spaces],
        out_specs=jax.tree.map(lambda out: pl.BlockSpec(memory_space=out.memory_space), outs),
        scratch_shapes=list(scratch),
        compiler_params=pltpu.CompilerParams(vmem_limit_bytes=16 << 20),
    )(*inputs)


def contract_lanes(lhs, rhs):
    return lax.dot_general(lhs, rhs, (((1,), (1,)), ((), ())), preferred_element_type=jnp.float32)


def layout(nspace, surf_count):
    capacity = max(2, (3 * surf_count // 2 + nspace - 1) // nspace)
    pack = max(1, min(LANES // capacity, nspace // 8))
    while nspace % pack:
        pack -= 1
    return capacity, pack, nspace // pack


def block_of(slots, width, blocks):
    block = jnp.zeros_like(slots)
    for b in range(1, blocks):
        block = block + jnp.where(slots >= b * width, 1, 0)
    return block, slots - block * width


def parts_of(rows):
    high = rows.astype(jnp.bfloat16).astype(jnp.float32)
    rest = rows - high
    middle = rest.astype(jnp.bfloat16).astype(jnp.float32)
    return [high, middle, rest - middle]


def places(place, width):
    rows = (width + 15) // 16 * 16
    count = place.shape[1]
    at = lax.broadcasted_iota(jnp.int32, (rows, count), 0)
    return jnp.where(at == place, 1.0, 0.0).astype(jnp.bfloat16)


def spread(parts, block, blocks):
    return [
        jnp.where(block == b, part, 0.0).astype(jnp.bfloat16)
        for part in parts
        for b in range(blocks)
    ]


def write_messages(out_ref, got, pack, blocks):
    for b in range(blocks):
        at = [(part * blocks + b) * 8 for part in range(3)]
        total = got[at[0] : at[0] + 8] + got[at[1] : at[1] + 8] + got[at[2] : at[2] + 8]
        for q in range(pack):
            out_ref[b * pack + q, :, 0 : total.shape[1]] = total


def first_body(
    capacity, pack, blocks, u_hbm, route_hbm, v_hbm, *rest,
):
    hbm, rest = (u_hbm, route_hbm, v_hbm) + rest[:7], rest[7:]
    message_hbm, ydn, xdn, xup, sides_ref, u_ref, v_ref, stress_ref, hour_ref = rest[:9]
    out_ref, rows_ref, route_ref, sems, message_sem = rest[-5:]
    targets = (u_ref, route_ref, v_ref, stress_ref, hour_ref) + rest[9:-5]
    copies = [
        pltpu.make_async_copy(source, target, sems.at[at])
        for at, (source, target) in enumerate(zip(hbm, targets))
    ]
    for copy in copies:
        copy.start()
    out_ref[...] = jnp.zeros(out_ref.shape, jnp.float32)
    rows_ref[...] = jnp.zeros(rows_ref.shape, jnp.float32)
    copies[0].wait()
    copies[1].wait()
    planes, columns, depth = u_ref.shape[1:]
    side = planes * columns
    lane = lax.broadcasted_iota(jnp.int32, (side, LANES), 1)
    for c in range(3):
        bottom = u_ref[c, :, :, 0:LANES].reshape(side, LANES)
        top = u_ref[c, :, :, depth - LANES : depth].reshape(side, LANES)
        both = jnp.where(lane == LANES - 1, top, bottom).T
        rows_ref[c : c + 1, 0:side] = both[0:1]
        rows_ref[c : c + 1, side : 2 * side] = both[LANES - 1 : LANES]
    width = pack * capacity
    route = route_ref[...]
    block, place = block_of(route, width, blocks)
    entries = spread(parts_of(rows_ref[...]), block, blocks)
    got = contract_lanes(jnp.concatenate(entries, 0), places(place, width))
    write_messages(out_ref, got, pack, blocks)
    message = pltpu.make_async_copy(out_ref, message_hbm, message_sem)
    message.start()
    sides_ref[0:1, :] = route[:, 0:side]
    sides_ref[1:2, :] = route[:, side : 2 * side]
    for copy in copies[2:5]:
        copy.wait()
    for c in range(13):
        ref = component(u_ref, v_ref, stress_ref, hour_ref, c)
        xup[c * columns : (c + 1) * columns, :] = ref[planes - 1]
        if c < 6:
            xdn[c * columns : (c + 1) * columns, :] = ref[0]
            ydn[c] = ref[:, 0, :]
    for copy in copies[5:]:
        copy.wait()
    message.wait()


def component(u_ref, v_ref, stress_ref, hour_ref, c):
    if c < 3:
        return u_ref.at[c]
    if c < 6:
        return v_ref.at[c - 3]
    if c < 12:
        return stress_ref.at[c - 6]
    return hour_ref


def corner_body(columns, xu, xd, out_ref):
    out_ref[...] = jnp.zeros(out_ref.shape, jnp.float32)
    for c in range(6):
        out_ref[c : c + 1, :] = xd[c * columns : c * columns + 1, :]
        out_ref[8 + c : 9 + c, :] = xu[c * columns : c * columns + 1, :]


def matrix_body(nodes_ref, diag_ref, matrix_ref, lines_ref, diag_lines_ref):
    pairs = nodes_ref.shape[1]
    group = 16

    def rows(g, carry):
        start = pl.multiple_of(g * group, group)
        slot = lax.broadcasted_iota(jnp.int32, (group, pairs), 0) + start
        total = jnp.where(nodes_ref[0:1, :] == slot, 1.0, 0.0)
        for j in range(1, 5):
            total = total - jnp.where(nodes_ref[j : j + 1, :] == slot, 0.25, 0.0)
        matrix_ref[pl.ds(start, group), :] = total.astype(jnp.bfloat16)
        return carry

    lax.fori_loop(0, matrix_ref.shape[0] // group, rows, 0)
    for r in range(pairs // LANES):
        for j in range(5):
            lines_ref[j, r : r + 1, :] = nodes_ref[j : j + 1, r * LANES : (r + 1) * LANES]
        for c in range(6):
            diag_lines_ref[c, r : r + 1, :] = diag_ref[c : c + 1, r * LANES : (r + 1) * LANES]


def dense_rows(table_ref, rows_ref, capacity, pack, offset):
    together = LANES // capacity
    lane = lax.broadcasted_iota(jnp.int32, (8, LANES), 1)
    for b in range(rows_ref.shape[0]):
        total = None
        for q in range(min(together, table_ref.shape[0] - b * together)):
            tile = table_ref[b * together + q]
            if pack > 1:
                tile = jnp.where((lane >= offset) & (lane < offset + capacity), tile, 0.0)
                tile = pltpu.roll(tile, (q * capacity - offset) & (LANES - 1), 1)
            elif q:
                tile = pltpu.roll(tile, q * capacity, 1)
            total = tile if total is None else total + tile
        rows_ref[b] = total
    return together * capacity


def looked_up(rows_ref, slots, width):
    shape = slots[0].shape
    found = [[None] * 3 for _ in slots]
    for b in range(rows_ref.shape[0]):
        rows = [jnp.broadcast_to(rows_ref[b, c : c + 1, :], shape) for c in range(3)]
        for slot, old in zip(slots, found):
            place = slot - b * width
            here = place >= 0
            for c in range(3):
                new = jnp.take_along_axis(rows[c], place & (LANES - 1), axis=1)
                old[c] = jnp.where(here, new, old[c]) if b else new
    return found


def pair_body(
    capacity, pack, blocks,
    table_ref, nodes_ref, diag_ref, gap_ref, stiff_ref, matrix_ref,
    out_hbm, rows_ref, out_ref, dense_ref, sem,
):
    offset = (lax.axis_index("space") % pack) * capacity
    dense = dense_rows(table_ref, dense_ref, capacity, pack, offset)
    picked = looked_up(dense_ref, [nodes_ref[j] for j in range(5)], dense)
    slave = picked[0]
    first = [diag_ref[c] + picked[3][c] - picked[1][c] for c in range(3)]
    second = [diag_ref[3 + c] + picked[4][c] - picked[2][c] for c in range(3)]
    normal = [
        first[(c + 1) % 3] * second[(c + 2) % 3] - first[(c + 2) % 3] * second[(c + 1) % 3]
        for c in range(3)
    ]
    gap = gap_ref[...]
    for c in range(3):
        centre = (picked[1][c] + picked[2][c] + picked[3][c] + picked[4][c]) * 0.25
        gap = gap + (slave[c] - centre) * normal[c]
    push = stiff_ref[...] * jnp.maximum(-gap, 0.0)
    out_ref[...] = jnp.zeros(out_ref.shape, jnp.float32)
    rows_ref[...] = jnp.zeros(rows_ref.shape, jnp.float32)
    for c in range(3):
        force = push * normal[c]
        for r in range(force.shape[0]):
            rows_ref[c : c + 1, r * LANES : (r + 1) * LANES] = force[r : r + 1]
    parts = [part.astype(jnp.bfloat16) for part in parts_of(rows_ref[...])]
    got = contract_lanes(jnp.concatenate(parts, 0), matrix_ref[...])
    total = got[0:8] + got[8:16] + got[16:24]
    width = pack * capacity
    for b in range(blocks):
        for q in range(pack):
            out_ref[b * pack + q, :, 0:width] = total[:, b * width : (b + 1) * width]
    copy = pltpu.make_async_copy(out_ref, out_hbm, sem)
    copy.start()
    copy.wait()


def split(value):
    return jnp.stack([value[:, at : at + LANES] for at in range(0, value.shape[1], LANES)])


def z_pair(f):
    lane = lax.broadcasted_iota(jnp.int32, f.shape, 2)
    turned = pltpu.roll(f, LANES - 1, 2)
    after = jnp.concatenate([turned[1:], turned[:1]], 0)
    upper = jnp.where(lane == LANES - 1, after, turned)
    return f + upper, upper - f


def node_terms(sums, diffs, sums_next, diffs_next):
    result = []
    for c in range(6):
        s0, s1, d0, d1 = sums[c], sums_next[c], diffs[c], diffs_next[c]
        if c < 3:
            result.append((s0 + s1, s1 - s0, d0 + d1))
        else:
            result.append((d1 - d0, d0 + d1, s1 - s0))
    return result


def element_terms(lower, upper, stress, hour):
    eight = []
    for m in range(3):
        row = [
            upper[m][0] - lower[m][0],
            lower[m][1] + upper[m][1],
            lower[m][2] + upper[m][2],
        ]
        row[m] = row[m] + 4.0
        eight.append(row)
    cof = [
        [
            eight[(m + 1) % 3][(n + 1) % 3] * eight[(m + 2) % 3][(n + 2) % 3]
            - eight[(m + 1) % 3][(n + 2) % 3] * eight[(m + 2) % 3][(n + 1) % 3]
            for n in range(3)
        ]
        for m in range(3)
    ]
    hour = hour * 64.0
    result = []
    for m in range(3):
        line = [
            stress[VOIGT[m][0]] * cof[0][n]
            + stress[VOIGT[m][1]] * cof[1][n]
            + stress[VOIGT[m][2]] * cof[2][n]
            for n in range(3)
        ]
        low, up = lower[3 + m], upper[3 + m]
        line.append(hour * (low[0] + up[0]))
        line.append(hour * (up[1] - low[1]))
        line.append(hour * (up[2] - low[2]))
        line.append(hour * (up[0] - low[0]))
        result.append(line)
    return result


def gathered_x(before, after):
    result = []
    for m in range(3):
        p, n = before[m], after[m]
        result.append(
            (
                p[0] - n[0],
                (p[1] + n[1]) + (p[5] - n[5]),
                (p[2] + n[2]) + (p[4] - n[4]),
                (p[3] + n[3]) + (p[6] - n[6]),
            )
        )
    return result


def along_z(p, r):
    lane = lax.broadcasted_iota(jnp.int32, p.shape, 2)
    block = lax.broadcasted_iota(jnp.int32, p.shape, 0)
    nb = p.shape[0]
    up = pltpu.roll(p + r, 1, 2)
    before_up = jnp.concatenate([jnp.zeros_like(up[:1]), up[:-1]], 0)
    last = (lane == LANES - 1) & (block == nb - 1)
    return jnp.where(lane == 0, before_up, up) + jnp.where(last, 0.0, p - r)


def edge_body(u_ref, v_ref, stress_ref, hour_ref, yu, xu, xd, corner, beyond_ref, row_ref):
    planes, columns, _ = u_ref.shape[1:]
    rows = row_ref.shape[0]
    row_ref[...] = jnp.zeros(row_ref.shape, jnp.float32)

    def assembled(first, middle, last):
        row_ref[0:1, :] = first
        row_ref[1 : planes + 1, :] = middle
        if last is not None:
            row_ref[planes + 1 : planes + 2, :] = last
        return split(row_ref[...])

    def line(ref, at):
        return ref[at : at + 1, :]

    def following(q):
        return pltpu.roll(q, rows - 1, 1)

    def own(c):
        middle = component(u_ref, v_ref, stress_ref, hour_ref, c)[:, columns - 1, :]
        at = c * columns + columns - 1
        return assembled(line(xd, at), middle, line(xu, at) if c < 6 else None)

    own_s, own_d, next_s, next_d = [], [], [], []
    for c in range(6):
        s, d = z_pair(own(c))
        own_s.append(s)
        own_d.append(d)
        s, d = z_pair(assembled(line(corner, c), yu[c], line(corner, 8 + c)))
        next_s.append(s)
        next_d.append(d)
    lower = node_terms(own_s, own_d, next_s, next_d)
    upper = [tuple(following(q) for q in terms) for terms in lower]
    factors = element_terms(lower, upper, [own(6 + c) for c in range(6)], own(12))
    after = [[following(q) for q in terms] for terms in factors]
    for m, (a, b, c, e) in enumerate(gathered_x(factors, after)):
        force = along_z(a + b, c + e)[:, 0:planes]
        for k in range(force.shape[0]):
            beyond_ref[m, :, k * LANES : (k + 1) * LANES] = force[k]


def node_plane(values, halo_s, halo_d):
    row = lax.broadcasted_iota(jnp.int32, values[0].shape, 1)
    end = values[0].shape[1] - 1
    sums, diffs, sums_next, diffs_next = [], [], [], []
    for c in range(6):
        s, d = z_pair(values[c])
        sums.append(s)
        diffs.append(d)
        sums_next.append(jnp.where(row == end, halo_s[c], pltpu.roll(s, end, 1)))
        diffs_next.append(jnp.where(row == end, halo_d[c], pltpu.roll(d, end, 1)))
    return node_terms(sums, diffs, sums_next, diffs_next)


def kept_nodes(node_ref, i):
    return [tuple(node_ref[i, c, t] for t in range(3)) for c in range(6)]


def kept_elements(elem_ref, i):
    return [[elem_ref[i, m, t] for t in range(7)] for m in range(3)]


def new_velocity(before, after, velocity, mass):
    row = lax.broadcasted_iota(jnp.int32, mass.shape, 1)
    weight = (time_step / 64.0) / mass
    result = []
    for m, (a, b, c, e) in enumerate(gathered_x(before, after)):
        p = (a - b) + jnp.where(row == 0, 0.0, pltpu.roll(a + b, 1, 1))
        r = (c - e) + jnp.where(row == 0, 0.0, pltpu.roll(c + e, 1, 1))
        result.append(velocity[m] - along_z(p, r) * weight)
    return result


def steps(start, stop, unroll, body):
    count = (stop - start) // unroll

    def several(t, carry):
        for k in range(unroll):
            body(start + t * unroll + k)
        return carry

    lax.fori_loop(0, count, several, 0)
    for i in range(start + count * unroll, stop):
        body(jnp.int32(i))


def inner_body(
    unroll, u_ref, v_ref, stress_ref, hour_ref, yu, node_ref, elem_ref, halo_s, halo_d
):
    planes = u_ref.shape[1]
    for c in range(6):
        halo_s[c], halo_d[c] = z_pair(split(yu[c]))

    def nodes(i):
        values = [split(u_ref[c, i]) for c in range(3)] + [split(v_ref[c, i]) for c in range(3)]
        terms = node_plane(
            values,
            [halo_s[c, :, pl.ds(i, 1), :] for c in range(6)],
            [halo_d[c, :, pl.ds(i, 1), :] for c in range(6)],
        )
        for c in range(6):
            for t in range(3):
                node_ref[i, c, t] = terms[c][t]

    def elements(i):
        factors = element_terms(
            kept_nodes(node_ref, i),
            kept_nodes(node_ref, i + 1),
            [split(stress_ref[c, i]) for c in range(6)],
            split(hour_ref[i]),
        )
        for m in range(3):
            for t in range(7):
                elem_ref[i, m, t] = factors[m][t]

    steps(0, planes, unroll, nodes)
    steps(0, planes - 1, unroll, elements)


def outer_body(
    unroll, v_ref, stress_ref, hour_ref, mass_ref, node_ref, elem_ref, xu, xd, corner, out_ref
):
    planes, columns, depth = v_ref.shape[1:]
    last = planes - 1

    def write_plane(i, before, after):
        velocity = [split(v_ref[m, i]) for m in range(3)]
        result = new_velocity(before, after, velocity, split(mass_ref[i]))
        for m in range(3):
            for k in range(depth // LANES):
                out_ref[m, i, :, k * LANES : (k + 1) * LANES] = result[m][k]

    def inside(i):
        write_plane(i, kept_elements(elem_ref, i - 1), kept_elements(elem_ref, i))

    def part(ref, c):
        return split(ref[c * columns : (c + 1) * columns, :])

    def plane_terms(ref, at):
        halo_s, halo_d = z_pair(split(corner[at : at + 8, :]))
        return node_plane(
            [part(ref, c) for c in range(6)],
            [halo_s[:, c : c + 1] for c in range(6)],
            [halo_d[:, c : c + 1] for c in range(6)],
        )

    below = element_terms(
        plane_terms(xd, 0),
        kept_nodes(node_ref, 0),
        [part(xd, 6 + c) for c in range(6)],
        part(xd, 12),
    )
    above = element_terms(
        kept_nodes(node_ref, last),
        plane_terms(xu, 8),
        [split(stress_ref[c, last]) for c in range(6)],
        split(hour_ref[last]),
    )
    write_plane(0, below, kept_elements(elem_ref, 0))
    write_plane(last, kept_elements(elem_ref, last - 1), above)
    steps(1, last, unroll, inside)


def final_body(
    capacity, pack,
    base_ref, mass_ref, table_ref, route_ref, left_ref,
    out_hbm, rows_ref, out_ref, dense_ref, sems,
):
    planes, columns, depth = base_ref.shape[1:]
    offset = (lax.axis_index("space") % pack) * capacity
    dense = dense_rows(table_ref, dense_ref, capacity, pack, offset)
    (contact,) = looked_up(dense_ref, [route_ref[...]], dense)
    rows_ref[...] = jnp.zeros(rows_ref.shape, jnp.float32)
    lane = lax.broadcasted_iota(jnp.int32, (planes, columns, LANES), 2)
    row = lax.broadcasted_iota(jnp.int32, (columns, LANES), 0)
    weights = [time_step / mass_ref[:, :, k : k + LANES] for k in range(0, depth, LANES)]
    low_weight = jnp.where(lane == 0, weights[0], 0.0)
    high_weight = jnp.where(lane == LANES - 1, weights[-1], 0.0)
    copies = []
    for m in range(3):
        rows_ref[m, 0:1, :] = contact[m][0:1]
        rows_ref[m, LANES - 1 : LANES, :] = contact[m][1:2]
        turned = rows_ref[m].T.reshape(planes, columns, LANES)
        for k in range(0, depth, LANES):
            left = jnp.stack(
                [
                    jnp.where(row == 0, left_ref[m, i : i + 1, k : k + LANES] * (1.0 / 64.0), 0.0)
                    for i in range(planes)
                ]
            )
            value = base_ref[m, :, :, k : k + LANES] - left * weights[k // LANES]
            if k == 0:
                value = value + low_weight * turned
            if k == depth - LANES:
                value = value + high_weight * turned
            out_ref[m, :, :, k : k + LANES] = value
        copies.append(pltpu.make_async_copy(out_ref.at[m], out_hbm.at[m], sems.at[m]))
        copies[m].start()
    for copy in copies:
        copy.wait()


def local(
    displacement,
    velocity,
    stress,
    hourglass,
    mass,
    contact_route,
    pair_nodes,
    pair_diagonals,
    pair_gap,
    pair_stiffness,
):
    planes, columns, depth = displacement.shape[1:]
    nspace = lax.axis_size("space")
    surf_count = 2 * planes * columns
    pairs = pair_nodes.shape[1]
    capacity, pack, blocks = layout(nspace, surf_count)
    f32 = jnp.float32
    lines = pairs // LANES

    def sized(*shape):
        return jax.ShapeDtypeStruct(shape, f32)

    message = sized(nspace, 8, LANES)
    small = (pair_nodes, pair_diagonals, pair_gap.reshape(lines, LANES))
    small += (pair_stiffness.reshape(lines, LANES),)
    kept = (displacement, velocity, stress, hourglass, mass) + small
    outgoing, ydn, xdn, xup, sides, *kept = kernel_call(
        functools.partial(first_body, capacity, pack, blocks),
        (displacement, contact_route.reshape(1, surf_count)) + kept[1:],
        (
            pltpu.HBM(message.shape, f32),
            sized(6, planes, depth),
            sized(6 * columns, depth),
            sized(13 * columns, depth),
            jax.ShapeDtypeStruct((2, surf_count // 2), jnp.int32),
            *(jax.ShapeDtypeStruct(one.shape, one.dtype) for one in kept),
        ),
        [
            pltpu.VMEM(message.shape, f32),
            pltpu.VMEM((8, surf_count), f32),
            pltpu.VMEM((1, surf_count), jnp.int32),
            pltpu.SemaphoreType.DMA((len(kept) + 1,)),
            pltpu.SemaphoreType.DMA,
        ],
        hbm_inputs=len(kept) + 1,
    )
    fields, (pair_nodes, pair_diagonals, gap, stiffness) = kept[:5], kept[5:]
    received = exchanged(outgoing)
    yu = shifted(ydn, "slab", -1)
    xu = shifted(xdn, "space", -1)
    xd = shifted(xup, "space", 1)
    slots = (nspace * capacity + 15) // 16 * 16
    matrix, nodes, diagonals = kernel_call(
        matrix_body,
        (pair_nodes, pair_diagonals),
        (
            jax.ShapeDtypeStruct((slots, pairs), jnp.bfloat16),
            jax.ShapeDtypeStruct((5, lines, LANES), jnp.int32),
            sized(6, lines, LANES),
        ),
    )
    dense = pltpu.VMEM((pl.cdiv(nspace, LANES // capacity), 8, LANES), f32)
    slot_force = kernel_call(
        functools.partial(pair_body, capacity, pack, blocks),
        (received, nodes, diagonals, gap, stiffness, matrix),
        pltpu.HBM(message.shape, f32),
        [
            pltpu.VMEM((8, pairs), f32),
            pltpu.VMEM(message.shape, f32),
            dense,
            pltpu.SemaphoreType.DMA,
        ],
    )
    returned = exchanged(slot_force)

    corner = kernel_call(functools.partial(corner_body, columns), (xu, xd), sized(16, depth))
    corner = shifted(corner, "slab", -1)
    nb = depth // LANES
    node, elem = kernel_call(
        functools.partial(inner_body, 2),
        (*fields[:4], yu),
        (
            sized(planes, 6, 3, nb, columns, LANES),
            sized(planes - 1, 3, 7, nb, columns, LANES),
        ),
        [
            pltpu.VMEM((6, nb, planes, LANES), f32),
            pltpu.VMEM((6, nb, planes, LANES), f32),
        ],
    )
    rows = (planes + 2 + 7) // 8 * 8
    beyond = kernel_call(
        edge_body,
        (*fields[:4], yu, xu, xd, corner),
        sized(3, planes, depth),
        [pltpu.VMEM((rows, depth), f32)],
    )
    left = shifted(beyond, "slab", 1)
    base = kernel_call(
        functools.partial(outer_body, 2),
        (*fields[1:], node, elem, xu, xd, corner),
        sized(*displacement.shape),
    )

    return kernel_call(
        functools.partial(final_body, capacity, pack),
        (base, fields[4], returned, sides, left),
        pltpu.HBM(displacement.shape, f32),
        [
            pltpu.VMEM((3, LANES, LANES), f32),
            pltpu.VMEM(displacement.shape, f32),
            dense,
            pltpu.SemaphoreType.DMA((3,)),
        ],
    )


def solution(mesh):
    in_specs = (
        P(None, "space", "slab", None),
        P(None, "space", "slab", None),
        P(None, "space", "slab", None),
        P("space", "slab", None),
        P("space", "slab", None),
        P(("space", "slab")),
        P(None, ("space", "slab")),
        P(None, ("space", "slab")),
        P(("space", "slab")),
        P(("space", "slab")),
    )
    out_specs = P(None, "space", "slab", None)
    return jax.shard_map(local, mesh=mesh, in_specs=in_specs, out_specs=out_specs, check_vma=False)
```

```python
import functools

import jax
import jax.numpy as jnp
from jax import lax
from jax.experimental import pallas as pl
from jax.experimental.pallas import tpu as pltpu
from jax.sharding import PartitionSpec as P


time_step = 0.5
LANES = 128
VOIGT = [[0, 5, 4], [5, 1, 3], [4, 3, 2]]


def shifted(value, axis, steps):
    count = lax.axis_size(axis)
    return lax.ppermute(value, axis, [(at, (at + steps) % count) for at in range(count)])


def exchanged(value):
    count = lax.axis_size("space")
    order = [(at + count // 4) % count for at in range(count)]
    return lax.all_to_all(
        value, "space", split_axis=0, concat_axis=0, tiled=True, axis_index_groups=[order]
    )


def seat(at, count):
    return (at - count // 4) % count


def kernel_call(body, inputs, outs, scratch=(), hbm_inputs=0):
    spaces = [pltpu.HBM if at < hbm_inputs else pltpu.VMEM for at in range(len(inputs))]
    inputs = [pltpu.with_memory_space_constraint(*pair) for pair in zip(inputs, spaces)]

    def placed(out):
        if isinstance(out, jax.ShapeDtypeStruct):
            return pltpu.VMEM(out.shape, out.dtype)
        return out

    outs = tuple(placed(out) for out in outs) if isinstance(outs, tuple) else placed(outs)
    return pl.pallas_call(
        body,
        out_shape=outs,
        in_specs=[pl.BlockSpec(memory_space=one) for one in spaces],
        out_specs=jax.tree.map(lambda out: pl.BlockSpec(memory_space=out.memory_space), outs),
        scratch_shapes=list(scratch),
        compiler_params=pltpu.CompilerParams(vmem_limit_bytes=16 << 20),
    )(*inputs)


def contract_lanes(lhs, rhs):
    return lax.dot_general(lhs, rhs, (((1,), (1,)), ((), ())), preferred_element_type=jnp.float32)


def layout(nspace, surf_count):
    capacity = max(2, (3 * surf_count // 2 + nspace - 1) // nspace)
    pack = max(1, min(LANES // capacity, nspace // 8))
    while nspace % pack:
        pack -= 1
    return capacity, pack, nspace // pack


def block_of(slots, width, blocks):
    block = jnp.zeros_like(slots)
    for b in range(1, blocks):
        block = block + jnp.where(slots >= b * width, 1, 0)
    return block, slots - block * width


def parts_of(rows):
    high = rows.astype(jnp.bfloat16).astype(jnp.float32)
    rest = rows - high
    middle = rest.astype(jnp.bfloat16).astype(jnp.float32)
    return [high, middle, rest - middle]


def places(place, width):
    rows = (width + 15) // 16 * 16
    count = place.shape[1]
    at = lax.broadcasted_iota(jnp.int32, (rows, count), 0)
    return jnp.where(at == place, 1.0, 0.0).astype(jnp.bfloat16)


def spread(parts, block, blocks):
    return [
        jnp.where(block == b, part, 0.0).astype(jnp.bfloat16)
        for part in parts
        for b in range(blocks)
    ]


def write_messages(out_ref, got, pack, blocks):
    for b in range(blocks):
        at = [(part * blocks + b) * 8 for part in range(3)]
        total = got[at[0] : at[0] + 8] + got[at[1] : at[1] + 8] + got[at[2] : at[2] + 8]
        for q in range(pack):
            out_ref[seat(b * pack + q, out_ref.shape[0]), :, 0 : total.shape[1]] = total


def first_body(
    capacity, pack, blocks, u_hbm, route_hbm, v_hbm, *rest,
):
    hbm, rest = (u_hbm, route_hbm, v_hbm) + rest[:7], rest[7:]
    message_hbm, ydn, xdn, xup, sides_ref, u_ref, v_ref, stress_ref, hour_ref = rest[:9]
    out_ref, rows_ref, route_ref, sems, message_sem = rest[-5:]
    targets = (u_ref, route_ref, v_ref, stress_ref, hour_ref) + rest[9:-5]
    copies = [
        pltpu.make_async_copy(source, target, sems.at[at])
        for at, (source, target) in enumerate(zip(hbm, targets))
    ]
    for copy in copies:
        copy.start()
    out_ref[...] = jnp.zeros(out_ref.shape, jnp.float32)
    rows_ref[...] = jnp.zeros(rows_ref.shape, jnp.float32)
    copies[0].wait()
    copies[1].wait()
    planes, columns, depth = u_ref.shape[1:]
    side = planes * columns
    lane = lax.broadcasted_iota(jnp.int32, (side, LANES), 1)
    for c in range(3):
        bottom = u_ref[c, :, :, 0:LANES].reshape(side, LANES)
        top = u_ref[c, :, :, depth - LANES : depth].reshape(side, LANES)
        both = jnp.where(lane == LANES - 1, top, bottom).T
        rows_ref[c : c + 1, 0:side] = both[0:1]
        rows_ref[c : c + 1, side : 2 * side] = both[LANES - 1 : LANES]
    width = pack * capacity
    route = route_ref[...]
    block, place = block_of(route, width, blocks)
    entries = spread(parts_of(rows_ref[...]), block, blocks)
    got = contract_lanes(jnp.concatenate(entries, 0), places(place, width))
    write_messages(out_ref, got, pack, blocks)
    message = pltpu.make_async_copy(out_ref, message_hbm, message_sem)
    message.start()
    sides_ref[0:1, :] = route[:, 0:side]
    sides_ref[1:2, :] = route[:, side : 2 * side]
    for copy in copies[2:5]:
        copy.wait()
    for c in range(13):
        ref = component(u_ref, v_ref, stress_ref, hour_ref, c)
        xup[c * columns : (c + 1) * columns, :] = ref[planes - 1]
        if c < 6:
            xdn[c * columns : (c + 1) * columns, :] = ref[0]
            ydn[c] = ref[:, 0, :]
    for copy in copies[5:]:
        copy.wait()
    message.wait()


def component(u_ref, v_ref, stress_ref, hour_ref, c):
    if c < 3:
        return u_ref.at[c]
    if c < 6:
        return v_ref.at[c - 3]
    if c < 12:
        return stress_ref.at[c - 6]
    return hour_ref


def corner_body(columns, xu, xd, out_ref):
    out_ref[...] = jnp.zeros(out_ref.shape, jnp.float32)
    for c in range(6):
        out_ref[c : c + 1, :] = xd[c * columns : c * columns + 1, :]
        out_ref[8 + c : 9 + c, :] = xu[c * columns : c * columns + 1, :]


def matrix_body(nodes_ref, diag_ref, matrix_ref, lines_ref, diag_lines_ref):
    pairs = nodes_ref.shape[1]
    group = 16

    def rows(g, carry):
        start = pl.multiple_of(g * group, group)
        slot = lax.broadcasted_iota(jnp.int32, (group, pairs), 0) + start
        total = jnp.where(nodes_ref[0:1, :] == slot, 1.0, 0.0)
        for j in range(1, 5):
            total = total - jnp.where(nodes_ref[j : j + 1, :] == slot, 0.25, 0.0)
        matrix_ref[pl.ds(start, group), :] = total.astype(jnp.bfloat16)
        return carry

    lax.fori_loop(0, matrix_ref.shape[0] // group, rows, 0)
    for r in range(pairs // LANES):
        for j in range(5):
            lines_ref[j, r : r + 1, :] = nodes_ref[j : j + 1, r * LANES : (r + 1) * LANES]
        for c in range(6):
            diag_lines_ref[c, r : r + 1, :] = diag_ref[c : c + 1, r * LANES : (r + 1) * LANES]


def dense_rows(table_ref, rows_ref, capacity, pack, offset):
    together = LANES // capacity
    lane = lax.broadcasted_iota(jnp.int32, (8, LANES), 1)
    for b in range(rows_ref.shape[0]):
        total = None
        for q in range(min(together, table_ref.shape[0] - b * together)):
            tile = table_ref[seat(b * together + q, table_ref.shape[0])]
            if pack > 1:
                tile = jnp.where((lane >= offset) & (lane < offset + capacity), tile, 0.0)
                tile = pltpu.roll(tile, (q * capacity - offset) & (LANES - 1), 1)
            elif q:
                tile = pltpu.roll(tile, q * capacity, 1)
            total = tile if total is None else total + tile
        rows_ref[b] = total
    return together * capacity


def looked_up(rows_ref, slots, width):
    shape = slots[0].shape
    found = [[None] * 3 for _ in slots]
    for b in range(rows_ref.shape[0]):
        rows = [jnp.broadcast_to(rows_ref[b, c : c + 1, :], shape) for c in range(3)]
        for slot, old in zip(slots, found):
            place = slot - b * width
            here = place >= 0
            for c in range(3):
                new = jnp.take_along_axis(rows[c], place & (LANES - 1), axis=1)
                old[c] = jnp.where(here, new, old[c]) if b else new
    return found


def pair_body(
    capacity, pack, blocks,
    table_ref, nodes_ref, diag_ref, gap_ref, stiff_ref, matrix_ref,
    out_hbm, rows_ref, out_ref, dense_ref, sem,
):
    offset = (lax.axis_index("space") % pack) * capacity
    dense = dense_rows(table_ref, dense_ref, capacity, pack, offset)
    picked = looked_up(dense_ref, [nodes_ref[j] for j in range(5)], dense)
    slave = picked[0]
    first = [diag_ref[c] + picked[3][c] - picked[1][c] for c in range(3)]
    second = [diag_ref[3 + c] + picked[4][c] - picked[2][c] for c in range(3)]
    normal = [
        first[(c + 1) % 3] * second[(c + 2) % 3] - first[(c + 2) % 3] * second[(c + 1) % 3]
        for c in range(3)
    ]
    gap = gap_ref[...]
    for c in range(3):
        centre = (picked[1][c] + picked[2][c] + picked[3][c] + picked[4][c]) * 0.25
        gap = gap + (slave[c] - centre) * normal[c]
    push = stiff_ref[...] * jnp.maximum(-gap, 0.0)
    out_ref[...] = jnp.zeros(out_ref.shape, jnp.float32)
    rows_ref[...] = jnp.zeros(rows_ref.shape, jnp.float32)
    for c in range(3):
        force = push * normal[c]
        for r in range(force.shape[0]):
            rows_ref[c : c + 1, r * LANES : (r + 1) * LANES] = force[r : r + 1]
    parts = [part.astype(jnp.bfloat16) for part in parts_of(rows_ref[...])]
    got = contract_lanes(jnp.concatenate(parts, 0), matrix_ref[...])
    total = got[0:8] + got[8:16] + got[16:24]
    width = pack * capacity
    for b in range(blocks):
        for q in range(pack):
            block = total[:, b * width : (b + 1) * width]
            out_ref[seat(b * pack + q, out_ref.shape[0]), :, 0:width] = block
    copy = pltpu.make_async_copy(out_ref, out_hbm, sem)
    copy.start()
    copy.wait()


def split(value):
    return jnp.stack([value[:, at : at + LANES] for at in range(0, value.shape[1], LANES)])


def z_pair(f):
    lane = lax.broadcasted_iota(jnp.int32, f.shape, 2)
    turned = pltpu.roll(f, LANES - 1, 2)
    after = jnp.concatenate([turned[1:], turned[:1]], 0)
    upper = jnp.where(lane == LANES - 1, after, turned)
    return f + upper, upper - f


def node_terms(sums, diffs, sums_next, diffs_next):
    result = []
    for c in range(6):
        s0, s1, d0, d1 = sums[c], sums_next[c], diffs[c], diffs_next[c]
        if c < 3:
            result.append((s0 + s1, s1 - s0, d0 + d1))
        else:
            result.append((d1 - d0, d0 + d1, s1 - s0))
    return result


def element_terms(lower, upper, stress, hour):
    eight = []
    for m in range(3):
        row = [
            upper[m][0] - lower[m][0],
            lower[m][1] + upper[m][1],
            lower[m][2] + upper[m][2],
        ]
        row[m] = row[m] + 4.0
        eight.append(row)
    cof = [
        [
            eight[(m + 1) % 3][(n + 1) % 3] * eight[(m + 2) % 3][(n + 2) % 3]
            - eight[(m + 1) % 3][(n + 2) % 3] * eight[(m + 2) % 3][(n + 1) % 3]
            for n in range(3)
        ]
        for m in range(3)
    ]
    hour = hour * 64.0
    result = []
    for m in range(3):
        line = [
            stress[VOIGT[m][0]] * cof[0][n]
            + stress[VOIGT[m][1]] * cof[1][n]
            + stress[VOIGT[m][2]] * cof[2][n]
            for n in range(3)
        ]
        low, up = lower[3 + m], upper[3 + m]
        line.append(hour * (low[0] + up[0]))
        line.append(hour * (up[1] - low[1]))
        line.append(hour * (up[2] - low[2]))
        line.append(hour * (up[0] - low[0]))
        result.append(line)
    return result


def gathered_x(before, after):
    result = []
    for m in range(3):
        p, n = before[m], after[m]
        result.append(
            (
                p[0] - n[0],
                (p[1] + n[1]) + (p[5] - n[5]),
                (p[2] + n[2]) + (p[4] - n[4]),
                (p[3] + n[3]) + (p[6] - n[6]),
            )
        )
    return result


def along_z(p, r):
    lane = lax.broadcasted_iota(jnp.int32, p.shape, 2)
    block = lax.broadcasted_iota(jnp.int32, p.shape, 0)
    nb = p.shape[0]
    up = pltpu.roll(p + r, 1, 2)
    before_up = jnp.concatenate([jnp.zeros_like(up[:1]), up[:-1]], 0)
    last = (lane == LANES - 1) & (block == nb - 1)
    return jnp.where(lane == 0, before_up, up) + jnp.where(last, 0.0, p - r)


def edge_body(u_ref, v_ref, stress_ref, hour_ref, yu, xu, xd, corner, beyond_ref, row_ref):
    planes, columns, _ = u_ref.shape[1:]
    rows = row_ref.shape[0]
    row_ref[...] = jnp.zeros(row_ref.shape, jnp.float32)

    def assembled(first, middle, last):
        row_ref[0:1, :] = first
        row_ref[1 : planes + 1, :] = middle
        if last is not None:
            row_ref[planes + 1 : planes + 2, :] = last
        return split(row_ref[...])

    def line(ref, at):
        return ref[at : at + 1, :]

    def following(q):
        return pltpu.roll(q, rows - 1, 1)

    def own(c):
        middle = component(u_ref, v_ref, stress_ref, hour_ref, c)[:, columns - 1, :]
        at = c * columns + columns - 1
        return assembled(line(xd, at), middle, line(xu, at) if c < 6 else None)

    own_s, own_d, next_s, next_d = [], [], [], []
    for c in range(6):
        s, d = z_pair(own(c))
        own_s.append(s)
        own_d.append(d)
        s, d = z_pair(assembled(line(corner, c), yu[c], line(corner, 8 + c)))
        next_s.append(s)
        next_d.append(d)
    lower = node_terms(own_s, own_d, next_s, next_d)
    upper = [tuple(following(q) for q in terms) for terms in lower]
    factors = element_terms(lower, upper, [own(6 + c) for c in range(6)], own(12))
    after = [[following(q) for q in terms] for terms in factors]
    for m, (a, b, c, e) in enumerate(gathered_x(factors, after)):
        force = along_z(a + b, c + e)[:, 0:planes]
        for k in range(force.shape[0]):
            beyond_ref[m, :, k * LANES : (k + 1) * LANES] = force[k]


def node_plane(values, halo_s, halo_d):
    row = lax.broadcasted_iota(jnp.int32, values[0].shape, 1)
    end = values[0].shape[1] - 1
    sums, diffs, sums_next, diffs_next = [], [], [], []
    for c in range(6):
        s, d = z_pair(values[c])
        sums.append(s)
        diffs.append(d)
        sums_next.append(jnp.where(row == end, halo_s[c], pltpu.roll(s, end, 1)))
        diffs_next.append(jnp.where(row == end, halo_d[c], pltpu.roll(d, end, 1)))
    return node_terms(sums, diffs, sums_next, diffs_next)


def kept_nodes(node_ref, i):
    return [tuple(node_ref[i, c, t] for t in range(3)) for c in range(6)]


def kept_elements(elem_ref, i):
    return [[elem_ref[i, m, t] for t in range(7)] for m in range(3)]


def new_velocity(before, after, velocity, mass):
    row = lax.broadcasted_iota(jnp.int32, mass.shape, 1)
    weight = (time_step / 64.0) / mass
    result = []
    for m, (a, b, c, e) in enumerate(gathered_x(before, after)):
        p = (a - b) + jnp.where(row == 0, 0.0, pltpu.roll(a + b, 1, 1))
        r = (c - e) + jnp.where(row == 0, 0.0, pltpu.roll(c + e, 1, 1))
        result.append(velocity[m] - along_z(p, r) * weight)
    return result


def steps(start, stop, unroll, body):
    count = (stop - start) // unroll

    def several(t, carry):
        for k in range(unroll):
            body(start + t * unroll + k)
        return carry

    lax.fori_loop(0, count, several, 0)
    for i in range(start + count * unroll, stop):
        body(jnp.int32(i))


def inner_body(
    unroll, u_ref, v_ref, stress_ref, hour_ref, yu, node_ref, elem_ref, halo_s, halo_d
):
    planes = u_ref.shape[1]
    for c in range(6):
        halo_s[c], halo_d[c] = z_pair(split(yu[c]))

    def nodes(i):
        values = [split(u_ref[c, i]) for c in range(3)] + [split(v_ref[c, i]) for c in range(3)]
        terms = node_plane(
            values,
            [halo_s[c, :, pl.ds(i, 1), :] for c in range(6)],
            [halo_d[c, :, pl.ds(i, 1), :] for c in range(6)],
        )
        for c in range(6):
            for t in range(3):
                node_ref[i, c, t] = terms[c][t]

    def elements(i):
        factors = element_terms(
            kept_nodes(node_ref, i),
            kept_nodes(node_ref, i + 1),
            [split(stress_ref[c, i]) for c in range(6)],
            split(hour_ref[i]),
        )
        for m in range(3):
            for t in range(7):
                elem_ref[i, m, t] = factors[m][t]

    steps(0, planes, unroll, nodes)
    steps(0, planes - 1, unroll, elements)


def outer_body(
    unroll, v_ref, stress_ref, hour_ref, mass_ref, node_ref, elem_ref, xu, xd, corner, out_ref
):
    planes, columns, depth = v_ref.shape[1:]
    last = planes - 1

    def write_plane(i, before, after):
        velocity = [split(v_ref[m, i]) for m in range(3)]
        result = new_velocity(before, after, velocity, split(mass_ref[i]))
        for m in range(3):
            for k in range(depth // LANES):
                out_ref[m, i, :, k * LANES : (k + 1) * LANES] = result[m][k]

    def inside(i):
        write_plane(i, kept_elements(elem_ref, i - 1), kept_elements(elem_ref, i))

    def part(ref, c):
        return split(ref[c * columns : (c + 1) * columns, :])

    def plane_terms(ref, at):
        halo_s, halo_d = z_pair(split(corner[at : at + 8, :]))
        return node_plane(
            [part(ref, c) for c in range(6)],
            [halo_s[:, c : c + 1] for c in range(6)],
            [halo_d[:, c : c + 1] for c in range(6)],
        )

    below = element_terms(
        plane_terms(xd, 0),
        kept_nodes(node_ref, 0),
        [part(xd, 6 + c) for c in range(6)],
        part(xd, 12),
    )
    above = element_terms(
        kept_nodes(node_ref, last),
        plane_terms(xu, 8),
        [split(stress_ref[c, last]) for c in range(6)],
        split(hour_ref[last]),
    )
    write_plane(0, below, kept_elements(elem_ref, 0))
    write_plane(last, kept_elements(elem_ref, last - 1), above)
    steps(1, last, unroll, inside)


def final_body(
    capacity, pack,
    base_ref, mass_ref, table_ref, route_ref, left_ref,
    out_hbm, rows_ref, out_ref, dense_ref, sems,
):
    planes, columns, depth = base_ref.shape[1:]
    offset = (lax.axis_index("space") % pack) * capacity
    dense = dense_rows(table_ref, dense_ref, capacity, pack, offset)
    (contact,) = looked_up(dense_ref, [route_ref[...]], dense)
    rows_ref[...] = jnp.zeros(rows_ref.shape, jnp.float32)
    lane = lax.broadcasted_iota(jnp.int32, (planes, columns, LANES), 2)
    row = lax.broadcasted_iota(jnp.int32, (columns, LANES), 0)
    weights = [time_step / mass_ref[:, :, k : k + LANES] for k in range(0, depth, LANES)]
    low_weight = jnp.where(lane == 0, weights[0], 0.0)
    high_weight = jnp.where(lane == LANES - 1, weights[-1], 0.0)
    copies = []
    for m in range(3):
        rows_ref[m, 0:1, :] = contact[m][0:1]
        rows_ref[m, LANES - 1 : LANES, :] = contact[m][1:2]
        turned = rows_ref[m].T.reshape(planes, columns, LANES)
        for k in range(0, depth, LANES):
            left = jnp.stack(
                [
                    jnp.where(row == 0, left_ref[m, i : i + 1, k : k + LANES] * (1.0 / 64.0), 0.0)
                    for i in range(planes)
                ]
            )
            value = base_ref[m, :, :, k : k + LANES] - left * weights[k // LANES]
            if k == 0:
                value = value + low_weight * turned
            if k == depth - LANES:
                value = value + high_weight * turned
            out_ref[m, :, :, k : k + LANES] = value
        copies.append(pltpu.make_async_copy(out_ref.at[m], out_hbm.at[m], sems.at[m]))
        copies[m].start()
    for copy in copies:
        copy.wait()


def local(
    displacement,
    velocity,
    stress,
    hourglass,
    mass,
    contact_route,
    pair_nodes,
    pair_diagonals,
    pair_gap,
    pair_stiffness,
):
    planes, columns, depth = displacement.shape[1:]
    nspace = lax.axis_size("space")
    surf_count = 2 * planes * columns
    pairs = pair_nodes.shape[1]
    capacity, pack, blocks = layout(nspace, surf_count)
    f32 = jnp.float32
    lines = pairs // LANES

    def sized(*shape):
        return jax.ShapeDtypeStruct(shape, f32)

    message = sized(nspace, 8, LANES)
    small = (pair_nodes, pair_diagonals, pair_gap.reshape(lines, LANES))
    small += (pair_stiffness.reshape(lines, LANES),)
    kept = (displacement, velocity, stress, hourglass, mass) + small
    outgoing, ydn, xdn, xup, sides, *kept = kernel_call(
        functools.partial(first_body, capacity, pack, blocks),
        (displacement, contact_route.reshape(1, surf_count)) + kept[1:],
        (
            pltpu.HBM(message.shape, f32),
            sized(6, planes, depth),
            sized(6 * columns, depth),
            sized(13 * columns, depth),
            jax.ShapeDtypeStruct((2, surf_count // 2), jnp.int32),
            *(jax.ShapeDtypeStruct(one.shape, one.dtype) for one in kept),
        ),
        [
            pltpu.VMEM(message.shape, f32),
            pltpu.VMEM((8, surf_count), f32),
            pltpu.VMEM((1, surf_count), jnp.int32),
            pltpu.SemaphoreType.DMA((len(kept) + 1,)),
            pltpu.SemaphoreType.DMA,
        ],
        hbm_inputs=len(kept) + 1,
    )
    fields, (pair_nodes, pair_diagonals, gap, stiffness) = kept[:5], kept[5:]
    received = exchanged(outgoing)
    yu = shifted(ydn, "slab", -1)
    xu = shifted(xdn, "space", -1)
    xd = shifted(xup, "space", 1)
    slots = (nspace * capacity + 15) // 16 * 16
    matrix, nodes, diagonals = kernel_call(
        matrix_body,
        (pair_nodes, pair_diagonals),
        (
            jax.ShapeDtypeStruct((slots, pairs), jnp.bfloat16),
            jax.ShapeDtypeStruct((5, lines, LANES), jnp.int32),
            sized(6, lines, LANES),
        ),
    )
    dense = pltpu.VMEM((pl.cdiv(nspace, LANES // capacity), 8, LANES), f32)
    slot_force = kernel_call(
        functools.partial(pair_body, capacity, pack, blocks),
        (received, nodes, diagonals, gap, stiffness, matrix),
        pltpu.HBM(message.shape, f32),
        [
            pltpu.VMEM((8, pairs), f32),
            pltpu.VMEM(message.shape, f32),
            dense,
            pltpu.SemaphoreType.DMA,
        ],
    )
    returned = exchanged(slot_force)

    corner = kernel_call(functools.partial(corner_body, columns), (xu, xd), sized(16, depth))
    corner = shifted(corner, "slab", -1)
    nb = depth // LANES
    node, elem = kernel_call(
        functools.partial(inner_body, 2),
        (*fields[:4], yu),
        (
            sized(planes, 6, 3, nb, columns, LANES),
            sized(planes - 1, 3, 7, nb, columns, LANES),
        ),
        [
            pltpu.VMEM((6, nb, planes, LANES), f32),
            pltpu.VMEM((6, nb, planes, LANES), f32),
        ],
    )
    rows = (planes + 2 + 7) // 8 * 8
    beyond = kernel_call(
        edge_body,
        (*fields[:4], yu, xu, xd, corner),
        sized(3, planes, depth),
        [pltpu.VMEM((rows, depth), f32)],
    )
    left = shifted(beyond, "slab", 1)
    base = kernel_call(
        functools.partial(outer_body, 2),
        (*fields[1:], node, elem, xu, xd, corner),
        sized(*displacement.shape),
    )

    return kernel_call(
        functools.partial(final_body, capacity, pack),
        (base, fields[4], returned, sides, left),
        pltpu.HBM(displacement.shape, f32),
        [
            pltpu.VMEM((3, LANES, LANES), f32),
            pltpu.VMEM(displacement.shape, f32),
            dense,
            pltpu.SemaphoreType.DMA((3,)),
        ],
    )


def solution(mesh):
    in_specs = (
        P(None, "space", "slab", None),
        P(None, "space", "slab", None),
        P(None, "space", "slab", None),
        P("space", "slab", None),
        P("space", "slab", None),
        P(("space", "slab")),
        P(None, ("space", "slab")),
        P(None, ("space", "slab")),
        P(("space", "slab")),
        P(("space", "slab")),
    )
    out_specs = P(None, "space", "slab", None)
    return jax.shard_map(local, mesh=mesh, in_specs=in_specs, out_specs=out_specs, check_vma=False)
```

```python
import functools

import jax
import jax.numpy as jnp
from jax import lax
from jax.experimental import pallas as pl
from jax.experimental.pallas import tpu as pltpu
from jax.sharding import PartitionSpec as P


time_step = 0.5
LANES = 128
VOIGT = [[0, 5, 4], [5, 1, 3], [4, 3, 2]]


def shifted(value, axis, steps):
    count = lax.axis_size(axis)
    return lax.ppermute(value, axis, [(at, (at + steps) % count) for at in range(count)])


def exchanged(value):
    count = lax.axis_size("space")
    order = [(at + count // 4) % count for at in range(count)]
    return lax.all_to_all(
        value, "space", split_axis=0, concat_axis=0, tiled=True, axis_index_groups=[order]
    )


def seat(at, count):
    return (at - count // 4) % count


def kernel_call(body, inputs, outs, scratch=(), hbm_inputs=0):
    spaces = [pltpu.HBM if at < hbm_inputs else pltpu.VMEM for at in range(len(inputs))]
    inputs = [pltpu.with_memory_space_constraint(*pair) for pair in zip(inputs, spaces)]

    def placed(out):
        if isinstance(out, jax.ShapeDtypeStruct):
            return pltpu.VMEM(out.shape, out.dtype)
        return out

    outs = tuple(placed(out) for out in outs) if isinstance(outs, tuple) else placed(outs)
    return pl.pallas_call(
        body,
        out_shape=outs,
        in_specs=[pl.BlockSpec(memory_space=one) for one in spaces],
        out_specs=jax.tree.map(lambda out: pl.BlockSpec(memory_space=out.memory_space), outs),
        scratch_shapes=list(scratch),
        compiler_params=pltpu.CompilerParams(vmem_limit_bytes=16 << 20),
    )(*inputs)


def contract_lanes(lhs, rhs):
    return lax.dot_general(lhs, rhs, (((1,), (1,)), ((), ())), preferred_element_type=jnp.float32)


def layout(nspace, surf_count):
    capacity = max(2, (3 * surf_count // 2 + nspace - 1) // nspace)
    pack = max(1, min(LANES // capacity, nspace // 8))
    while nspace % pack:
        pack -= 1
    return capacity, pack, nspace // pack


def block_of(slots, width, blocks):
    block = jnp.zeros_like(slots)
    for b in range(1, blocks):
        block = block + jnp.where(slots >= b * width, 1, 0)
    return block, slots - block * width


def parts_of(rows):
    high = rows.astype(jnp.bfloat16).astype(jnp.float32)
    rest = rows - high
    middle = rest.astype(jnp.bfloat16).astype(jnp.float32)
    return [high, middle, rest - middle]


def places(place, width):
    rows = (width + 15) // 16 * 16
    count = place.shape[1]
    at = lax.broadcasted_iota(jnp.int32, (rows, count), 0)
    return jnp.where(at == place, 1.0, 0.0).astype(jnp.bfloat16)


def spread(parts, block, blocks):
    return [
        jnp.where(block == b, part, 0.0).astype(jnp.bfloat16)
        for part in parts
        for b in range(blocks)
    ]


def write_messages(out_ref, got, pack, blocks):
    for b in range(blocks):
        at = [(part * blocks + b) * 8 for part in range(3)]
        total = got[at[0] : at[0] + 8] + got[at[1] : at[1] + 8] + got[at[2] : at[2] + 8]
        for q in range(pack):
            out_ref[seat(b * pack + q, out_ref.shape[0]), :, 0 : total.shape[1]] = total


def first_body(
    capacity, pack, blocks, u_hbm, route_hbm, v_hbm, *rest,
):
    hbm, rest = (u_hbm, route_hbm, v_hbm) + rest[:7], rest[7:]
    message_hbm, ydn, yup, xdn, xup, sides_ref, u_ref, v_ref, stress_ref, hour_ref = rest[:10]
    out_ref, rows_ref, route_ref, sems, message_sem = rest[-5:]
    targets = (u_ref, route_ref, v_ref, stress_ref, hour_ref) + rest[10:-5]
    copies = [
        pltpu.make_async_copy(source, target, sems.at[at])
        for at, (source, target) in enumerate(zip(hbm, targets))
    ]
    for copy in copies:
        copy.start()
    out_ref[...] = jnp.zeros(out_ref.shape, jnp.float32)
    rows_ref[...] = jnp.zeros(rows_ref.shape, jnp.float32)
    copies[0].wait()
    copies[1].wait()
    planes, columns, depth = u_ref.shape[1:]
    side = planes * columns
    lane = lax.broadcasted_iota(jnp.int32, (side, LANES), 1)
    for c in range(3):
        bottom = u_ref[c, :, :, 0:LANES].reshape(side, LANES)
        top = u_ref[c, :, :, depth - LANES : depth].reshape(side, LANES)
        both = jnp.where(lane == LANES - 1, top, bottom).T
        rows_ref[c : c + 1, 0:side] = both[0:1]
        rows_ref[c : c + 1, side : 2 * side] = both[LANES - 1 : LANES]
    width = pack * capacity
    route = route_ref[...]
    block, place = block_of(route, width, blocks)
    entries = spread(parts_of(rows_ref[...]), block, blocks)
    got = contract_lanes(jnp.concatenate(entries, 0), places(place, width))
    write_messages(out_ref, got, pack, blocks)
    message = pltpu.make_async_copy(out_ref, message_hbm, message_sem)
    message.start()
    sides_ref[0:1, :] = route[:, 0:side]
    sides_ref[1:2, :] = route[:, side : 2 * side]
    for copy in copies[2:5]:
        copy.wait()
    for c in range(13):
        ref = component(u_ref, v_ref, stress_ref, hour_ref, c)
        xup[c * columns : (c + 1) * columns, :] = ref[planes - 1]
        yup[c] = ref[:, columns - 1, :]
        if c < 6:
            xdn[c * columns : (c + 1) * columns, :] = ref[0]
            ydn[c] = ref[:, 0, :]
    for copy in copies[5:]:
        copy.wait()
    message.wait()


def component(u_ref, v_ref, stress_ref, hour_ref, c):
    if c < 3:
        return u_ref.at[c]
    if c < 6:
        return v_ref.at[c - 3]
    if c < 12:
        return stress_ref.at[c - 6]
    return hour_ref


def corner_body(columns, xu, xd, left_ref, right_ref):
    left_ref[...] = jnp.zeros(left_ref.shape, jnp.float32)
    right_ref[...] = jnp.zeros(right_ref.shape, jnp.float32)
    for c in range(13):
        at = c * columns
        right_ref[c : c + 1, :] = xd[at + columns - 1 : at + columns, :]
        if c < 6:
            left_ref[c : c + 1, :] = xd[at : at + 1, :]
            left_ref[8 + c : 9 + c, :] = xu[at : at + 1, :]
            right_ref[16 + c : 17 + c, :] = xu[at + columns - 1 : at + columns, :]


def matrix_body(nodes_ref, diag_ref, matrix_ref, lines_ref, diag_lines_ref):
    pairs = nodes_ref.shape[1]
    group = 16

    def rows(g, carry):
        start = pl.multiple_of(g * group, group)
        slot = lax.broadcasted_iota(jnp.int32, (group, pairs), 0) + start
        total = jnp.where(nodes_ref[0:1, :] == slot, 1.0, 0.0)
        for j in range(1, 5):
            total = total - jnp.where(nodes_ref[j : j + 1, :] == slot, 0.25, 0.0)
        matrix_ref[pl.ds(start, group), :] = total.astype(jnp.bfloat16)
        return carry

    lax.fori_loop(0, matrix_ref.shape[0] // group, rows, 0)
    for r in range(pairs // LANES):
        for j in range(5):
            lines_ref[j, r : r + 1, :] = nodes_ref[j : j + 1, r * LANES : (r + 1) * LANES]
        for c in range(6):
            diag_lines_ref[c, r : r + 1, :] = diag_ref[c : c + 1, r * LANES : (r + 1) * LANES]


def dense_rows(table_ref, rows_ref, capacity, pack, offset):
    together = LANES // capacity
    lane = lax.broadcasted_iota(jnp.int32, (8, LANES), 1)
    for b in range(rows_ref.shape[0]):
        total = None
        for q in range(min(together, table_ref.shape[0] - b * together)):
            tile = table_ref[seat(b * together + q, table_ref.shape[0])]
            if pack > 1:
                tile = jnp.where((lane >= offset) & (lane < offset + capacity), tile, 0.0)
                tile = pltpu.roll(tile, (q * capacity - offset) & (LANES - 1), 1)
            elif q:
                tile = pltpu.roll(tile, q * capacity, 1)
            total = tile if total is None else total + tile
        rows_ref[b] = total
    return together * capacity


def looked_up(rows_ref, slots, width):
    shape = slots[0].shape
    found = [[None] * 3 for _ in slots]
    for b in range(rows_ref.shape[0]):
        rows = [jnp.broadcast_to(rows_ref[b, c : c + 1, :], shape) for c in range(3)]
        for slot, old in zip(slots, found):
            place = slot - b * width
            here = place >= 0
            for c in range(3):
                new = jnp.take_along_axis(rows[c], place & (LANES - 1), axis=1)
                old[c] = jnp.where(here, new, old[c]) if b else new
    return found


def pair_body(
    capacity, pack, blocks,
    table_ref, nodes_ref, diag_ref, gap_ref, stiff_ref, matrix_ref,
    out_hbm, rows_ref, out_ref, dense_ref, sem,
):
    offset = (lax.axis_index("space") % pack) * capacity
    dense = dense_rows(table_ref, dense_ref, capacity, pack, offset)
    picked = looked_up(dense_ref, [nodes_ref[j] for j in range(5)], dense)
    slave = picked[0]
    first = [diag_ref[c] + picked[3][c] - picked[1][c] for c in range(3)]
    second = [diag_ref[3 + c] + picked[4][c] - picked[2][c] for c in range(3)]
    normal = [
        first[(c + 1) % 3] * second[(c + 2) % 3] - first[(c + 2) % 3] * second[(c + 1) % 3]
        for c in range(3)
    ]
    gap = gap_ref[...]
    for c in range(3):
        centre = (picked[1][c] + picked[2][c] + picked[3][c] + picked[4][c]) * 0.25
        gap = gap + (slave[c] - centre) * normal[c]
    push = stiff_ref[...] * jnp.maximum(-gap, 0.0)
    out_ref[...] = jnp.zeros(out_ref.shape, jnp.float32)
    rows_ref[...] = jnp.zeros(rows_ref.shape, jnp.float32)
    for c in range(3):
        force = push * normal[c]
        for r in range(force.shape[0]):
            rows_ref[c : c + 1, r * LANES : (r + 1) * LANES] = force[r : r + 1]
    parts = [part.astype(jnp.bfloat16) for part in parts_of(rows_ref[...])]
    got = contract_lanes(jnp.concatenate(parts, 0), matrix_ref[...])
    total = got[0:8] + got[8:16] + got[16:24]
    width = pack * capacity
    for b in range(blocks):
        for q in range(pack):
            block = total[:, b * width : (b + 1) * width]
            out_ref[seat(b * pack + q, out_ref.shape[0]), :, 0:width] = block
    copy = pltpu.make_async_copy(out_ref, out_hbm, sem)
    copy.start()
    copy.wait()


def split(value):
    return jnp.stack([value[:, at : at + LANES] for at in range(0, value.shape[1], LANES)])


def z_pair(f):
    lane = lax.broadcasted_iota(jnp.int32, f.shape, 2)
    turned = pltpu.roll(f, LANES - 1, 2)
    after = jnp.concatenate([turned[1:], turned[:1]], 0)
    upper = jnp.where(lane == LANES - 1, after, turned)
    return f + upper, upper - f


def node_terms(sums, diffs, sums_next, diffs_next):
    result = []
    for c in range(6):
        s0, s1, d0, d1 = sums[c], sums_next[c], diffs[c], diffs_next[c]
        if c < 3:
            result.append((s0 + s1, s1 - s0, d0 + d1))
        else:
            result.append((d1 - d0, d0 + d1, s1 - s0))
    return result


def element_terms(lower, upper, stress, hour):
    eight = []
    for m in range(3):
        row = [
            upper[m][0] - lower[m][0],
            lower[m][1] + upper[m][1],
            lower[m][2] + upper[m][2],
        ]
        row[m] = row[m] + 4.0
        eight.append(row)
    cof = [
        [
            eight[(m + 1) % 3][(n + 1) % 3] * eight[(m + 2) % 3][(n + 2) % 3]
            - eight[(m + 1) % 3][(n + 2) % 3] * eight[(m + 2) % 3][(n + 1) % 3]
            for n in range(3)
        ]
        for m in range(3)
    ]
    hour = hour * 64.0
    result = []
    for m in range(3):
        line = [
            stress[VOIGT[m][0]] * cof[0][n]
            + stress[VOIGT[m][1]] * cof[1][n]
            + stress[VOIGT[m][2]] * cof[2][n]
            for n in range(3)
        ]
        low, up = lower[3 + m], upper[3 + m]
        line.append(hour * (low[0] + up[0]))
        line.append(hour * (up[1] - low[1]))
        line.append(hour * (up[2] - low[2]))
        line.append(hour * (up[0] - low[0]))
        result.append(line)
    return result


def gathered_x(before, after):
    result = []
    for m in range(3):
        p, n = before[m], after[m]
        result.append(
            (
                p[0] - n[0],
                (p[1] + n[1]) + (p[5] - n[5]),
                (p[2] + n[2]) + (p[4] - n[4]),
                (p[3] + n[3]) + (p[6] - n[6]),
            )
        )
    return result


def along_z(p, r):
    lane = lax.broadcasted_iota(jnp.int32, p.shape, 2)
    block = lax.broadcasted_iota(jnp.int32, p.shape, 0)
    nb = p.shape[0]
    up = pltpu.roll(p + r, 1, 2)
    before_up = jnp.concatenate([jnp.zeros_like(up[:1]), up[:-1]], 0)
    last = (lane == LANES - 1) & (block == nb - 1)
    return jnp.where(lane == 0, before_up, up) + jnp.where(last, 0.0, p - r)


def edge_body(columns, ydn, yd, xu, xd, corner, out_ref, row_ref):
    planes = ydn.shape[1]
    rows = row_ref.shape[0]
    row_ref[...] = jnp.zeros(row_ref.shape, jnp.float32)

    def assembled(first, middle, last):
        row_ref[0:1, :] = first
        row_ref[1 : planes + 1, :] = middle
        if last is not None:
            row_ref[planes + 1 : planes + 2, :] = last
        return split(row_ref[...])

    def line(ref, at):
        return ref[at : at + 1, :]

    def following(q):
        return pltpu.roll(q, rows - 1, 1)

    left_s, left_d, own_s, own_d = [], [], [], []
    for c in range(6):
        s, d = z_pair(assembled(line(corner, c), yd[c], line(corner, 16 + c)))
        left_s.append(s)
        left_d.append(d)
        s, d = z_pair(assembled(line(xd, c * columns), ydn[c], line(xu, c * columns)))
        own_s.append(s)
        own_d.append(d)
    stress = [assembled(line(corner, 6 + c), yd[6 + c], None) for c in range(6)]
    hour = assembled(line(corner, 12), yd[12], None)
    lower = node_terms(left_s, left_d, own_s, own_d)
    upper = [tuple(following(q) for q in terms) for terms in lower]
    factors = element_terms(lower, upper, stress, hour)
    after = [[following(q) for q in terms] for terms in factors]
    for m, (a, b, c, e) in enumerate(gathered_x(factors, after)):
        out_ref[m, 0] = a + b
        out_ref[m, 1] = c + e


def node_plane(values, halo_s, halo_d):
    row = lax.broadcasted_iota(jnp.int32, values[0].shape, 1)
    end = values[0].shape[1] - 1
    sums, diffs, sums_next, diffs_next = [], [], [], []
    for c in range(6):
        s, d = z_pair(values[c])
        sums.append(s)
        diffs.append(d)
        sums_next.append(jnp.where(row == end, halo_s[c], pltpu.roll(s, end, 1)))
        diffs_next.append(jnp.where(row == end, halo_d[c], pltpu.roll(d, end, 1)))
    return node_terms(sums, diffs, sums_next, diffs_next)


def kept_nodes(node_ref, i):
    return [tuple(node_ref[i, c, t] for t in range(3)) for c in range(6)]


def kept_elements(elem_ref, i):
    return [[elem_ref[i, m, t] for t in range(7)] for m in range(3)]


def new_velocity(before, after, left, velocity, mass):
    row = lax.broadcasted_iota(jnp.int32, mass.shape, 1)
    weight = (time_step / 64.0) / mass
    result = []
    for m, (a, b, c, e) in enumerate(gathered_x(before, after)):
        p = (a - b) + jnp.where(row == 0, left[m][0], pltpu.roll(a + b, 1, 1))
        r = (c - e) + jnp.where(row == 0, left[m][1], pltpu.roll(c + e, 1, 1))
        result.append(velocity[m] - along_z(p, r) * weight)
    return result


def steps(start, stop, unroll, body):
    count = (stop - start) // unroll

    def several(t, carry):
        for k in range(unroll):
            body(start + t * unroll + k)
        return carry

    lax.fori_loop(0, count, several, 0)
    for i in range(start + count * unroll, stop):
        body(jnp.int32(i))


def inner_body(
    unroll, u_ref, v_ref, stress_ref, hour_ref, yu, node_ref, elem_ref, halo_s, halo_d
):
    planes = u_ref.shape[1]
    for c in range(6):
        halo_s[c], halo_d[c] = z_pair(split(yu[c]))

    def nodes(i):
        values = [split(u_ref[c, i]) for c in range(3)] + [split(v_ref[c, i]) for c in range(3)]
        terms = node_plane(
            values,
            [halo_s[c, :, pl.ds(i, 1), :] for c in range(6)],
            [halo_d[c, :, pl.ds(i, 1), :] for c in range(6)],
        )
        for c in range(6):
            for t in range(3):
                node_ref[i, c, t] = terms[c][t]

    def elements(i):
        factors = element_terms(
            kept_nodes(node_ref, i),
            kept_nodes(node_ref, i + 1),
            [split(stress_ref[c, i]) for c in range(6)],
            split(hour_ref[i]),
        )
        for m in range(3):
            for t in range(7):
                elem_ref[i, m, t] = factors[m][t]

    steps(0, planes, unroll, nodes)
    steps(0, planes - 1, unroll, elements)


def outer_body(
    unroll, v_ref, stress_ref, hour_ref, mass_ref, node_ref, elem_ref, edge_ref, xu, xd, corner,
    out_ref,
):
    planes, columns, depth = v_ref.shape[1:]
    last = planes - 1

    def write_plane(i, before, after):
        velocity = [split(v_ref[m, i]) for m in range(3)]
        left = [[edge_ref[m, t, :, pl.ds(i, 1), :] for t in range(2)] for m in range(3)]
        result = new_velocity(before, after, left, velocity, split(mass_ref[i]))
        for m in range(3):
            for k in range(depth // LANES):
                out_ref[m, i, :, k * LANES : (k + 1) * LANES] = result[m][k]

    def inside(i):
        write_plane(i, kept_elements(elem_ref, i - 1), kept_elements(elem_ref, i))

    def part(ref, c):
        return split(ref[c * columns : (c + 1) * columns, :])

    def plane_terms(ref, at):
        halo_s, halo_d = z_pair(split(corner[at : at + 8, :]))
        return node_plane(
            [part(ref, c) for c in range(6)],
            [halo_s[:, c : c + 1] for c in range(6)],
            [halo_d[:, c : c + 1] for c in range(6)],
        )

    below = element_terms(
        plane_terms(xd, 0),
        kept_nodes(node_ref, 0),
        [part(xd, 6 + c) for c in range(6)],
        part(xd, 12),
    )
    above = element_terms(
        kept_nodes(node_ref, last),
        plane_terms(xu, 8),
        [split(stress_ref[c, last]) for c in range(6)],
        split(hour_ref[last]),
    )
    write_plane(0, below, kept_elements(elem_ref, 0))
    write_plane(last, kept_elements(elem_ref, last - 1), above)
    steps(1, last, unroll, inside)


def final_body(
    capacity, pack,
    base_ref, mass_ref, table_ref, route_ref,
    out_hbm, rows_ref, out_ref, dense_ref, sems,
):
    planes, columns, depth = base_ref.shape[1:]
    offset = (lax.axis_index("space") % pack) * capacity
    dense = dense_rows(table_ref, dense_ref, capacity, pack, offset)
    (contact,) = looked_up(dense_ref, [route_ref[...]], dense)
    rows_ref[...] = jnp.zeros(rows_ref.shape, jnp.float32)
    lane = lax.broadcasted_iota(jnp.int32, (planes, columns, LANES), 2)
    low_weight = jnp.where(lane == 0, time_step / mass_ref[:, :, 0:LANES], 0.0)
    high_weight = jnp.where(
        lane == LANES - 1, time_step / mass_ref[:, :, depth - LANES : depth], 0.0
    )
    copies = []
    for m in range(3):
        rows_ref[m, 0:1, :] = contact[m][0:1]
        rows_ref[m, LANES - 1 : LANES, :] = contact[m][1:2]
        turned = rows_ref[m].T.reshape(planes, columns, LANES)
        for k in range(0, depth, LANES):
            value = base_ref[m, :, :, k : k + LANES]
            if k == 0:
                value = value + low_weight * turned
            if k == depth - LANES:
                value = value + high_weight * turned
            out_ref[m, :, :, k : k + LANES] = value
        copies.append(pltpu.make_async_copy(out_ref.at[m], out_hbm.at[m], sems.at[m]))
        copies[m].start()
    for copy in copies:
        copy.wait()


def local(
    displacement,
    velocity,
    stress,
    hourglass,
    mass,
    contact_route,
    pair_nodes,
    pair_diagonals,
    pair_gap,
    pair_stiffness,
):
    planes, columns, depth = displacement.shape[1:]
    nspace = lax.axis_size("space")
    surf_count = 2 * planes * columns
    pairs = pair_nodes.shape[1]
    capacity, pack, blocks = layout(nspace, surf_count)
    f32 = jnp.float32
    lines = pairs // LANES

    def sized(*shape):
        return jax.ShapeDtypeStruct(shape, f32)

    message = sized(nspace, 8, LANES)
    small = (pair_nodes, pair_diagonals, pair_gap.reshape(lines, LANES))
    small += (pair_stiffness.reshape(lines, LANES),)
    kept = (displacement, velocity, stress, hourglass, mass) + small
    outgoing, ydn, yup, xdn, xup, sides, *kept = kernel_call(
        functools.partial(first_body, capacity, pack, blocks),
        (displacement, contact_route.reshape(1, surf_count)) + kept[1:],
        (
            pltpu.HBM(message.shape, f32),
            sized(6, planes, depth),
            sized(13, planes, depth),
            sized(6 * columns, depth),
            sized(13 * columns, depth),
            jax.ShapeDtypeStruct((2, surf_count // 2), jnp.int32),
            *(jax.ShapeDtypeStruct(one.shape, one.dtype) for one in kept),
        ),
        [
            pltpu.VMEM(message.shape, f32),
            pltpu.VMEM((8, surf_count), f32),
            pltpu.VMEM((1, surf_count), jnp.int32),
            pltpu.SemaphoreType.DMA((len(kept) + 1,)),
            pltpu.SemaphoreType.DMA,
        ],
        hbm_inputs=len(kept) + 1,
    )
    fields, (pair_nodes, pair_diagonals, gap, stiffness) = kept[:5], kept[5:]
    received = exchanged(outgoing)
    yu = shifted(ydn, "slab", -1)
    yd = shifted(yup, "slab", 1)
    xu = shifted(xdn, "space", -1)
    xd = shifted(xup, "space", 1)
    slots = (nspace * capacity + 15) // 16 * 16
    matrix, nodes, diagonals = kernel_call(
        matrix_body,
        (pair_nodes, pair_diagonals),
        (
            jax.ShapeDtypeStruct((slots, pairs), jnp.bfloat16),
            jax.ShapeDtypeStruct((5, lines, LANES), jnp.int32),
            sized(6, lines, LANES),
        ),
    )
    dense = pltpu.VMEM((pl.cdiv(nspace, LANES // capacity), 8, LANES), f32)
    slot_force = kernel_call(
        functools.partial(pair_body, capacity, pack, blocks),
        (received, nodes, diagonals, gap, stiffness, matrix),
        pltpu.HBM(message.shape, f32),
        [
            pltpu.VMEM((8, pairs), f32),
            pltpu.VMEM(message.shape, f32),
            dense,
            pltpu.SemaphoreType.DMA,
        ],
    )
    returned = exchanged(slot_force)

    to_left, to_right = kernel_call(
        functools.partial(corner_body, columns), (xu, xd), (sized(16, depth), sized(24, depth))
    )
    right_corner = shifted(to_left, "slab", -1)
    left_corner = shifted(to_right, "slab", 1)
    nb = depth // LANES
    node, elem = kernel_call(
        functools.partial(inner_body, 2),
        (*fields[:4], yu),
        (
            sized(planes, 6, 3, nb, columns, LANES),
            sized(planes - 1, 3, 7, nb, columns, LANES),
        ),
        [
            pltpu.VMEM((6, nb, planes, LANES), f32),
            pltpu.VMEM((6, nb, planes, LANES), f32),
        ],
    )
    rows = (planes + 2 + 7) // 8 * 8
    edge = kernel_call(
        functools.partial(edge_body, columns),
        (ydn, yd, xu, xd, left_corner),
        sized(3, 2, nb, rows, LANES),
        [pltpu.VMEM((rows, depth), f32)],
    )
    base = kernel_call(
        functools.partial(outer_body, 2),
        (*fields[1:], node, elem, edge, xu, xd, right_corner),
        sized(*displacement.shape),
    )

    return kernel_call(
        functools.partial(final_body, capacity, pack),
        (base, fields[4], returned, sides),
        pltpu.HBM(displacement.shape, f32),
        [
            pltpu.VMEM((3, LANES, LANES), f32),
            pltpu.VMEM(displacement.shape, f32),
            dense,
            pltpu.SemaphoreType.DMA((3,)),
        ],
    )


def solution(mesh):
    in_specs = (
        P(None, "space", "slab", None),
        P(None, "space", "slab", None),
        P(None, "space", "slab", None),
        P("space", "slab", None),
        P("space", "slab", None),
        P(("space", "slab")),
        P(None, ("space", "slab")),
        P(None, ("space", "slab")),
        P(("space", "slab")),
        P(("space", "slab")),
    )
    out_specs = P(None, "space", "slab", None)
    return jax.shard_map(local, mesh=mesh, in_specs=in_specs, out_specs=out_specs, check_vma=False)
```

```python
import functools

import jax
import jax.numpy as jnp
from jax import lax
from jax.experimental import pallas as pl
from jax.experimental.pallas import tpu as pltpu
from jax.sharding import PartitionSpec as P


time_step = 0.5
LANES = 128
VOIGT = [[0, 5, 4], [5, 1, 3], [4, 3, 2]]


def shifted(value, axis, steps):
    count = lax.axis_size(axis)
    return lax.ppermute(value, axis, [(at, (at + steps) % count) for at in range(count)])


def exchanged(value):
    count = lax.axis_size("space")
    order = [(at + count // 4) % count for at in range(count)]
    return lax.all_to_all(
        value, "space", split_axis=0, concat_axis=0, tiled=True, axis_index_groups=[order]
    )


def seat(at, count):
    return (at - count // 4) % count


def kernel_call(body, inputs, outs, scratch=(), hbm_inputs=0):
    spaces = [pltpu.HBM if at < hbm_inputs else pltpu.VMEM for at in range(len(inputs))]
    inputs = [pltpu.with_memory_space_constraint(*pair) for pair in zip(inputs, spaces)]

    def placed(out):
        if isinstance(out, jax.ShapeDtypeStruct):
            return pltpu.VMEM(out.shape, out.dtype)
        return out

    outs = tuple(placed(out) for out in outs) if isinstance(outs, tuple) else placed(outs)
    return pl.pallas_call(
        body,
        out_shape=outs,
        in_specs=[pl.BlockSpec(memory_space=one) for one in spaces],
        out_specs=jax.tree.map(lambda out: pl.BlockSpec(memory_space=out.memory_space), outs),
        scratch_shapes=list(scratch),
        compiler_params=pltpu.CompilerParams(vmem_limit_bytes=16 << 20),
    )(*inputs)


def contract_lanes(lhs, rhs):
    return lax.dot_general(lhs, rhs, (((1,), (1,)), ((), ())), preferred_element_type=jnp.float32)


def layout(nspace, surf_count):
    capacity = max(2, (3 * surf_count // 2 + nspace - 1) // nspace)
    pack = max(1, min(LANES // capacity, nspace // 8))
    while nspace % pack:
        pack -= 1
    return capacity, pack, nspace // pack


def block_of(slots, width, blocks):
    block = jnp.zeros_like(slots)
    for b in range(1, blocks):
        block = block + jnp.where(slots >= b * width, 1, 0)
    return block, slots - block * width


def parts_of(rows):
    high = rows.astype(jnp.bfloat16).astype(jnp.float32)
    rest = rows - high
    middle = rest.astype(jnp.bfloat16).astype(jnp.float32)
    return [high, middle, rest - middle]


def places(place, width):
    rows = (width + 15) // 16 * 16
    count = place.shape[1]
    at = lax.broadcasted_iota(jnp.int32, (rows, count), 0)
    return jnp.where(at == place, 1.0, 0.0).astype(jnp.bfloat16)


def spread(parts, block, blocks):
    return [
        jnp.where(block == b, part, 0.0).astype(jnp.bfloat16)
        for part in parts
        for b in range(blocks)
    ]


def write_messages(out_ref, got, pack, blocks):
    for b in range(blocks):
        at = [(part * blocks + b) * 8 for part in range(3)]
        total = got[at[0] : at[0] + 8] + got[at[1] : at[1] + 8] + got[at[2] : at[2] + 8]
        for q in range(pack):
            out_ref[seat(b * pack + q, out_ref.shape[0]), :, 0 : total.shape[1]] = total


def first_body(
    capacity, pack, blocks, u_hbm, route_hbm, v_hbm, *rest,
):
    hbm, rest = (u_hbm, route_hbm, v_hbm) + rest[:7], rest[7:]
    message_hbm, xdn_hbm, xup_hbm, ydn, yup, sides_ref = rest[:6]
    u_ref, v_ref, stress_ref, hour_ref = rest[6:10]
    out_ref, xdn, xup, rows_ref, route_ref, sems, out_sems = rest[-7:]
    targets = (u_ref, route_ref, v_ref, stress_ref, hour_ref) + rest[10:-7]
    copies = [
        pltpu.make_async_copy(source, target, sems.at[at])
        for at, (source, target) in enumerate(zip(hbm, targets))
    ]
    for copy in copies:
        copy.start()
    out_ref[...] = jnp.zeros(out_ref.shape, jnp.float32)
    rows_ref[...] = jnp.zeros(rows_ref.shape, jnp.float32)
    copies[0].wait()
    copies[1].wait()
    planes, columns, depth = u_ref.shape[1:]
    side = planes * columns
    lane = lax.broadcasted_iota(jnp.int32, (side, LANES), 1)
    for c in range(3):
        bottom = u_ref[c, :, :, 0:LANES].reshape(side, LANES)
        top = u_ref[c, :, :, depth - LANES : depth].reshape(side, LANES)
        both = jnp.where(lane == LANES - 1, top, bottom).T
        rows_ref[c : c + 1, 0:side] = both[0:1]
        rows_ref[c : c + 1, side : 2 * side] = both[LANES - 1 : LANES]
    width = pack * capacity
    route = route_ref[...]
    block, place = block_of(route, width, blocks)
    entries = spread(parts_of(rows_ref[...]), block, blocks)
    got = contract_lanes(jnp.concatenate(entries, 0), places(place, width))
    write_messages(out_ref, got, pack, blocks)
    leaving = [
        pltpu.make_async_copy(source, target, out_sems.at[at])
        for at, (source, target) in enumerate(
            ((out_ref, message_hbm), (xdn, xdn_hbm), (xup, xup_hbm))
        )
    ]
    leaving[0].start()
    sides_ref[0:1, :] = route[:, 0:side]
    sides_ref[1:2, :] = route[:, side : 2 * side]
    for copy in copies[2:5]:
        copy.wait()
    for c in range(13):
        ref = component(u_ref, v_ref, stress_ref, hour_ref, c)
        xup[c * columns : (c + 1) * columns, :] = ref[planes - 1]
        if c < 6:
            xdn[c * columns : (c + 1) * columns, :] = ref[0]
    leaving[1].start()
    leaving[2].start()
    for c in range(13):
        ref = component(u_ref, v_ref, stress_ref, hour_ref, c)
        yup[c] = ref[:, columns - 1, :]
        if c < 6:
            ydn[c] = ref[:, 0, :]
    for copy in copies[5:] + leaving:
        copy.wait()


def component(u_ref, v_ref, stress_ref, hour_ref, c):
    if c < 3:
        return u_ref.at[c]
    if c < 6:
        return v_ref.at[c - 3]
    if c < 12:
        return stress_ref.at[c - 6]
    return hour_ref


def corner_body(columns, xu, xd, left_ref, right_ref):
    left_ref[...] = jnp.zeros(left_ref.shape, jnp.float32)
    right_ref[...] = jnp.zeros(right_ref.shape, jnp.float32)
    for c in range(13):
        at = c * columns
        right_ref[c : c + 1, :] = xd[at + columns - 1 : at + columns, :]
        if c < 6:
            left_ref[c : c + 1, :] = xd[at : at + 1, :]
            left_ref[8 + c : 9 + c, :] = xu[at : at + 1, :]
            right_ref[16 + c : 17 + c, :] = xu[at + columns - 1 : at + columns, :]


def matrix_body(nodes_ref, diag_ref, matrix_ref, lines_ref, diag_lines_ref):
    pairs = nodes_ref.shape[1]
    group = 16

    def rows(g, carry):
        start = pl.multiple_of(g * group, group)
        slot = lax.broadcasted_iota(jnp.int32, (group, pairs), 0) + start
        total = jnp.where(nodes_ref[0:1, :] == slot, 1.0, 0.0)
        for j in range(1, 5):
            total = total - jnp.where(nodes_ref[j : j + 1, :] == slot, 0.25, 0.0)
        matrix_ref[pl.ds(start, group), :] = total.astype(jnp.bfloat16)
        return carry

    lax.fori_loop(0, matrix_ref.shape[0] // group, rows, 0)
    for r in range(pairs // LANES):
        for j in range(5):
            lines_ref[j, r : r + 1, :] = nodes_ref[j : j + 1, r * LANES : (r + 1) * LANES]
        for c in range(6):
            diag_lines_ref[c, r : r + 1, :] = diag_ref[c : c + 1, r * LANES : (r + 1) * LANES]


def dense_rows(table_ref, rows_ref, capacity, pack, offset):
    together = LANES // capacity
    lane = lax.broadcasted_iota(jnp.int32, (8, LANES), 1)
    for b in range(rows_ref.shape[0]):
        total = None
        for q in range(min(together, table_ref.shape[0] - b * together)):
            tile = table_ref[seat(b * together + q, table_ref.shape[0])]
            if pack > 1:
                tile = jnp.where((lane >= offset) & (lane < offset + capacity), tile, 0.0)
                tile = pltpu.roll(tile, (q * capacity - offset) & (LANES - 1), 1)
            elif q:
                tile = pltpu.roll(tile, q * capacity, 1)
            total = tile if total is None else total + tile
        rows_ref[b] = total
    return together * capacity


def looked_up(rows_ref, slots, width):
    shape = slots[0].shape
    found = [[None] * 3 for _ in slots]
    for b in range(rows_ref.shape[0]):
        rows = [jnp.broadcast_to(rows_ref[b, c : c + 1, :], shape) for c in range(3)]
        for slot, old in zip(slots, found):
            place = slot - b * width
            here = place >= 0
            for c in range(3):
                new = jnp.take_along_axis(rows[c], place & (LANES - 1), axis=1)
                old[c] = jnp.where(here, new, old[c]) if b else new
    return found


def pair_body(
    capacity, pack, blocks,
    table_ref, nodes_ref, diag_ref, gap_ref, stiff_ref, matrix_ref,
    out_hbm, rows_ref, out_ref, dense_ref, sem,
):
    offset = (lax.axis_index("space") % pack) * capacity
    dense = dense_rows(table_ref, dense_ref, capacity, pack, offset)
    picked = looked_up(dense_ref, [nodes_ref[j] for j in range(5)], dense)
    slave = picked[0]
    first = [diag_ref[c] + picked[3][c] - picked[1][c] for c in range(3)]
    second = [diag_ref[3 + c] + picked[4][c] - picked[2][c] for c in range(3)]
    normal = [
        first[(c + 1) % 3] * second[(c + 2) % 3] - first[(c + 2) % 3] * second[(c + 1) % 3]
        for c in range(3)
    ]
    gap = gap_ref[...]
    for c in range(3):
        centre = (picked[1][c] + picked[2][c] + picked[3][c] + picked[4][c]) * 0.25
        gap = gap + (slave[c] - centre) * normal[c]
    push = stiff_ref[...] * jnp.maximum(-gap, 0.0)
    out_ref[...] = jnp.zeros(out_ref.shape, jnp.float32)
    rows_ref[...] = jnp.zeros(rows_ref.shape, jnp.float32)
    for c in range(3):
        force = push * normal[c]
        for r in range(force.shape[0]):
            rows_ref[c : c + 1, r * LANES : (r + 1) * LANES] = force[r : r + 1]
    parts = [part.astype(jnp.bfloat16) for part in parts_of(rows_ref[...])]
    got = contract_lanes(jnp.concatenate(parts, 0), matrix_ref[...])
    total = got[0:8] + got[8:16] + got[16:24]
    width = pack * capacity
    for b in range(blocks):
        for q in range(pack):
            block = total[:, b * width : (b + 1) * width]
            out_ref[seat(b * pack + q, out_ref.shape[0]), :, 0:width] = block
    copy = pltpu.make_async_copy(out_ref, out_hbm, sem)
    copy.start()
    copy.wait()


def split(value):
    return jnp.stack([value[:, at : at + LANES] for at in range(0, value.shape[1], LANES)])


def z_pair(f):
    lane = lax.broadcasted_iota(jnp.int32, f.shape, 2)
    turned = pltpu.roll(f, LANES - 1, 2)
    after = jnp.concatenate([turned[1:], turned[:1]], 0)
    upper = jnp.where(lane == LANES - 1, after, turned)
    return f + upper, upper - f


def node_terms(sums, diffs, sums_next, diffs_next):
    result = []
    for c in range(6):
        s0, s1, d0, d1 = sums[c], sums_next[c], diffs[c], diffs_next[c]
        if c < 3:
            result.append((s0 + s1, s1 - s0, d0 + d1))
        else:
            result.append((d1 - d0, d0 + d1, s1 - s0))
    return result


def element_terms(lower, upper, stress, hour):
    eight = []
    for m in range(3):
        row = [
            upper[m][0] - lower[m][0],
            lower[m][1] + upper[m][1],
            lower[m][2] + upper[m][2],
        ]
        row[m] = row[m] + 4.0
        eight.append(row)
    cof = [
        [
            eight[(m + 1) % 3][(n + 1) % 3] * eight[(m + 2) % 3][(n + 2) % 3]
            - eight[(m + 1) % 3][(n + 2) % 3] * eight[(m + 2) % 3][(n + 1) % 3]
            for n in range(3)
        ]
        for m in range(3)
    ]
    hour = hour * 64.0
    result = []
    for m in range(3):
        line = [
            stress[VOIGT[m][0]] * cof[0][n]
            + stress[VOIGT[m][1]] * cof[1][n]
            + stress[VOIGT[m][2]] * cof[2][n]
            for n in range(3)
        ]
        low, up = lower[3 + m], upper[3 + m]
        line.append(hour * (low[0] + up[0]))
        line.append(hour * (up[1] - low[1]))
        line.append(hour * (up[2] - low[2]))
        line.append(hour * (up[0] - low[0]))
        result.append(line)
    return result


def gathered_x(before, after):
    result = []
    for m in range(3):
        p, n = before[m], after[m]
        result.append(
            (
                p[0] - n[0],
                (p[1] + n[1]) + (p[5] - n[5]),
                (p[2] + n[2]) + (p[4] - n[4]),
                (p[3] + n[3]) + (p[6] - n[6]),
            )
        )
    return result


def along_z(p, r):
    lane = lax.broadcasted_iota(jnp.int32, p.shape, 2)
    block = lax.broadcasted_iota(jnp.int32, p.shape, 0)
    nb = p.shape[0]
    up = pltpu.roll(p + r, 1, 2)
    before_up = jnp.concatenate([jnp.zeros_like(up[:1]), up[:-1]], 0)
    last = (lane == LANES - 1) & (block == nb - 1)
    return jnp.where(lane == 0, before_up, up) + jnp.where(last, 0.0, p - r)


def edge_body(columns, ydn, yd, xu, xd, corner, out_ref, row_ref):
    planes = ydn.shape[1]
    rows = row_ref.shape[0]
    row_ref[...] = jnp.zeros(row_ref.shape, jnp.float32)

    def assembled(first, middle, last):
        row_ref[0:1, :] = first
        row_ref[1 : planes + 1, :] = middle
        if last is not None:
            row_ref[planes + 1 : planes + 2, :] = last
        return split(row_ref[...])

    def line(ref, at):
        return ref[at : at + 1, :]

    def following(q):
        return pltpu.roll(q, rows - 1, 1)

    left_s, left_d, own_s, own_d = [], [], [], []
    for c in range(6):
        s, d = z_pair(assembled(line(corner, c), yd[c], line(corner, 16 + c)))
        left_s.append(s)
        left_d.append(d)
        s, d = z_pair(assembled(line(xd, c * columns), ydn[c], line(xu, c * columns)))
        own_s.append(s)
        own_d.append(d)
    stress = [assembled(line(corner, 6 + c), yd[6 + c], None) for c in range(6)]
    hour = assembled(line(corner, 12), yd[12], None)
    lower = node_terms(left_s, left_d, own_s, own_d)
    upper = [tuple(following(q) for q in terms) for terms in lower]
    factors = element_terms(lower, upper, stress, hour)
    after = [[following(q) for q in terms] for terms in factors]
    for m, (a, b, c, e) in enumerate(gathered_x(factors, after)):
        out_ref[m, 0] = a + b
        out_ref[m, 1] = c + e


def node_plane(values, halo_s, halo_d):
    row = lax.broadcasted_iota(jnp.int32, values[0].shape, 1)
    end = values[0].shape[1] - 1
    sums, diffs, sums_next, diffs_next = [], [], [], []
    for c in range(6):
        s, d = z_pair(values[c])
        sums.append(s)
        diffs.append(d)
        sums_next.append(jnp.where(row == end, halo_s[c], pltpu.roll(s, end, 1)))
        diffs_next.append(jnp.where(row == end, halo_d[c], pltpu.roll(d, end, 1)))
    return node_terms(sums, diffs, sums_next, diffs_next)


def kept_nodes(node_ref, i):
    return [tuple(node_ref[i, c, t] for t in range(3)) for c in range(6)]


def kept_elements(elem_ref, i):
    return [[elem_ref[i, m, t] for t in range(7)] for m in range(3)]


def new_velocity(before, after, left, velocity, mass):
    row = lax.broadcasted_iota(jnp.int32, mass.shape, 1)
    weight = (time_step / 64.0) / mass
    result = []
    for m, (a, b, c, e) in enumerate(gathered_x(before, after)):
        p = (a - b) + jnp.where(row == 0, left[m][0], pltpu.roll(a + b, 1, 1))
        r = (c - e) + jnp.where(row == 0, left[m][1], pltpu.roll(c + e, 1, 1))
        result.append(velocity[m] - along_z(p, r) * weight)
    return result


def steps(start, stop, unroll, body):
    count = (stop - start) // unroll

    def several(t, carry):
        for k in range(unroll):
            body(start + t * unroll + k)
        return carry

    lax.fori_loop(0, count, several, 0)
    for i in range(start + count * unroll, stop):
        body(jnp.int32(i))


def inner_body(
    unroll, u_ref, v_ref, stress_ref, hour_ref, yu, node_ref, elem_ref, halo_s, halo_d
):
    planes = u_ref.shape[1]
    for c in range(6):
        halo_s[c], halo_d[c] = z_pair(split(yu[c]))

    def nodes(i):
        values = [split(u_ref[c, i]) for c in range(3)] + [split(v_ref[c, i]) for c in range(3)]
        terms = node_plane(
            values,
            [halo_s[c, :, pl.ds(i, 1), :] for c in range(6)],
            [halo_d[c, :, pl.ds(i, 1), :] for c in range(6)],
        )
        for c in range(6):
            for t in range(3):
                node_ref[i, c, t] = terms[c][t]

    def elements(i):
        factors = element_terms(
            kept_nodes(node_ref, i),
            kept_nodes(node_ref, i + 1),
            [split(stress_ref[c, i]) for c in range(6)],
            split(hour_ref[i]),
        )
        for m in range(3):
            for t in range(7):
                elem_ref[i, m, t] = factors[m][t]

    steps(0, planes, unroll, nodes)
    steps(0, planes - 1, unroll, elements)


def outer_body(
    unroll, v_ref, stress_ref, hour_ref, mass_ref, node_ref, elem_ref, edge_ref, xu, xd, corner,
    out_ref,
):
    planes, columns, depth = v_ref.shape[1:]
    last = planes - 1

    def write_plane(i, before, after):
        velocity = [split(v_ref[m, i]) for m in range(3)]
        left = [[edge_ref[m, t, :, pl.ds(i, 1), :] for t in range(2)] for m in range(3)]
        result = new_velocity(before, after, left, velocity, split(mass_ref[i]))
        for m in range(3):
            for k in range(depth // LANES):
                out_ref[m, i, :, k * LANES : (k + 1) * LANES] = result[m][k]

    def inside(i):
        write_plane(i, kept_elements(elem_ref, i - 1), kept_elements(elem_ref, i))

    def part(ref, c):
        return split(ref[c * columns : (c + 1) * columns, :])

    def plane_terms(ref, at):
        halo_s, halo_d = z_pair(split(corner[at : at + 8, :]))
        return node_plane(
            [part(ref, c) for c in range(6)],
            [halo_s[:, c : c + 1] for c in range(6)],
            [halo_d[:, c : c + 1] for c in range(6)],
        )

    below = element_terms(
        plane_terms(xd, 0),
        kept_nodes(node_ref, 0),
        [part(xd, 6 + c) for c in range(6)],
        part(xd, 12),
    )
    above = element_terms(
        kept_nodes(node_ref, last),
        plane_terms(xu, 8),
        [split(stress_ref[c, last]) for c in range(6)],
        split(hour_ref[last]),
    )
    write_plane(0, below, kept_elements(elem_ref, 0))
    write_plane(last, kept_elements(elem_ref, last - 1), above)
    steps(1, last, unroll, inside)


def final_body(
    capacity, pack,
    base_ref, mass_ref, table_ref, route_ref,
    out_hbm, rows_ref, out_ref, dense_ref, sems,
):
    planes, columns, depth = base_ref.shape[1:]
    offset = (lax.axis_index("space") % pack) * capacity
    dense = dense_rows(table_ref, dense_ref, capacity, pack, offset)
    (contact,) = looked_up(dense_ref, [route_ref[...]], dense)
    rows_ref[...] = jnp.zeros(rows_ref.shape, jnp.float32)
    lane = lax.broadcasted_iota(jnp.int32, (planes, columns, LANES), 2)
    low_weight = jnp.where(lane == 0, time_step / mass_ref[:, :, 0:LANES], 0.0)
    high_weight = jnp.where(
        lane == LANES - 1, time_step / mass_ref[:, :, depth - LANES : depth], 0.0
    )
    copies = []
    for m in range(3):
        rows_ref[m, 0:1, :] = contact[m][0:1]
        rows_ref[m, LANES - 1 : LANES, :] = contact[m][1:2]
        turned = rows_ref[m].T.reshape(planes, columns, LANES)
        for k in range(0, depth, LANES):
            value = base_ref[m, :, :, k : k + LANES]
            if k == 0:
                value = value + low_weight * turned
            if k == depth - LANES:
                value = value + high_weight * turned
            out_ref[m, :, :, k : k + LANES] = value
        copies.append(pltpu.make_async_copy(out_ref.at[m], out_hbm.at[m], sems.at[m]))
        copies[m].start()
    for copy in copies:
        copy.wait()


def local(
    displacement,
    velocity,
    stress,
    hourglass,
    mass,
    contact_route,
    pair_nodes,
    pair_diagonals,
    pair_gap,
    pair_stiffness,
):
    planes, columns, depth = displacement.shape[1:]
    nspace = lax.axis_size("space")
    surf_count = 2 * planes * columns
    pairs = pair_nodes.shape[1]
    capacity, pack, blocks = layout(nspace, surf_count)
    f32 = jnp.float32
    lines = pairs // LANES

    def sized(*shape):
        return jax.ShapeDtypeStruct(shape, f32)

    message = sized(nspace, 8, LANES)
    small = (pair_nodes, pair_diagonals, pair_gap.reshape(lines, LANES))
    small += (pair_stiffness.reshape(lines, LANES),)
    kept = (displacement, velocity, stress, hourglass, mass) + small
    outgoing, xdn, xup, ydn, yup, sides, *kept = kernel_call(
        functools.partial(first_body, capacity, pack, blocks),
        (displacement, contact_route.reshape(1, surf_count)) + kept[1:],
        (
            pltpu.HBM(message.shape, f32),
            pltpu.HBM((6 * columns, depth), f32),
            pltpu.HBM((13 * columns, depth), f32),
            sized(6, planes, depth),
            sized(13, planes, depth),
            jax.ShapeDtypeStruct((2, surf_count // 2), jnp.int32),
            *(jax.ShapeDtypeStruct(one.shape, one.dtype) for one in kept),
        ),
        [
            pltpu.VMEM(message.shape, f32),
            pltpu.VMEM((6 * columns, depth), f32),
            pltpu.VMEM((13 * columns, depth), f32),
            pltpu.VMEM((8, surf_count), f32),
            pltpu.VMEM((1, surf_count), jnp.int32),
            pltpu.SemaphoreType.DMA((len(kept) + 1,)),
            pltpu.SemaphoreType.DMA((3,)),
        ],
        hbm_inputs=len(kept) + 1,
    )
    fields, (pair_nodes, pair_diagonals, gap, stiffness) = kept[:5], kept[5:]
    received = exchanged(outgoing)
    yu = shifted(ydn, "slab", -1)
    yd = shifted(yup, "slab", 1)
    xu = shifted(xdn, "space", -1)
    xd = shifted(xup, "space", 1)
    slots = (nspace * capacity + 15) // 16 * 16
    matrix, nodes, diagonals = kernel_call(
        matrix_body,
        (pair_nodes, pair_diagonals),
        (
            jax.ShapeDtypeStruct((slots, pairs), jnp.bfloat16),
            jax.ShapeDtypeStruct((5, lines, LANES), jnp.int32),
            sized(6, lines, LANES),
        ),
    )
    dense = pltpu.VMEM((pl.cdiv(nspace, LANES // capacity), 8, LANES), f32)
    slot_force = kernel_call(
        functools.partial(pair_body, capacity, pack, blocks),
        (received, nodes, diagonals, gap, stiffness, matrix),
        pltpu.HBM(message.shape, f32),
        [
            pltpu.VMEM((8, pairs), f32),
            pltpu.VMEM(message.shape, f32),
            dense,
            pltpu.SemaphoreType.DMA,
        ],
    )
    returned = exchanged(slot_force)

    to_left, to_right = kernel_call(
        functools.partial(corner_body, columns), (xu, xd), (sized(16, depth), sized(24, depth))
    )
    right_corner = shifted(to_left, "slab", -1)
    left_corner = shifted(to_right, "slab", 1)
    nb = depth // LANES
    node, elem = kernel_call(
        functools.partial(inner_body, 2),
        (*fields[:4], yu),
        (
            sized(planes, 6, 3, nb, columns, LANES),
            sized(planes - 1, 3, 7, nb, columns, LANES),
        ),
        [
            pltpu.VMEM((6, nb, planes, LANES), f32),
            pltpu.VMEM((6, nb, planes, LANES), f32),
        ],
    )
    rows = (planes + 2 + 7) // 8 * 8
    edge = kernel_call(
        functools.partial(edge_body, columns),
        (ydn, yd, xu, xd, left_corner),
        sized(3, 2, nb, rows, LANES),
        [pltpu.VMEM((rows, depth), f32)],
    )
    base = kernel_call(
        functools.partial(outer_body, 2),
        (*fields[1:], node, elem, edge, xu, xd, right_corner),
        sized(*displacement.shape),
    )

    return kernel_call(
        functools.partial(final_body, capacity, pack),
        (base, fields[4], returned, sides),
        pltpu.HBM(displacement.shape, f32),
        [
            pltpu.VMEM((3, LANES, LANES), f32),
            pltpu.VMEM(displacement.shape, f32),
            dense,
            pltpu.SemaphoreType.DMA((3,)),
        ],
    )


def solution(mesh):
    in_specs = (
        P(None, "space", "slab", None),
        P(None, "space", "slab", None),
        P(None, "space", "slab", None),
        P("space", "slab", None),
        P("space", "slab", None),
        P(("space", "slab")),
        P(None, ("space", "slab")),
        P(None, ("space", "slab")),
        P(("space", "slab")),
        P(("space", "slab")),
    )
    out_specs = P(None, "space", "slab", None)
    return jax.shard_map(local, mesh=mesh, in_specs=in_specs, out_specs=out_specs, check_vma=False)
```
